16 devices in a mesh: replica: 2 (over y, z), model: 8 (over x, core).
Axes of the slice: x: 4, y: 2, z: 1, core: 2. Of those that a mesh axis runs over, the one named last changes fastest.
The devices are a block of a 4x4x8 slice.
Arguments:
- prompt: bfloat16 [32, 768, 2048], P('replica', 'model'), parts along dimension 0
- lengths: int32 [32], P('replica'), parts along dimension 0
- new_tok: bfloat16 [32, 2048], P('replica'), parts along dimension 0
- norm_attn: bfloat16 [1, 2048], replicated
- w_q: bfloat16 [1, 2048, 2048], P(None, None, 'model')
- w_k: bfloat16 [1, 2048, 2048], P(None, None, 'model')
- w_v: bfloat16 [1, 2048, 2048], P(None, None, 'model')
- w_o: bfloat16 [1, 2048, 2048], P(None, 'model')
- norm_mlp: bfloat16 [1, 2048], replicated
- w_gate: bfloat16 [1, 2048, 8192], P(None, None, 'model')
- w_up: bfloat16 [1, 2048, 8192], P(None, None, 'model')
- w_down: bfloat16 [1, 8192, 2048], P(None, 'model')
Outputs:
- output 1: bfloat16 [32, 2048], P('replica'), parts along dimension 0
- output 2: bfloat16 [32, 2048], P('replica'), parts along dimension 0
- output 3: bfloat16 [1, 32, 769, 16, 128], P(None, 'replica', None, 'model'), parts along dimension 1
- output 4: bfloat16 [1, 32, 769, 16, 128], P(None, 'replica', None, 'model'), parts along dimension 1
There are 2 independent parts. The reference program is written for one: setup_inputs(seed, part) draws one part's arguments, and reference() takes and returns one part's arrays. A program takes and returns all parts, laid end to end along the dimension named above; an argument that names none is the same for every part.
All inputs are finite; a program needn't handle non-finite values.
Results may differ from the reference program's by a relative error of at most 0.0109685.
Values are sent between devices in bfloat16 or wider.
A program may use at most 768 MiB of HBM per device.

```python
import jax
import jax.numpy as jnp
from jax import lax

BATCH_SIZE = 16
SEQ_LEN = 768
Q_BLOCK = 96
D_MODEL = 2048
NUM_HEADS = 16
KV_HEADS = 16
HEAD_DIM = 128
FF_DIM = 8192
N_LAYERS = 1

Q_WIDTH = NUM_HEADS * HEAD_DIM
KV_WIDTH = KV_HEADS * HEAD_DIM
GROUP_SIZE = NUM_HEADS // KV_HEADS
N_QBLOCKS = SEQ_LEN // Q_BLOCK
N_TOKENS = BATCH_SIZE * SEQ_LEN


def setup_inputs(seed: int = 0, part: int = 0) -> dict:
    part_keys = jax.random.split(jax.random.fold_in(jax.random.key(seed), part), 4)
    shared_keys = jax.random.split(jax.random.key(seed + 1), 9)
    qk_scale = (2.0 / D_MODEL) ** 0.5
    in_scale = D_MODEL ** -0.5

    def normal_bf16(rng_key, dims, scale_val):
        return (jax.random.normal(rng_key, dims, jnp.float32) * scale_val).astype(jnp.bfloat16)

    def gain_bf16(rng_key):
        return jax.random.uniform(rng_key, (N_LAYERS, D_MODEL), jnp.float32, 0.6, 1.4).astype(jnp.bfloat16)

    lengths = jax.random.randint(part_keys[1], (BATCH_SIZE,), SEQ_LEN // 2 + 1, SEQ_LEN + 1)
    full_row = jax.random.randint(part_keys[2], (), 0, BATCH_SIZE)
    lengths = jnp.where(jnp.arange(BATCH_SIZE) == full_row, SEQ_LEN, lengths).astype(jnp.int32)
    return {
        'prompt': normal_bf16(part_keys[0], (BATCH_SIZE, SEQ_LEN, D_MODEL), 1.0),
        'lengths': lengths,
        'new_tok': normal_bf16(part_keys[3], (BATCH_SIZE, D_MODEL), 1.0),
        'norm_attn': gain_bf16(shared_keys[0]),
        'w_q': normal_bf16(shared_keys[1], (N_LAYERS, D_MODEL, Q_WIDTH), qk_scale),
        'w_k': normal_bf16(shared_keys[2], (N_LAYERS, D_MODEL, KV_WIDTH), qk_scale),
        'w_v': normal_bf16(shared_keys[3], (N_LAYERS, D_MODEL, KV_WIDTH), in_scale),
        'w_o': normal_bf16(shared_keys[4], (N_LAYERS, Q_WIDTH, D_MODEL), Q_WIDTH ** -0.5),
        'norm_mlp': gain_bf16(shared_keys[5]),
        'w_gate': normal_bf16(shared_keys[6], (N_LAYERS, D_MODEL, FF_DIM), in_scale),
        'w_up': normal_bf16(shared_keys[7], (N_LAYERS, D_MODEL, FF_DIM), in_scale),
        'w_down': normal_bf16(shared_keys[8], (N_LAYERS, FF_DIM, D_MODEL), FF_DIM ** -0.5),
    }


def rms_norm(hidden, gain_vec):
    hid_f32 = hidden.astype(jnp.float32)
    inv_rms = lax.rsqrt(jnp.mean(hid_f32 * hid_f32, axis=-1, keepdims=True) + 1e-5)
    return (hid_f32 * inv_rms * gain_vec.astype(jnp.float32)).astype(jnp.bfloat16)


def rotary(heads_f32, positions):
    half_dim = HEAD_DIM // 2
    inv_freq = 10000.0 ** (-2.0 * jnp.arange(half_dim, dtype=jnp.float32) / HEAD_DIM)
    angles = positions.astype(jnp.float32)[..., None] * inv_freq
    cos_tab = jnp.cos(angles)[..., None, :]
    sin_tab = jnp.sin(angles)[..., None, :]
    lo_half = heads_f32[..., :half_dim]
    hi_half = heads_f32[..., half_dim:]
    return jnp.concatenate([lo_half * cos_tab - hi_half * sin_tab, hi_half * cos_tab + lo_half * sin_tab], axis=-1)


def prefill_attention(queries, key_rot, val_proj, lengths):
    q_blocks = jnp.moveaxis(queries.astype(jnp.float32).reshape(BATCH_SIZE, N_QBLOCKS, Q_BLOCK, KV_HEADS, GROUP_SIZE, HEAD_DIM), 1, 0)
    key_f32 = key_rot.astype(jnp.float32)
    val_f32 = val_proj.astype(jnp.float32)
    key_pos = jnp.arange(SEQ_LEN)
    key_valid = key_pos[None, :] < lengths[:, None]

    def one_block(block_args):
        q_blk, blk_idx = block_args
        q_pos = blk_idx * Q_BLOCK + jnp.arange(Q_BLOCK)
        scores = jnp.einsum('bqhgd,bkhd->bqhgk', q_blk, key_f32) * (HEAD_DIM ** -0.5)
        visible = (key_pos[None, None, :] <= q_pos[None, :, None]) & key_valid[:, None, :]
        scores = jnp.where(visible[:, :, None, None, :], scores, -1e30)
        attn_prob = jax.nn.softmax(scores, axis=-1)
        return jnp.einsum('bqhgk,bkhd->bqhgd', attn_prob, val_f32)

    blocks_out = lax.map(one_block, (q_blocks, jnp.arange(N_QBLOCKS)))
    return jnp.moveaxis(blocks_out, 0, 1).reshape(BATCH_SIZE, SEQ_LEN, Q_WIDTH).astype(jnp.bfloat16)


def decode_attention(q_new, key_cache, value_cache, lengths):
    q_f32 = q_new.astype(jnp.float32).reshape(BATCH_SIZE, KV_HEADS, GROUP_SIZE, HEAD_DIM)
    scores = jnp.einsum('bhgd,bkhd->bhgk', q_f32, key_cache.astype(jnp.float32)) * (HEAD_DIM ** -0.5)
    cache_pos = jnp.arange(SEQ_LEN + 1)
    visible = (cache_pos[None, :] < lengths[:, None]) | (cache_pos[None, :] == SEQ_LEN)
    scores = jnp.where(visible[:, None, None, :], scores, -1e30)
    attn_prob = jax.nn.softmax(scores, axis=-1)
    out_f32 = jnp.einsum('bhgk,bkhd->bhgd', attn_prob, value_cache.astype(jnp.float32))
    return out_f32.reshape(BATCH_SIZE, Q_WIDTH).astype(jnp.bfloat16)


def reference(prompt, lengths, new_tok, norm_attn, w_q, w_k, w_v, w_o, norm_mlp, w_gate, w_up, w_down):
    seq_pos = jnp.arange(SEQ_LEN)

    def layer_step(loop_state, layer_w):
        hidden, dec_hidden = loop_state
        g_attn, wq_l, wk_l, wv_l, wo_l, g_mlp, wg_l, wu_l, wd_l = layer_w
        normed = rms_norm(hidden, g_attn).reshape(N_TOKENS, D_MODEL)
        q_rot = rotary(jnp.dot(normed, wq_l, preferred_element_type=jnp.float32).reshape(BATCH_SIZE, SEQ_LEN, NUM_HEADS, HEAD_DIM), seq_pos).astype(jnp.bfloat16)
        k_rot = rotary(jnp.dot(normed, wk_l, preferred_element_type=jnp.float32).reshape(BATCH_SIZE, SEQ_LEN, KV_HEADS, HEAD_DIM), seq_pos).astype(jnp.bfloat16)
        v_proj = jnp.dot(normed, wv_l, preferred_element_type=jnp.float32).astype(jnp.bfloat16).reshape(BATCH_SIZE, SEQ_LEN, KV_HEADS, HEAD_DIM)
        attn_out = prefill_attention(q_rot, k_rot, v_proj, lengths).reshape(N_TOKENS, Q_WIDTH)
        hidden = (hidden.astype(jnp.float32) + jnp.dot(attn_out, wo_l, preferred_element_type=jnp.float32).reshape(BATCH_SIZE, SEQ_LEN, D_MODEL)).astype(jnp.bfloat16)
        normed = rms_norm(hidden, g_mlp).reshape(N_TOKENS, D_MODEL)
        mlp_mid = (jax.nn.silu(jnp.dot(normed, wg_l, preferred_element_type=jnp.float32)) * jnp.dot(normed, wu_l, preferred_element_type=jnp.float32)).astype(jnp.bfloat16)
        hidden = (hidden.astype(jnp.float32) + jnp.dot(mlp_mid, wd_l, preferred_element_type=jnp.float32).reshape(BATCH_SIZE, SEQ_LEN, D_MODEL)).astype(jnp.bfloat16)

        tok_norm = rms_norm(dec_hidden, g_attn)
        q_new = rotary(jnp.dot(tok_norm, wq_l, preferred_element_type=jnp.float32).reshape(BATCH_SIZE, NUM_HEADS, HEAD_DIM), lengths).astype(jnp.bfloat16)
        k_new = rotary(jnp.dot(tok_norm, wk_l, preferred_element_type=jnp.float32).reshape(BATCH_SIZE, KV_HEADS, HEAD_DIM), lengths).astype(jnp.bfloat16)
        v_new = jnp.dot(tok_norm, wv_l, preferred_element_type=jnp.float32).astype(jnp.bfloat16).reshape(BATCH_SIZE, KV_HEADS, HEAD_DIM)
        key_cache = jnp.concatenate([k_rot, k_new[:, None]], axis=1)
        value_cache = jnp.concatenate([v_proj, v_new[:, None]], axis=1)
        tok_attn = decode_attention(q_new, key_cache, value_cache, lengths)
        dec_hidden = (dec_hidden.astype(jnp.float32) + jnp.dot(tok_attn, wo_l, preferred_element_type=jnp.float32)).astype(jnp.bfloat16)
        tok_norm = rms_norm(dec_hidden, g_mlp)
        tok_mid = (jax.nn.silu(jnp.dot(tok_norm, wg_l, preferred_element_type=jnp.float32)) * jnp.dot(tok_norm, wu_l, preferred_element_type=jnp.float32)).astype(jnp.bfloat16)
        dec_hidden = (dec_hidden.astype(jnp.float32) + jnp.dot(tok_mid, wd_l, preferred_element_type=jnp.float32)).astype(jnp.bfloat16)
        return (hidden, dec_hidden), (key_cache, value_cache)

    (hidden, dec_hidden), (key_cache, value_cache) = lax.scan(layer_step, (prompt, new_tok), (norm_attn, w_q, w_k, w_v, w_o, norm_mlp, w_gate, w_up, w_down))
    last_sel = seq_pos[None, :] == (lengths - 1)[:, None]
    last_hidden = jnp.sum(jnp.where(last_sel[:, :, None], hidden.astype(jnp.float32), 0.0), axis=1).astype(jnp.bfloat16)
    return dec_hidden, last_hidden, key_cache, value_cache
```

```python
import jax
import jax.numpy as jnp
from jax import lax
from jax.sharding import PartitionSpec as P

HEAD_DIM = 128
NEG_BIG = -1e30
N_CHUNKS = 4


def rms_norm(hidden, gain_vec):
    hid_f32 = hidden.astype(jnp.float32)
    inv_rms = lax.rsqrt(jnp.mean(hid_f32 * hid_f32, axis=-1, keepdims=True) + 1e-5)
    return (hid_f32 * inv_rms * gain_vec.astype(jnp.float32)).astype(jnp.bfloat16)


def rotary(heads_f32, positions):
    half_dim = HEAD_DIM // 2
    inv_freq = 10000.0 ** (-2.0 * jnp.arange(half_dim, dtype=jnp.float32) / HEAD_DIM)
    angles = positions.astype(jnp.float32)[..., None] * inv_freq
    cos_tab = jnp.cos(angles)[..., None, :]
    sin_tab = jnp.sin(angles)[..., None, :]
    lo_half = heads_f32[..., :half_dim]
    hi_half = heads_f32[..., half_dim:]
    return jnp.concatenate([lo_half * cos_tab - hi_half * sin_tab, hi_half * cos_tab + lo_half * sin_tab], axis=-1)


def dot_f32(lhs, rhs):
    return jnp.dot(lhs, rhs, preferred_element_type=jnp.float32)


def solution(mesh):
    n_dev = mesh.shape['model']
    seq_spec = P('replica', 'model', None)
    col_spec = P(None, None, 'model')
    row_spec = P(None, 'model', None)
    gain_spec = P(None, None)
    tok_spec = P('replica', None)
    cache_spec = P(None, 'replica', None, 'model', None)
    in_specs = (seq_spec, P('replica'), tok_spec, gain_spec, col_spec, col_spec, col_spec, row_spec, gain_spec, col_spec, col_spec, row_spec)
    out_specs = (tok_spec, tok_spec, cache_spec, cache_spec)

    def per_device(prompt, lengths, new_tok, norm_attn, w_q, w_k, w_v, w_o, norm_mlp, w_gate, w_up, w_down):
        my_idx = lax.axis_index('model')
        n_batch, seq_loc, d_model = prompt.shape
        heads = w_q.shape[2] // HEAD_DIM
        seq_len = seq_loc * n_dev
        wq, wk, wv, wo, wg, wu, wd = w_q[0], w_k[0], w_v[0], w_o[0], w_gate[0], w_up[0], w_down[0]
        normed = rms_norm(prompt, norm_attn[0])
        last_loc = lengths - 1 - my_idx * seq_loc
        mine = (last_loc >= 0) & (last_loc < seq_loc)
        picked = jnp.take_along_axis(prompt, jnp.clip(last_loc, 0, seq_loc - 1)[:, None, None], axis=1)[:, 0]
        last_x = lax.psum(jnp.where(mine[:, None], picked, 0).astype(jnp.float32), 'model').astype(jnp.bfloat16)

        pos = jnp.arange(seq_len)
        per = n_batch // N_CHUNKS
        keys, vals = [], []
        for c in range(N_CHUNKS):
            full = lax.all_gather(normed[c * per:(c + 1) * per], 'model', axis=1, tiled=True)
            flat = full.reshape(per * seq_len, d_model)
            k_c = rotary(dot_f32(flat, wk).reshape(per, seq_len, heads, HEAD_DIM), pos).astype(jnp.bfloat16)
            v_c = dot_f32(flat, wv).astype(jnp.bfloat16).reshape(per, seq_len, heads, HEAD_DIM)
            keys.append(k_c)
            vals.append(v_c)
        key_pre = jnp.concatenate(keys, axis=0)
        val_pre = jnp.concatenate(vals, axis=0)

        rows = jnp.concatenate([new_tok, last_x], axis=0)
        rows_n = rms_norm(rows, norm_attn[0])
        row_pos = jnp.concatenate([lengths, lengths - 1], axis=0)
        q_rows = rotary(dot_f32(rows_n, wq).reshape(2 * n_batch, heads, HEAD_DIM), row_pos).astype(jnp.bfloat16)
        tok_n = rows_n[:n_batch]
        k_new = rotary(dot_f32(tok_n, wk).reshape(n_batch, heads, HEAD_DIM), lengths).astype(jnp.bfloat16)
        v_new = dot_f32(tok_n, wv).astype(jnp.bfloat16).reshape(n_batch, heads, HEAD_DIM)
        key_cache = jnp.concatenate([key_pre, k_new[:, None]], axis=1)
        val_cache = jnp.concatenate([val_pre, v_new[:, None]], axis=1)

        q2 = jnp.stack([q_rows[:n_batch], q_rows[n_batch:]], axis=1)
        scores = jnp.einsum('brhd,bkhd->bhrk', q2, key_cache, preferred_element_type=jnp.float32) * (HEAD_DIM ** -0.5)
        slot = jnp.arange(seq_len + 1)
        prefix = slot[None, :] < lengths[:, None]
        vis = jnp.stack([prefix | (slot[None, :] == seq_len), prefix], axis=1)
        scores = jnp.where(vis[:, None], scores, NEG_BIG)
        prob = jax.nn.softmax(scores, axis=-1)
        att = jnp.einsum('bhrk,bkhd->brhd', prob.astype(jnp.bfloat16), val_cache, preferred_element_type=jnp.float32)
        att = jnp.concatenate([att[:, 0], att[:, 1]], axis=0).reshape(2 * n_batch, heads * HEAD_DIM).astype(jnp.bfloat16)
        rows = (rows.astype(jnp.float32) + lax.psum(dot_f32(att, wo), 'model')).astype(jnp.bfloat16)
        rows_n = rms_norm(rows, norm_mlp[0])
        mid = (jax.nn.silu(dot_f32(rows_n, wg)) * dot_f32(rows_n, wu)).astype(jnp.bfloat16)
        rows = (rows.astype(jnp.float32) + lax.psum(dot_f32(mid, wd), 'model')).astype(jnp.bfloat16)
        return rows[:n_batch], rows[n_batch:], key_cache[None], val_cache[None]

    return jax.shard_map(per_device, mesh=mesh, in_specs=in_specs, out_specs=out_specs, check_vma=False)
```

```python
import functools

import numpy as np

import jax
import jax.numpy as jnp
from jax import lax
from jax.experimental import pallas as pl
from jax.experimental.pallas import tpu as pltpu
from jax.sharding import PartitionSpec as P

HEAD_DIM = 128
NEG_BIG = -1e30
MESH = pl.DeviceIdType.MESH
GROUP = 2
F32 = jnp.float32
BF16 = jnp.bfloat16


def dot_f32(lhs, rhs):
    return jnp.dot(lhs, rhs, preferred_element_type=F32)


def rms_rows(rows_f32, gain_f32):
    inv_rms = lax.rsqrt(jnp.mean(rows_f32 * rows_f32, axis=-1, keepdims=True) + 1e-5)
    return (rows_f32 * inv_rms * gain_f32).astype(BF16)


def rope_half(head_f32, cos_t, sin_t):
    return head_f32 * cos_t + pltpu.roll(head_f32, HEAD_DIM // 2, 1) * sin_t


def remote(src, dst, send_sem, recv_sem, dev):
    return pltpu.make_async_remote_copy(src_ref=src, dst_ref=dst, send_sem=send_sem, recv_sem=recv_sem,
                                        device_id={'model': dev}, device_id_type=MESH)


def wait_bytes(ref, sem):
    pltpu.make_async_copy(ref, ref, sem).wait()


def greet(me, n_dev):
    barrier = pltpu.get_barrier_semaphore()
    for off in range(1, n_dev):
        pl.semaphore_signal(barrier, inc=1, device_id={'model': lax.rem(me + off, n_dev)}, device_id_type=MESH)
    pl.semaphore_wait(barrier, n_dev - 1)


def exchange_kernel(n_dev, len_ref, x_hbm, wk_hbm, wv_hbm, wq_hbm, tok_ref, gain_ref, cos_ref, sin_ref,
                    kout, vout, q_out, rows_out, kn_out, vn_out,
                    wbuf, wq_buf, xown, xrecv, stage, ktmp, lfull, lrecv, lcols, crow, srow,
                    xcopy_sem, wcopy_sem, wrecv_sem, wsend_sem, xrecv_sem, xsend_sem,
                    kv_recv_sem, kv_send_sem, kv_local_sem, l_send_sem, l_recv_sem):
    n_batch, seq_loc, d_model = xown.shape
    n_chip = n_dev // 2
    half = n_batch // 2
    n_chunk = half // GROUP
    m_rows = GROUP * seq_loc
    me = lax.axis_index('model')
    chip, core = me // 2, lax.rem(me, 2)
    left, right = lax.rem(chip + n_chip - 1, n_chip), lax.rem(chip + 1, n_chip)
    partner = chip * 2 + 1 - core
    w_hbm = (wk_hbm, wv_hbm)
    outs = (kout, vout)

    wlocal = [pltpu.make_async_copy(w_hbm[kv], wbuf.at[0, core, kv], wcopy_sem.at[kv]) for kv in range(2)]
    for cp in wlocal:
        cp.start()

    def xcopy(ch):
        return pltpu.make_async_copy(x_hbm.at[pl.ds(ch * GROUP, GROUP)], xown.at[pl.ds(ch * GROUP, GROUP)], xcopy_sem.at[ch])

    for ch in range(2 * n_chunk):
        xcopy(ch).start()
    wq_copy = pltpu.make_async_copy(wq_hbm, wq_buf, wcopy_sem.at[2])
    wq_copy.start()

    greet(me, n_dev)

    wsends = []
    for kv in range(2):
        wsends.append(remote(w_hbm[kv], wbuf.at[1, core, kv], wsend_sem.at[0, kv], wrecv_sem.at[1, core, kv], right * 2 + core))
        wsends.append(remote(w_hbm[kv], wbuf.at[2, core, kv], wsend_sem.at[1, kv], wrecv_sem.at[2, core, kv], left * 2 + core))
        wsends.append(remote(w_hbm[kv], wbuf.at[0, core, kv], wsend_sem.at[2, kv], wrecv_sem.at[0, core, kv], partner))
    for cp in wsends:
        cp.start()
    xsends = []
    for ci in range(n_chunk):
        xsends.append(remote(x_hbm.at[pl.ds(ci * GROUP, GROUP)], xrecv.at[0, pl.ds(ci * GROUP, GROUP)],
                             xsend_sem.at[0, ci], xrecv_sem.at[0, ci], right * 2 + core))
        xsends.append(remote(x_hbm.at[pl.ds(half + ci * GROUP, GROUP)], xrecv.at[1, pl.ds(ci * GROUP, GROUP)],
                             xsend_sem.at[1, ci], xrecv_sem.at[1, ci], left * 2 + core))
    for cp in xsends:
        cp.start()

    gain = gain_ref[...].astype(F32)

    def normalize(ref):
        for g in range(GROUP):
            ref[g] = rms_rows(ref[g].astype(F32), gain)

    def make_kv(rows_ref, unit, ci, slot, kcore, owner, b0, dst, target):
        rows = rows_ref[...].reshape(m_rows, d_model)
        start = pl.multiple_of(owner * seq_loc, seq_loc)
        cos_t = jnp.concatenate([cos_ref[pl.ds(start, seq_loc), :]] * GROUP, axis=0)
        sin_t = jnp.concatenate([sin_ref[pl.ds(start, seq_loc), :]] * GROUP, axis=0)
        for kv in range(2):
            acc = dot_f32(rows, wbuf[slot, kcore, kv])
            for h in range(2):
                head = acc[:, h * HEAD_DIM:(h + 1) * HEAD_DIM]
                if kv == 0:
                    head = rope_half(head, cos_t, sin_t)
                ktmp[pl.ds(h, m_rows, stride=2), :] = head
            piece = stage.at[unit, dst, kv, pl.ds(ci * GROUP, GROUP)]
            piece.reshape(2 * m_rows, HEAD_DIM)[...] = ktmp[...].astype(BF16)
            place = outs[kv].at[pl.ds(b0, GROUP), pl.ds(start, seq_loc)]
            if target is None:
                pltpu.make_async_copy(piece, place, kv_local_sem.at[kv]).start()
            else:
                remote(piece, place, kv_send_sem, kv_recv_sem.at[kv], target).start()

    for cp in wlocal:
        cp.wait()
    base = me * seq_loc

    @pl.loop(0, 2 * n_chunk)
    def _(ch):
        xcopy(ch).wait()
        rows_ref = xown.at[pl.ds(ch * GROUP, GROUP)]
        for g in range(GROUP):
            b = ch * GROUP + g
            hit = lax.broadcasted_iota(jnp.int32, (16, seq_loc), 1) == len_ref[b] - 1 - base
            row = dot_f32(jnp.where(hit, 1.0, 0.0).astype(BF16), xown[b])
            lfull[pl.ds(b, 1), :] = row[0:1]
        normalize(rows_ref)
        make_kv(rows_ref, ch // n_chunk, lax.rem(ch, n_chunk), 0, core, me, ch * GROUP, 3, None)

    width = d_model // n_dev

    def col(j):
        return pl.ds(pl.multiple_of(j * width, width), width)

    for off in range(1, n_dev):
        peer = lax.rem(me + off, n_dev)
        remote(lfull.at[:, col(peer)], lrecv.at[me], l_send_sem.at[0], l_recv_sem.at[0], peer).start()
    lrecv[me] = lfull[:, col(me)]

    for kv in range(2):
        wait_bytes(wbuf.at[0, 1 - core, kv], wrecv_sem.at[0, 1 - core, kv])

    @pl.loop(0, 2 * n_chunk)
    def _(ch):
        make_kv(xown.at[pl.ds(ch * GROUP, GROUP)], ch // n_chunk, lax.rem(ch, n_chunk), 0, 1 - core, me, ch * GROUP, 2, partner)

    fwds = []
    for slot in (1, 2):
        for kv in range(2):
            wait_bytes(wbuf.at[slot, core, kv], wrecv_sem.at[slot, core, kv])
            fwds.append(remote(wbuf.at[slot, core, kv], wbuf.at[slot, core, kv], wsend_sem.at[2 + slot, kv],
                               wrecv_sem.at[slot, core, kv], partner))
            fwds[-1].start()
    for slot in (1, 2):
        for kv in range(2):
            wait_bytes(wbuf.at[slot, 1 - core, kv], wrecv_sem.at[slot, 1 - core, kv])

    @pl.loop(0, n_chunk)
    def _(ci):
        for kcore in range(2):
            make_kv(xown.at[pl.ds(ci * GROUP, GROUP)], 0, ci, 1, kcore, me, ci * GROUP, kcore, left * 2 + kcore)
            make_kv(xown.at[pl.ds(half + ci * GROUP, GROUP)], 1, ci, 2, kcore, me, half + ci * GROUP, kcore, right * 2 + kcore)

    wait_bytes(lrecv.at[pl.ds(0, n_dev - 1)], l_recv_sem.at[0])
    lcols[me] = jnp.sum(lrecv[...], axis=0).astype(BF16)
    for off in range(1, n_dev):
        peer = lax.rem(me + off, n_dev)
        remote(lcols.at[me], lcols.at[me], l_send_sem.at[1], l_recv_sem.at[1], peer).start()

    @pl.loop(0, n_chunk)
    def _(ci):
        for side in range(2):
            rows_ref = xrecv.at[side, pl.ds(ci * GROUP, GROUP)]
            wait_bytes(rows_ref, xrecv_sem.at[side, ci])
            normalize(rows_ref)
            owner = (left if side == 0 else right) * 2 + core
            beyond = right if side == 0 else left
            b0 = side * half + ci * GROUP
            for kcore in range(2):
                make_kv(rows_ref, 2 + side, ci, 2 - side, kcore, owner, b0, kcore, beyond * 2 + kcore)
            make_kv(rows_ref, 2 + side, ci, 0, 1 - core, owner, b0, 2, partner)
            make_kv(rows_ref, 2 + side, ci, 0, core, owner, b0, 3, None)

    wait_bytes(lcols.at[pl.ds(0, n_dev - 1)], l_recv_sem.at[1])
    wq_copy.wait()
    rows_out[0:n_batch, :] = tok_ref[...]
    for j in range(n_dev):
        rows_out[n_batch:2 * n_batch, j * width:(j + 1) * width] = lcols[j]
    for b in range(n_batch):
        for r in range(2):
            at = jnp.maximum(len_ref[b] - r, 0)
            crow[pl.ds(r * n_batch + b, 1), :] = cos_ref[pl.ds(at, 1), :]
            srow[pl.ds(r * n_batch + b, 1), :] = sin_ref[pl.ds(at, 1), :]
    rows_n = rms_rows(rows_out[...].astype(F32), gain)
    q_acc = dot_f32(rows_n, wq_buf[...])
    for h in range(2):
        q_out[:, h * HEAD_DIM:(h + 1) * HEAD_DIM] = rope_half(q_acc[:, h * HEAD_DIM:(h + 1) * HEAD_DIM], crow[...], srow[...]).astype(BF16)
    for kv, new_out in enumerate((kn_out, vn_out)):
        acc = dot_f32(rows_n[0:n_batch], wbuf[0, core, kv])
        for h in range(2):
            head = acc[:, h * HEAD_DIM:(h + 1) * HEAD_DIM]
            if kv == 0:
                head = rope_half(head, crow[0:n_batch, :], srow[0:n_batch, :])
            ktmp[pl.ds(h, n_batch, stride=2), :] = head
        new_out.reshape(2 * n_batch, HEAD_DIM)[...] = ktmp[0:2 * n_batch, :].astype(BF16)

    quarter = n_batch // 4
    seq_len = seq_loc * n_dev
    for kv in range(2):
        wait_bytes(outs[kv].at[pl.ds(0, quarter), pl.ds(0, seq_len)], kv_local_sem.at[kv])
        wait_bytes(outs[kv].at[pl.ds(0, 3 * quarter), pl.ds(0, seq_len)], kv_recv_sem.at[kv])
    for cp in wsends + fwds + xsends:
        cp.wait_send()
    wait_bytes(lrecv.at[pl.ds(0, n_dev - 1)], l_send_sem.at[0])
    wait_bytes(lcols.at[pl.ds(0, n_dev - 1)], l_send_sem.at[1])
    wait_bytes(stage.at[:, pl.ds(0, 3)], kv_send_sem)


def attention_kernel(len_ref, q_ref, kn_ref, vn_ref, k_in, v_in, k_out, v_out, att_ref):
    b = pl.program_id(0)
    n_slot = k_out.shape[1]
    k_out[0, 0:n_slot - 1] = k_in[0, 0:n_slot - 1]
    v_out[0, 0:n_slot - 1] = v_in[0, 0:n_slot - 1]
    k_out[0, n_slot - 1:n_slot] = kn_ref[...]
    v_out[0, n_slot - 1:n_slot] = vn_ref[...]
    keys = k_out.at[0].reshape(2 * n_slot, HEAD_DIM)[...]
    vals = v_out.at[0].reshape(2 * n_slot, HEAD_DIM)[...]
    scores = lax.dot_general(q_ref[0], keys, (((1,), (1,)), ((), ())), preferred_element_type=F32) * (HEAD_DIM ** -0.5)
    row = lax.broadcasted_iota(jnp.int32, scores.shape, 0)
    colm = lax.broadcasted_iota(jnp.int32, scores.shape, 1)
    slot = colm // 2
    see = (slot < len_ref[b]) | ((slot == n_slot - 1) & (row < 2))
    see = see & (lax.rem(row, 2) == lax.rem(colm, 2))
    scores = jnp.where(see, scores, NEG_BIG)
    prob = jnp.exp(scores - jnp.max(scores, axis=1, keepdims=True))
    total = jnp.sum(prob, axis=1, keepdims=True)
    att_ref[0] = dot_f32(prob.astype(BF16), vals) / total


def tail_kernel(n_dev, att_ref, rows_ref, wo_ref, gain_ref, wg_hbm, wu_hbm, wd_hbm, out_ref,
                wg, wu, wd, part, recv, hid, rows, w_sem, send_sem, recv_sem, g_send_sem, g_recv_sem):
    me = lax.axis_index('model')
    n_row, d_model = rows.shape
    width = d_model // n_dev
    copies = [pltpu.make_async_copy(src, dst, w_sem.at[i]) for i, (src, dst) in enumerate(((wg_hbm, wg), (wu_hbm, wu), (wd_hbm, wd)))]
    for cp in copies:
        cp.start()

    def col(j):
        return pl.ds(pl.multiple_of(j * width, width), width)

    def add_partials(step, residual):
        for off in range(1, n_dev):
            peer = lax.rem(me + off, n_dev)
            remote(part.at[step, :, col(peer)], recv.at[step, me], send_sem.at[step], recv_sem.at[step], peer).start()
        recv[step, me] = part[step, :, col(me)]
        wait_bytes(recv.at[step, pl.ds(0, n_dev - 1)], recv_sem.at[step])
        hid[step, me] = (residual[:, col(me)].astype(F32) + jnp.sum(recv[step], axis=0)).astype(BF16)
        for off in range(1, n_dev):
            peer = lax.rem(me + off, n_dev)
            remote(hid.at[step, me], hid.at[step, me], g_send_sem.at[step], g_recv_sem.at[step], peer).start()
        wait_bytes(hid.at[step, pl.ds(0, n_dev - 1)], g_recv_sem.at[step])

    part[0] = dot_f32(att_ref[...], wo_ref[...])
    greet(me, n_dev)
    add_partials(0, rows_ref)
    for j in range(n_dev):
        rows[:, j * width:(j + 1) * width] = hid[0, j]
    rows_n = rms_rows(rows[...].astype(F32), gain_ref[...].astype(F32))
    copies[0].wait()
    gate = dot_f32(rows_n, wg[...])
    copies[1].wait()
    up = dot_f32(rows_n, wu[...])
    mid = (gate * (1.0 / (1.0 + jnp.exp(-gate))) * up).astype(BF16)
    copies[2].wait()
    part[1] = dot_f32(mid, wd[...])
    add_partials(1, rows)
    for j in range(n_dev):
        out_ref[:, j * width:(j + 1) * width] = hid[1, j]
    for step in range(2):
        wait_bytes(recv.at[step, pl.ds(0, n_dev - 1)], send_sem.at[step])
        wait_bytes(hid.at[step, pl.ds(0, n_dev - 1)], g_send_sem.at[step])


def rotary_tables(n_pos):
    inv_freq = np.float32(10000.0) ** (-2.0 * np.arange(HEAD_DIM // 2, dtype=np.float32) / HEAD_DIM).astype(np.float32)
    angles = np.arange(n_pos, dtype=np.float32)[:, None] * inv_freq.astype(np.float32)
    cos, sin = np.cos(angles), np.sin(angles)
    return (np.concatenate([cos, cos], axis=1).astype(np.float32), np.concatenate([-sin, sin], axis=1).astype(np.float32))


def solution(mesh):
    n_dev = mesh.shape['model']
    seq_spec = P('replica', 'model', None)
    col_spec = P(None, None, 'model')
    row_spec = P(None, 'model', None)
    gain_spec = P(None, None)
    tok_spec = P('replica', None)
    cache_spec = P(None, 'replica', None, 'model', None)
    in_specs = (seq_spec, P('replica'), tok_spec, gain_spec, col_spec, col_spec, col_spec, row_spec, gain_spec, col_spec, col_spec, row_spec)
    out_specs = (tok_spec, tok_spec, cache_spec, cache_spec)
    hbm = pl.BlockSpec(memory_space=pl.ANY)
    vmem = pl.BlockSpec(memory_space=pltpu.VMEM)
    smem = pl.BlockSpec(memory_space=pltpu.SMEM)
    dma = pltpu.SemaphoreType.DMA

    def per_device(prompt, lengths, new_tok, norm_attn, w_q, w_k, w_v, w_o, norm_mlp, w_gate, w_up, w_down):
        n_batch, seq_loc, d_model = prompt.shape
        kv_width = w_k.shape[2]
        heads = kv_width // HEAD_DIM
        seq_len = seq_loc * n_dev
        half = n_batch // 2
        n_chunk = half // GROUP
        width = d_model // n_dev
        wq, wk, wv, wo, wg, wu, wd = w_q[0], w_k[0], w_v[0], w_o[0], w_gate[0], w_up[0], w_down[0]
        cos_tab, sin_tab = (jnp.asarray(t) for t in rotary_tables(seq_len + 8))

        cache = jax.ShapeDtypeStruct((n_batch, seq_len + 1, heads, HEAD_DIM), BF16)
        new_kv = jax.ShapeDtypeStruct((n_batch, heads, HEAD_DIM), BF16)
        key_buf, val_buf, q_rows, rows, k_new, v_new = pl.pallas_call(
            functools.partial(exchange_kernel, n_dev),
            out_shape=(cache, cache, jax.ShapeDtypeStruct((2 * n_batch, kv_width), BF16),
                       jax.ShapeDtypeStruct((2 * n_batch, d_model), BF16), new_kv, new_kv),
            in_specs=[smem, hbm, hbm, hbm, hbm, vmem, vmem, vmem, vmem],
            out_specs=(hbm, hbm, vmem, vmem, vmem, vmem),
            scratch_shapes=[
                pltpu.VMEM((3, 2, 2, d_model, kv_width), BF16),
                pltpu.VMEM((d_model, kv_width), BF16),
                pltpu.VMEM((n_batch, seq_loc, d_model), BF16),
                pltpu.VMEM((2, half, seq_loc, d_model), BF16),
                pltpu.VMEM((4, 4, 2, half, seq_loc, heads, HEAD_DIM), BF16),
                pltpu.VMEM((2 * GROUP * seq_loc, HEAD_DIM), F32),
                pltpu.VMEM((n_batch, d_model), F32),
                pltpu.VMEM((n_dev, n_batch, width), F32),
                pltpu.VMEM((n_dev, n_batch, width), BF16),
                pltpu.VMEM((2 * n_batch, HEAD_DIM), F32),
                pltpu.VMEM((2 * n_batch, HEAD_DIM), F32),
                dma((2 * n_chunk,)), dma((3,)), dma((3, 2, 2)), dma((5, 2)), dma((2, n_chunk)), dma((2, n_chunk)),
                dma((2,)), dma(()), dma((2,)), dma((2,)), dma((2,)),
            ],
            compiler_params=pltpu.CompilerParams(collective_id=0, has_side_effects=True, vmem_limit_bytes=60 * 2 ** 20),
            name='exchange',
        )(lengths, prompt, wk, wv, wq, new_tok, norm_attn, cos_tab, sin_tab)

        q_pairs = q_rows.reshape(2, n_batch, heads, HEAD_DIM).transpose(1, 0, 2, 3).reshape(n_batch, 2 * heads, HEAD_DIM)
        q_pairs = jnp.concatenate([q_pairs, q_pairs], axis=1)
        cache_block = pl.BlockSpec((1, seq_len + 1, heads, HEAD_DIM), lambda b, lens: (b, 0, 0, 0))
        new_block = pl.BlockSpec((1, heads, HEAD_DIM), lambda b, lens: (b, 0, 0))
        pair_block = pl.BlockSpec((1, 4 * heads, HEAD_DIM), lambda b, lens: (b, 0, 0))
        key_cache, val_cache, att = pl.pallas_call(
            attention_kernel,
            grid_spec=pltpu.PrefetchScalarGridSpec(
                num_scalar_prefetch=1, grid=(n_batch,),
                in_specs=[pair_block, new_block, new_block, cache_block, cache_block],
                out_specs=(cache_block, cache_block, pair_block)),
            out_shape=(cache, cache, jax.ShapeDtypeStruct((n_batch, 4 * heads, HEAD_DIM), F32)),
            name='attend',
        )(lengths, q_pairs, k_new, v_new, key_buf, val_buf)
        att = att[:, :2 * heads].reshape(n_batch, 2, kv_width).transpose(1, 0, 2).reshape(2 * n_batch, kv_width).astype(BF16)

        ff = wg.shape[1]
        out = pl.pallas_call(
            functools.partial(tail_kernel, n_dev),
            out_shape=jax.ShapeDtypeStruct((2 * n_batch, d_model), BF16),
            in_specs=[vmem, vmem, vmem, vmem, hbm, hbm, hbm],
            out_specs=vmem,
            scratch_shapes=[
                pltpu.VMEM((d_model, ff), BF16), pltpu.VMEM((d_model, ff), BF16), pltpu.VMEM((ff, d_model), BF16),
                pltpu.VMEM((2, 2 * n_batch, d_model), F32),
                pltpu.VMEM((2, n_dev, 2 * n_batch, width), F32),
                pltpu.VMEM((2, n_dev, 2 * n_batch, width), BF16),
                pltpu.VMEM((2 * n_batch, d_model), BF16),
                dma((3,)), dma((2,)), dma((2,)), dma((2,)), dma((2,)),
            ],
            compiler_params=pltpu.CompilerParams(collective_id=1, has_side_effects=True, vmem_limit_bytes=40 * 2 ** 20),
            name='tail',
        )(att, rows, wo, norm_mlp, wg, wu, wd)
        return out[:n_batch], out[n_batch:], key_cache[None], val_cache[None]

    return jax.shard_map(per_device, mesh=mesh, in_specs=in_specs, out_specs=out_specs, check_vma=False)
```

```python
import functools

import numpy as np

import jax
import jax.numpy as jnp
from jax import lax
from jax.experimental import pallas as pl
from jax.experimental.pallas import tpu as pltpu
from jax.sharding import PartitionSpec as P

HEAD_DIM = 128
NEG_BIG = -1e30
MESH = pl.DeviceIdType.MESH
GROUP = 2
F32 = jnp.float32
BF16 = jnp.bfloat16


def dot_f32(lhs, rhs):
    return jnp.dot(lhs, rhs, preferred_element_type=F32)


def rms_rows(rows_f32, gain_f32):
    inv_rms = lax.rsqrt(jnp.mean(rows_f32 * rows_f32, axis=-1, keepdims=True) + 1e-5)
    return (rows_f32 * inv_rms * gain_f32).astype(BF16)


def rope_half(head_f32, cos_t, sin_t):
    return head_f32 * cos_t + pltpu.roll(head_f32, HEAD_DIM // 2, 1) * sin_t


def remote(src, dst, send_sem, recv_sem, dev):
    return pltpu.make_async_remote_copy(src_ref=src, dst_ref=dst, send_sem=send_sem, recv_sem=recv_sem,
                                        device_id={'model': dev}, device_id_type=MESH)


def wait_bytes(ref, sem):
    pltpu.make_async_copy(ref, ref, sem).wait()


def greet(me, n_dev):
    barrier = pltpu.get_barrier_semaphore()
    for off in range(1, n_dev):
        pl.semaphore_signal(barrier, inc=1, device_id={'model': lax.rem(me + off, n_dev)}, device_id_type=MESH)
    pl.semaphore_wait(barrier, n_dev - 1)


def layer_kernel(n_dev, len_ref, x_hbm, wk_hbm, wv_hbm, wq_hbm, wo_hbm, wg_hbm, wu_hbm, wd_hbm, tok_ref, gain_ref, gain2_ref, cos_ref, sin_ref,
                 kout, vout, out_ref,
                 wbuf, wq, wo, wg, wu, wd, xown, xrecv, stage, ktmp, lfull, lrecv, lcols, crow, srow,
                 rows, qtmp, qall, knew, vnew, kself, vself, near, psend, prec, att, part, recv, hid,
                 xcopy_sem, wcopy_sem, wrecv_sem, wsend_sem, xrecv_sem, xsend_sem,
                 kv_recv_sem, kv_send_sem, kv_local_sem, l_send_sem, l_recv_sem, q_sem, p_sem, r_send_sem, r_recv_sem, h_send_sem, h_recv_sem, new_sem):
    n_batch, seq_loc, d_model = xown.shape
    n_chip = n_dev // 2
    half = n_batch // 2
    n_chunk = half // GROUP
    m_rows = GROUP * seq_loc
    seq_len = seq_loc * n_dev
    width = d_model // n_dev
    me = lax.axis_index('model')
    chip, core = me // 2, lax.rem(me, 2)
    left, right = lax.rem(chip + n_chip - 1, n_chip), lax.rem(chip + 1, n_chip)
    partner = chip * 2 + 1 - core
    w_hbm = (wk_hbm, wv_hbm)
    outs = (kout, vout)
    owners = (me, me, left * 2 + core, right * 2 + core)
    firsts = (0, half, 0, half)
    aims = (left, right, right, left)
    slots = (1, 2, 2, 1)

    def col(j):
        return pl.ds(pl.multiple_of(j * width, width), width)

    wlocal = [pltpu.make_async_copy(w_hbm[kv], wbuf.at[0, core, kv], wcopy_sem.at[kv]) for kv in range(2)]
    for cp in wlocal:
        cp.start()

    def xcopy(ch):
        return pltpu.make_async_copy(x_hbm.at[pl.ds(ch * GROUP, GROUP)], xown.at[pl.ds(ch * GROUP, GROUP)], xcopy_sem.at[ch])

    for ch in range(2 * n_chunk):
        xcopy(ch).start()
    later = [pltpu.make_async_copy(src, dst, wcopy_sem.at[2 + i])
             for i, (src, dst) in enumerate(((wq_hbm, wq), (wo_hbm, wo), (wg_hbm, wg), (wu_hbm, wu), (wd_hbm, wd)))]
    for cp in later:
        cp.start()

    greet(me, n_dev)

    wsends = []
    for kv in range(2):
        wsends.append(remote(w_hbm[kv], wbuf.at[1, core, kv], wsend_sem.at[0, kv], wrecv_sem.at[1, core, kv], right * 2 + core))
        wsends.append(remote(w_hbm[kv], wbuf.at[2, core, kv], wsend_sem.at[1, kv], wrecv_sem.at[2, core, kv], left * 2 + core))
        wsends.append(remote(w_hbm[kv], wbuf.at[0, core, kv], wsend_sem.at[2, kv], wrecv_sem.at[0, core, kv], partner))
    for cp in wsends:
        cp.start()

    xsends = []

    def send_rows(ci):
        for side, aim in ((0, right), (1, left)):
            xsends.append(remote(x_hbm.at[pl.ds(side * half + ci * GROUP, GROUP)], xrecv.at[side, pl.ds(ci * GROUP, GROUP)],
                                 xsend_sem.at[side, ci], xrecv_sem.at[side, ci], aim * 2 + core))
            xsends[-1].start()

    def to_peers(src_of, dst, send_sem, recv_sem):
        for off in range(1, n_dev):
            peer = lax.rem(me + off, n_dev)
            remote(src_of(peer), dst, send_sem, recv_sem, peer).start()

    gain = gain_ref[...].astype(F32)

    def normalize(ref):
        for g in range(GROUP):
            ref[g] = rms_rows(ref[g].astype(F32), gain)

    def piece_of(unit, ci, dst, kv):
        start = pl.multiple_of(owners[unit] * seq_loc, seq_loc)
        return (stage.at[unit, dst, kv, pl.ds(ci * GROUP, GROUP)],
                outs[kv].at[pl.ds(firsts[unit] + ci * GROUP, GROUP), pl.ds(start, seq_loc)])

    def make_kv(rows_ref, unit, ci, slot, kcore, dst):
        mat = rows_ref[...].reshape(m_rows, d_model)
        start = pl.multiple_of(owners[unit] * seq_loc, seq_loc)
        cos_t = jnp.concatenate([cos_ref[pl.ds(start, seq_loc), :]] * GROUP, axis=0)
        sin_t = jnp.concatenate([sin_ref[pl.ds(start, seq_loc), :]] * GROUP, axis=0)
        for kv in range(2):
            acc = dot_f32(mat, wbuf[slot, kcore, kv])
            for h in range(2):
                head = acc[:, h * HEAD_DIM:(h + 1) * HEAD_DIM]
                if kv == 0:
                    head = rope_half(head, cos_t, sin_t)
                ktmp[pl.ds(h, m_rows, stride=2), :] = head
            piece, place = piece_of(unit, ci, dst, kv)
            piece.reshape(2 * m_rows, HEAD_DIM)[...] = ktmp[...].astype(BF16)
            if dst == 3:
                pltpu.make_async_copy(piece, place, kv_local_sem.at[kv]).start()
            elif dst == 2:
                remote(piece, place, kv_send_sem, kv_recv_sem.at[kv], partner).start()

    def own_rows(unit, ci):
        return xown.at[pl.ds(firsts[unit] + ci * GROUP, GROUP)]

    waiting = [(units, ci, kcore, kv) for units in ((0, 1), (3, 2)) for ci in range(n_chunk) for kcore in range(2) for kv in range(2)]

    def send_kv(count):
        for _ in range(min(count, len(waiting))):
            units, ci, kcore, kv = waiting.pop(0)
            for unit in units:
                piece, place = piece_of(unit, ci, kcore, kv)
                remote(piece, place, kv_send_sem, kv_recv_sem.at[kv], aims[unit] * 2 + kcore).start()

    for cp in wlocal:
        cp.wait()
    base = me * seq_loc
    for unit in range(2):
        @pl.loop(0, n_chunk)
        def _(ci):
            xcopy(unit * n_chunk + ci).wait()
            for g in range(GROUP):
                b = firsts[unit] + ci * GROUP + g
                hit = lax.broadcasted_iota(jnp.int32, (16, seq_loc), 1) == len_ref[b] - 1 - base
                row = dot_f32(jnp.where(hit, 1.0, 0.0).astype(BF16), xown[b])
                lfull[pl.ds(b, 1), :] = row[0:1]
            normalize(own_rows(unit, ci))
            make_kv(own_rows(unit, ci), unit, ci, 0, core, 3)

    to_peers(lambda peer: lfull.at[:, col(peer)], lrecv.at[me], l_send_sem.at[0], l_recv_sem.at[0])
    lrecv[me] = lfull[:, col(me)]
    for ci in range(n_chunk // 2):
        send_rows(ci)

    for kv in range(2):
        wait_bytes(wbuf.at[0, 1 - core, kv], wrecv_sem.at[0, 1 - core, kv])
    for unit in range(2):
        @pl.loop(0, n_chunk)
        def _(ci):
            make_kv(own_rows(unit, ci), unit, ci, 0, 1 - core, 2)

    far = 1 << 20
    shape = near.shape
    r_idx = lax.broadcasted_iota(jnp.int32, shape, 0)
    c_idx = lax.broadcasted_iota(jnp.int32, shape, 1)
    match = (c_idx // (2 * seq_loc) == lax.rem(r_idx, half)) & (lax.rem(c_idx, 2) == lax.rem(r_idx // half, 2))
    near[...] = jnp.where(match, lax.rem(c_idx // 2, seq_loc), far)

    fwds = []
    for kv in range(2):
        for slot in (1, 2):
            wait_bytes(wbuf.at[slot, core, kv], wrecv_sem.at[slot, core, kv])
            fwds.append(remote(wbuf.at[slot, core, kv], wbuf.at[slot, core, kv], wsend_sem.at[2 + slot, kv],
                               wrecv_sem.at[slot, core, kv], partner))
            fwds[-1].start()
    for slot in (1, 2):
        for kv in range(2):
            wait_bytes(wbuf.at[slot, 1 - core, kv], wrecv_sem.at[slot, 1 - core, kv])

    @pl.loop(0, n_chunk)
    def _(ci):
        for kcore in range(2):
            for unit in range(2):
                make_kv(own_rows(unit, ci), unit, ci, slots[unit], kcore, kcore)

    wait_bytes(lrecv.at[pl.ds(0, n_dev - 1)], l_recv_sem.at[0])
    lcols[me] = jnp.sum(lrecv[...], axis=0).astype(BF16)
    to_peers(lambda peer: lcols.at[me], lcols.at[me], l_send_sem.at[1], l_recv_sem.at[1])
    for ci in range(n_chunk // 2, n_chunk):
        send_rows(ci)

    def received(ci):
        for side in range(2):
            rows_ref = xrecv.at[side, pl.ds(ci * GROUP, GROUP)]
            wait_bytes(rows_ref, xrecv_sem.at[side, ci])
            normalize(rows_ref)
            for kcore in range(2):
                make_kv(rows_ref, 2 + side, ci, slots[2 + side], kcore, kcore)
            make_kv(rows_ref, 2 + side, ci, 0, 1 - core, 2)
            make_kv(rows_ref, 2 + side, ci, 0, core, 3)

    @pl.loop(0, n_chunk // 2)
    def _(ci):
        received(ci)

    wait_bytes(lcols.at[pl.ds(0, n_dev - 1)], l_recv_sem.at[1])
    later[0].wait()
    rows[0:n_batch, :] = tok_ref[...]
    for j in range(n_dev):
        rows[n_batch:2 * n_batch, j * width:(j + 1) * width] = lcols[j]
    for b in range(n_batch):
        for r in range(2):
            at = jnp.maximum(len_ref[b] - r, 0)
            crow[pl.ds(r * n_batch + b, 1), :] = cos_ref[pl.ds(at, 1), :]
            srow[pl.ds(r * n_batch + b, 1), :] = sin_ref[pl.ds(at, 1), :]
    rows_n = rms_rows(rows[...].astype(F32), gain)
    q_acc = dot_f32(rows_n, wq[...])
    for h in range(2):
        head = rope_half(q_acc[:, h * HEAD_DIM:(h + 1) * HEAD_DIM], crow[...], srow[...])
        for r in range(2):
            for s in range(2):
                qtmp[pl.ds(((s * 2 + r) * 2 + h) * half, half), :] = head[r * n_batch + s * half:r * n_batch + (s + 1) * half]
    qall[me] = qtmp[...].astype(BF16)
    to_peers(lambda peer: qall.at[me], qall.at[me], q_sem.at[0], q_sem.at[1])
    send_kv(6)
    kself[...] = jnp.zeros_like(kself)
    vself[...] = jnp.zeros_like(vself)
    news = []
    for kv, (new, own) in enumerate(((knew, kself), (vnew, vself))):
        acc = dot_f32(rows_n[0:n_batch], wbuf[0, core, kv])
        for h in range(2):
            head = acc[:, h * HEAD_DIM:(h + 1) * HEAD_DIM]
            if kv == 0:
                head = rope_half(head, crow[0:n_batch, :], srow[0:n_batch, :])
            ktmp[pl.ds(h, n_batch, stride=2), :] = head
            head = head.astype(BF16).astype(F32)
            for s in range(2):
                own[pl.ds((s * 4 + h) * half, half), :] = head[s * half:(s + 1) * half]
        new.reshape(2 * n_batch, HEAD_DIM)[...] = ktmp[0:2 * n_batch, :].astype(BF16)
        news.append(pltpu.make_async_copy(new, outs[kv].at[pl.ds(0, n_batch), seq_len], new_sem.at[kv]))
        news[-1].start()

    @pl.loop(n_chunk // 2, n_chunk)
    def _(ci):
        received(ci)

    wait_bytes(qall.at[pl.ds(0, n_dev - 1)], q_sem.at[1])
    n_q = 4 * half
    scale = HEAD_DIM ** -0.5
    lane = lax.broadcasted_iota(jnp.int32, (n_q, HEAD_DIM), 1)
    q_row = lax.broadcasted_iota(jnp.int32, (n_q, 1), 0)
    q_len = []
    for s in range(2):
        vec = jnp.zeros((n_q, 1), jnp.int32)
        for b in range(half):
            vec = jnp.where(lax.rem(q_row, half) == b, len_ref[s * half + b], vec)
        q_len.append(vec)

    def partial_att(unit, dst):
        s = unit % 2
        target = (aims[unit] * 2, aims[unit] * 2 + 1, partner, me)[dst]
        q32 = qall[target, s * n_q:(s + 1) * n_q, :]
        keys = stage.at[unit, dst, 0].reshape(2 * half * seq_loc, HEAD_DIM)[...]
        vals = stage.at[unit, dst, 1].reshape(2 * half * seq_loc, HEAD_DIM)[...]
        scores = lax.dot_general(q32, keys, (((1,), (1,)), ((), ())), preferred_element_type=F32) * scale
        scores = jnp.where(near[...] < q_len[s] - owners[unit] * seq_loc, scores, NEG_BIG)
        top = jnp.max(scores, axis=1, keepdims=True)
        prob = jnp.exp(scores - top)
        total = jnp.sum(prob, axis=1, keepdims=True)
        acc = dot_f32(prob.astype(BF16), vals)
        dest = prec.at[3, unit] if dst == 3 else psend.at[dst, unit]
        dest[0] = acc
        dest[1] = jnp.where(lane < HEAD_DIM // 2, top, total)
        if dst == 2:
            remote(psend.at[dst, unit], prec.at[2, unit], p_sem.at[0], p_sem.at[1], partner).start()
        elif dst < 2:
            remote(psend.at[dst, unit], prec.at[core, unit], p_sem.at[0], p_sem.at[1], target).start()

    for dst in range(4):
        for unit in range(4):
            partial_att(unit, dst)
        send_kv(2)

    wait_bytes(prec.at[pl.ds(0, 3)], p_sem.at[1])
    for s in range(2):
        q32 = qall[me, s * n_q:(s + 1) * n_q, :].astype(F32)
        is_new = q_row < n_q // 2
        self_score = jnp.sum(q32 * kself[s * n_q:(s + 1) * n_q, :], axis=1, keepdims=True) * scale
        tops = [jnp.where(is_new, self_score, NEG_BIG)]
        sums = [jnp.where(is_new, 1.0, 0.0)]
        accs = [vself[s * n_q:(s + 1) * n_q, :]]
        for unit in (s, s + 2):
            for src in range(4):
                stat = prec[src, unit, 1]
                tops.append(stat[:, 0:1])
                sums.append(stat[:, HEAD_DIM // 2:HEAD_DIM // 2 + 1])
                accs.append(prec[src, unit, 0])
        top = functools.reduce(jnp.maximum, tops)
        facs = [jnp.exp(t - top) for t in tops]
        total = sum(f * l for f, l in zip(facs, sums))
        merged = sum(f * a for f, a in zip(facs, accs)) / total
        for r in range(2):
            for h in range(2):
                att[r * n_batch + s * half:r * n_batch + (s + 1) * half, h * HEAD_DIM:(h + 1) * HEAD_DIM] = \
                    merged[(r * 2 + h) * half:(r * 2 + h + 1) * half]

    def add_partials(step, lot):
        to_peers(lambda peer: part.at[step, :, col(peer)], recv.at[step, me], r_send_sem.at[step], r_recv_sem.at[step])
        send_kv(lot)
        recv[step, me] = part[step, :, col(me)]
        mine = rows[:, col(me)].astype(F32)
        wait_bytes(recv.at[step, pl.ds(0, n_dev - 1)], r_recv_sem.at[step])
        hid[step, me] = (mine + jnp.sum(recv[step], axis=0)).astype(BF16)
        to_peers(lambda peer: hid.at[step, me], hid.at[step, me], h_send_sem.at[step], h_recv_sem.at[step])
        send_kv(lot)
        wait_bytes(hid.at[step, pl.ds(0, n_dev - 1)], h_recv_sem.at[step])

    later[1].wait()
    part[0] = dot_f32(att[...].astype(BF16), wo[...])
    add_partials(0, 4)
    for j in range(n_dev):
        rows[:, j * width:(j + 1) * width] = hid[0, j]
    for cp in later[2:]:
        cp.wait()
    rows_n = rms_rows(rows[...].astype(F32), gain2_ref[...].astype(F32))
    gate = dot_f32(rows_n, wg[...])
    mid = (gate * (1.0 / (1.0 + jnp.exp(-gate))) * dot_f32(rows_n, wu[...])).astype(BF16)
    part[1] = dot_f32(mid, wd[...])
    add_partials(1, 5)
    for j in range(n_dev):
        out_ref[:, j * width:(j + 1) * width] = hid[1, j]
    send_kv(len(waiting))

    quarter = n_batch // 4
    for kv in range(2):
        news[kv].wait()
        wait_bytes(outs[kv].at[pl.ds(0, quarter), pl.ds(0, seq_len)], kv_local_sem.at[kv])
        wait_bytes(outs[kv].at[pl.ds(0, 3 * quarter), pl.ds(0, seq_len)], kv_recv_sem.at[kv])
    for cp in wsends + fwds + xsends:
        cp.wait_send()
    wait_bytes(lrecv.at[pl.ds(0, n_dev - 1)], l_send_sem.at[0])
    wait_bytes(lcols.at[pl.ds(0, n_dev - 1)], l_send_sem.at[1])
    wait_bytes(qall.at[pl.ds(0, n_dev - 1)], q_sem.at[0])
    wait_bytes(psend, p_sem.at[0])
    for step in range(2):
        wait_bytes(recv.at[step, pl.ds(0, n_dev - 1)], r_send_sem.at[step])
        wait_bytes(hid.at[step, pl.ds(0, n_dev - 1)], h_send_sem.at[step])
    wait_bytes(stage.at[:, pl.ds(0, 3)], kv_send_sem)


def rotary_tables(n_pos):
    inv_freq = np.float32(10000.0) ** (-2.0 * np.arange(HEAD_DIM // 2, dtype=np.float32) / HEAD_DIM).astype(np.float32)
    angles = np.arange(n_pos, dtype=np.float32)[:, None] * inv_freq.astype(np.float32)
    cos, sin = np.cos(angles), np.sin(angles)
    return (np.concatenate([cos, cos], axis=1).astype(np.float32), np.concatenate([-sin, sin], axis=1).astype(np.float32))


def solution(mesh):
    n_dev = mesh.shape['model']
    seq_spec = P('replica', 'model', None)
    col_spec = P(None, None, 'model')
    row_spec = P(None, 'model', None)
    gain_spec = P(None, None)
    tok_spec = P('replica', None)
    cache_spec = P(None, 'replica', None, 'model', None)
    in_specs = (seq_spec, P('replica'), tok_spec, gain_spec, col_spec, col_spec, col_spec, row_spec, gain_spec, col_spec, col_spec, row_spec)
    out_specs = (tok_spec, tok_spec, cache_spec, cache_spec)
    hbm = pl.BlockSpec(memory_space=pl.ANY)
    vmem = pl.BlockSpec(memory_space=pltpu.VMEM)
    smem = pl.BlockSpec(memory_space=pltpu.SMEM)
    dma = pltpu.SemaphoreType.DMA

    def per_device(prompt, lengths, new_tok, norm_attn, w_q, w_k, w_v, w_o, norm_mlp, w_gate, w_up, w_down):
        n_batch, seq_loc, d_model = prompt.shape
        kv_width = w_k.shape[2]
        heads = kv_width // HEAD_DIM
        seq_len = seq_loc * n_dev
        half = n_batch // 2
        n_chunk = half // GROUP
        width = d_model // n_dev
        wq, wk, wv, wo, wg, wu, wd = w_q[0], w_k[0], w_v[0], w_o[0], w_gate[0], w_up[0], w_down[0]
        cos_tab, sin_tab = (jnp.asarray(t) for t in rotary_tables(seq_len + 8))

        ff = wg.shape[1]
        n_q = 4 * half
        cache = jax.ShapeDtypeStruct((n_batch, seq_len + 1, heads, HEAD_DIM), BF16)
        scratch = lambda *shape, dtype=F32: pltpu.VMEM(shape, dtype)
        key_cache, val_cache, out = pl.pallas_call(
            functools.partial(layer_kernel, n_dev),
            out_shape=(cache, cache, jax.ShapeDtypeStruct((2 * n_batch, d_model), BF16)),
            in_specs=[smem] + [hbm] * 8 + [vmem] * 5,
            out_specs=(hbm, hbm, vmem),
            scratch_shapes=[
                scratch(3, 2, 2, d_model, kv_width, dtype=BF16),
                scratch(d_model, kv_width, dtype=BF16),
                scratch(kv_width, d_model, dtype=BF16),
                scratch(d_model, ff, dtype=BF16), scratch(d_model, ff, dtype=BF16), scratch(ff, d_model, dtype=BF16),
                scratch(n_batch, seq_loc, d_model, dtype=BF16),
                scratch(2, half, seq_loc, d_model, dtype=BF16),
                scratch(4, 4, 2, half, seq_loc, heads, HEAD_DIM, dtype=BF16),
                scratch(2 * GROUP * seq_loc, HEAD_DIM),
                scratch(n_batch, d_model), scratch(n_dev, n_batch, width), scratch(n_dev, n_batch, width, dtype=BF16),
                scratch(2 * n_batch, HEAD_DIM), scratch(2 * n_batch, HEAD_DIM),
                scratch(2 * n_batch, d_model, dtype=BF16),
                scratch(2 * n_q, HEAD_DIM), scratch(n_dev, 2 * n_q, HEAD_DIM, dtype=BF16),
                scratch(n_batch, heads, HEAD_DIM, dtype=BF16), scratch(n_batch, heads, HEAD_DIM, dtype=BF16),
                scratch(2 * n_q, HEAD_DIM), scratch(2 * n_q, HEAD_DIM),
                scratch(n_q, 2 * half * seq_loc, dtype=jnp.int32),
                scratch(3, 4, 2, n_q, HEAD_DIM), scratch(4, 4, 2, n_q, HEAD_DIM),
                scratch(2 * n_batch, kv_width),
                scratch(2, 2 * n_batch, d_model), scratch(2, n_dev, 2 * n_batch, width),
                scratch(2, n_dev, 2 * n_batch, width, dtype=BF16),
                dma((2 * n_chunk,)), dma((7,)), dma((3, 2, 2)), dma((5, 2)), dma((2, n_chunk)), dma((2, n_chunk)),
                dma((2,)), dma(()), dma((2,)), dma((2,)), dma((2,)), dma((2,)), dma((2,)),
                dma((2,)), dma((2,)), dma((2,)), dma((2,)), dma((2,)),
            ],
            compiler_params=pltpu.CompilerParams(collective_id=0, has_side_effects=True, vmem_limit_bytes=63 * 2 ** 20),
            name='layer',
        )(lengths, prompt, wk, wv, wq, wo, wg, wu, wd, new_tok, norm_attn, norm_mlp, cos_tab, sin_tab)
        return out[:n_batch], out[n_batch:], key_cache[None], val_cache[None]

    return jax.shard_map(per_device, mesh=mesh, in_specs=in_specs, out_specs=out_specs, check_vma=False)
```

```python
import functools

import numpy as np

import jax
import jax.numpy as jnp
from jax import lax
from jax.experimental import pallas as pl
from jax.experimental.pallas import tpu as pltpu
from jax.sharding import PartitionSpec as P

HEAD_DIM = 128
NEG_BIG = -1e30
MESH = pl.DeviceIdType.MESH
GROUP = 2
LOTS = (5, 1, 2)
F32 = jnp.float32
BF16 = jnp.bfloat16


def dot_f32(lhs, rhs):
    return jnp.dot(lhs, rhs, preferred_element_type=F32)


def rms_rows(rows_f32, gain_f32):
    inv_rms = lax.rsqrt(jnp.mean(rows_f32 * rows_f32, axis=-1, keepdims=True) + 1e-5)
    return (rows_f32 * inv_rms * gain_f32).astype(BF16)


def rope_half(head_f32, cos_t, sin_t):
    return head_f32 * cos_t + pltpu.roll(head_f32, HEAD_DIM // 2, 1) * sin_t


def remote(src, dst, send_sem, recv_sem, dev):
    return pltpu.make_async_remote_copy(src_ref=src, dst_ref=dst, send_sem=send_sem, recv_sem=recv_sem,
                                        device_id={'model': dev}, device_id_type=MESH)


def wait_bytes(ref, sem):
    pltpu.make_async_copy(ref, ref, sem).wait()


def layer_kernel(n_dev, n_rep, len_ref, x_hbm, wk_hbm, wv_hbm, wq_hbm, wo_hbm, wg_hbm, wu_hbm, wd_hbm, tok_ref, gain_ref, gain2_ref, cos_ref, sin_ref,
                 kout, vout, dec_out, last_out,
                 wbuf, wq, wo, wg, wu, wd, xown, xrecv, stage, ktmp, lfull, lgot, lpair, lrecv, lcols, crow, srow,
                 rows, qtmp, qall, knew, vnew, kself, vself, near, psend, prec, att, part, got, pair, recv, hid,
                 xcopy_sem, wcopy_sem, wrecv_sem, wsend_sem, wown_sem, wfwd_sem, ysend_sem, yrecv_sem, xrecv_sem, xsend_sem,
                 kv_recv_sem, kv_send_sem, kv_local_sem, p_sem, new_sem, sum_sem, all_sem):
    n_batch, seq_loc, d_model = xown.shape
    n_chip = n_dev // 2
    half = n_batch // 2
    n_chunk = half // GROUP
    m_rows = GROUP * seq_loc
    seq_len = seq_loc * n_dev
    width = d_model // n_dev
    me = lax.axis_index('model')
    rep = lax.axis_index('replica')
    chip, core = me // 2, lax.rem(me, 2)
    left, right = lax.rem(chip + n_chip - 1, n_chip), lax.rem(chip + 1, n_chip)
    partner = chip * 2 + 1 - core
    w_hbm = (wk_hbm, wv_hbm)
    outs = (kout, vout)
    owners = (me, me, left * 2 + core, right * 2 + core)
    firsts = (0, half, 0, half)
    aims = (left, right, right, left)
    slots = (1, 2, 2, 1)

    def col(j):
        return pl.ds(pl.multiple_of(j * width, width), width)

    wlocal = [pltpu.make_async_copy(w_hbm[kv], wbuf.at[0, core, kv], wcopy_sem.at[kv]) for kv in range(2)]
    for cp in wlocal:
        cp.start()

    def xcopy(ch):
        return pltpu.make_async_copy(x_hbm.at[pl.ds(ch * GROUP, GROUP)], xown.at[pl.ds(ch * GROUP, GROUP)], xcopy_sem.at[ch])

    for ch in range(2 * n_chunk):
        xcopy(ch).start()
    later = [pltpu.make_async_copy(src, dst, wcopy_sem.at[2 + i])
             for i, (src, dst) in enumerate(((wq_hbm, wq), (wo_hbm, wo), (wg_hbm, wg), (wu_hbm, wu), (wd_hbm, wd)))]
    for cp in later:
        cp.start()

    barrier = pltpu.get_barrier_semaphore()
    for off in range(1, n_dev):
        pl.semaphore_signal(barrier, inc=1, device_id={'model': lax.rem(me + off, n_dev)}, device_id_type=MESH)

    @pl.loop(1, n_rep)
    def _(off):
        pl.semaphore_signal(barrier, inc=1, device_id={'replica': lax.rem(rep + off, n_rep)}, device_id_type=MESH)

    pl.semaphore_wait(barrier, n_dev + n_rep - 2)

    n_sub = 2
    slice_rows = d_model // n_rep
    sub_rows = slice_rows // n_sub

    def w_slice(h):
        return pl.ds(pl.multiple_of(rep * slice_rows + h * sub_rows, sub_rows), sub_rows)

    wsends = []
    for kv in range(2):
        for h in range(n_sub):
            for slot, aim in ((1, right), (2, left)):
                wsends.append(remote(w_hbm[kv].at[w_slice(h)], wbuf.at[slot, core, kv, w_slice(h)],
                                     wsend_sem.at[slot - 1, kv, h], wrecv_sem.at[slot - 1, kv, h], aim * 2 + core))
        wsends.append(remote(w_hbm[kv], wbuf.at[0, core, kv], wown_sem.at[0, kv], wown_sem.at[1, kv], partner))
    for cp in wsends:
        cp.start()

    def pass_on(kv, h):
        for slot in (1, 2):
            block = wbuf.at[slot, core, kv, w_slice(h)]
            wait_bytes(block, wrecv_sem.at[slot - 1, kv, h])

            @pl.loop(1, n_rep)
            def _(off):
                pltpu.make_async_remote_copy(src_ref=block, dst_ref=block, send_sem=ysend_sem, recv_sem=yrecv_sem.at[slot - 1, kv],
                                             device_id={'replica': lax.rem(rep + off, n_rep)}, device_id_type=MESH).start()

    xsends = []

    def send_rows(ci):
        for side, aim in ((0, right), (1, left)):
            xsends.append(remote(x_hbm.at[pl.ds(side * half + ci * GROUP, GROUP)], xrecv.at[side, pl.ds(ci * GROUP, GROUP)],
                                 xsend_sem.at[side, ci], xrecv_sem.at[side, ci], aim * 2 + core))
            xsends[-1].start()

    def other_chips():
        return [lax.rem(chip + off, n_chip) for off in range(1, n_chip)]

    def sum_pair(index, full, got_ref):
        for c in range(n_chip):
            remote(full.at[:, col(c * 2 + 1 - core)], got_ref.at[c], sum_sem.at[index, 0], sum_sem.at[index, 1], partner).start()

    def sum_chips(index, full, got_ref, pair_ref, recv_ref):
        wait_bytes(got_ref, sum_sem.at[index, 1])
        for c in range(n_chip):
            pair_ref[c] = full[:, col(c * 2 + core)] + got_ref[c]
        for c in other_chips():
            remote(pair_ref.at[c], recv_ref.at[chip], sum_sem.at[index, 2], sum_sem.at[index, 3], c * 2 + core).start()
        recv_ref[chip] = pair_ref[chip]

    def sum_end(index, recv_ref):
        wait_bytes(recv_ref.at[pl.ds(0, n_chip - 1)], sum_sem.at[index, 3])
        return jnp.sum(recv_ref[...], axis=0)

    def gather(index, buf):
        for c in other_chips():
            remote(buf.at[me], buf.at[me], all_sem.at[index, 0], all_sem.at[index, 1], c * 2 + core).start()
        remote(buf.at[me], buf.at[me], all_sem.at[index, 2], all_sem.at[index, 3], partner).start()

    def gather_pass(index, buf):
        wait_bytes(buf.at[pl.ds(0, n_chip - 1)], all_sem.at[index, 1])
        for c in other_chips():
            remote(buf.at[c * 2 + core], buf.at[c * 2 + core], all_sem.at[index, 2], all_sem.at[index, 3], partner).start()

    def gather_end(index, buf):
        wait_bytes(buf.at[pl.ds(0, n_chip)], all_sem.at[index, 3])

    gain = gain_ref[...].astype(F32)

    def normalize(ref):
        for g in range(GROUP):
            ref[g] = rms_rows(ref[g].astype(F32), gain)

    def make_kv(rows_ref, unit, ci, owner, b0, slot, kcore, dst):
        mat = rows_ref[...].reshape(m_rows, d_model)
        start = pl.multiple_of(owner * seq_loc, seq_loc)
        cos_t = jnp.concatenate([cos_ref[pl.ds(start, seq_loc), :]] * GROUP, axis=0)
        sin_t = jnp.concatenate([sin_ref[pl.ds(start, seq_loc), :]] * GROUP, axis=0)
        for kv in range(2):
            acc = dot_f32(mat, wbuf[slot, kcore, kv])
            for h in range(2):
                head = acc[:, h * HEAD_DIM:(h + 1) * HEAD_DIM]
                if kv == 0:
                    head = rope_half(head, cos_t, sin_t)
                ktmp[pl.ds(h, m_rows, stride=2), :] = head
            piece = stage.at[unit, dst, kv, pl.ds(ci * GROUP, GROUP)]
            piece.reshape(2 * m_rows, HEAD_DIM)[...] = ktmp[...].astype(BF16)
            place = outs[kv].at[pl.ds(b0, GROUP), pl.ds(start, seq_loc)]
            if slot == 0 and dst == 3:
                pltpu.make_async_copy(piece, place, kv_local_sem.at[kv]).start()
            elif slot == 0:
                remote(piece, place, kv_send_sem, kv_recv_sem.at[kv], partner).start()

    waiting = [(units, ci, kcore, kv) for units in ((0, 1), (3, 2)) for ci in range(n_chunk) for kcore in range(2) for kv in range(2)]

    def send_kv(count):
        for _ in range(min(count, len(waiting))):
            units, ci, kcore, kv = waiting.pop(0)
            for unit in units:
                start = pl.multiple_of(owners[unit] * seq_loc, seq_loc)
                remote(stage.at[unit, kcore, kv, pl.ds(ci * GROUP, GROUP)],
                       outs[kv].at[pl.ds(firsts[unit] + ci * GROUP, GROUP), pl.ds(start, seq_loc)],
                       kv_send_sem, kv_recv_sem.at[kv], aims[unit] * 2 + kcore).start()

    for cp in wlocal:
        cp.wait()
    base = me * seq_loc

    @pl.loop(0, 2 * n_chunk)
    def _(ch):
        xcopy(ch).wait()
        own = xown.at[pl.ds(ch * GROUP, GROUP)]
        for g in range(GROUP):
            b = ch * GROUP + g
            hit = lax.broadcasted_iota(jnp.int32, (16, seq_loc), 1) == len_ref[b] - 1 - base
            row = dot_f32(jnp.where(hit, 1.0, 0.0).astype(BF16), xown[b])
            lfull[pl.ds(b, 1), :] = row[0:1]
        normalize(own)
        make_kv(own, ch // n_chunk, lax.rem(ch, n_chunk), me, ch * GROUP, 0, core, 3)

    pass_on(0, 0)
    sum_pair(0, lfull, lgot)
    for kv in range(2):
        wait_bytes(wbuf.at[0, 1 - core, kv], wown_sem.at[1, kv])

    @pl.loop(0, 2 * n_chunk)
    def _(ch):
        make_kv(xown.at[pl.ds(ch * GROUP, GROUP)], ch // n_chunk, lax.rem(ch, n_chunk), me, ch * GROUP, 0, 1 - core, 2)

        @pl.when(ch == n_chunk - 1)
        def _():
            pass_on(0, 1)
            sum_chips(0, lfull, lgot, lpair, lrecv)

    send_rows(0)
    pass_on(1, 0)

    far = 1 << 20
    r_idx = lax.broadcasted_iota(jnp.int32, near.shape, 0)
    c_idx = lax.broadcasted_iota(jnp.int32, near.shape, 1)
    match = (c_idx // (2 * seq_loc) == lax.rem(r_idx, half)) & (lax.rem(c_idx, 2) == lax.rem(r_idx // half, 2))
    near[...] = jnp.where(match, lax.rem(c_idx // 2, seq_loc), far)

    pass_on(1, 1)
    lcols[me] = sum_end(0, lrecv).astype(BF16)
    gather(0, lcols)
    send_rows(1)

    rows[0:n_batch, :] = tok_ref[...]
    for b in range(n_batch):
        for r in range(2):
            at = jnp.maximum(len_ref[b] - r, 0)
            crow[pl.ds(r * n_batch + b, 1), :] = cos_ref[pl.ds(at, 1), :]
            srow[pl.ds(r * n_batch + b, 1), :] = sin_ref[pl.ds(at, 1), :]
    later[0].wait()
    gather_pass(0, lcols)
    gather_end(0, lcols)
    for j in range(n_dev):
        rows[n_batch:2 * n_batch, j * width:(j + 1) * width] = lcols[j]
    rows_n = rms_rows(rows[...].astype(F32), gain)
    q_acc = dot_f32(rows_n, wq[...])
    for h in range(2):
        head = rope_half(q_acc[:, h * HEAD_DIM:(h + 1) * HEAD_DIM], crow[...], srow[...])
        for r in range(2):
            for s in range(2):
                qtmp[pl.ds(((s * 2 + r) * 2 + h) * half, half), :] = head[r * n_batch + s * half:r * n_batch + (s + 1) * half]
    qall[me] = qtmp[...].astype(BF16)
    gather(1, qall)
    for ci in range(2, n_chunk):
        send_rows(ci)
    kself[...] = jnp.zeros_like(kself)
    vself[...] = jnp.zeros_like(vself)
    news = []
    for kv, (new, own) in enumerate(((knew, kself), (vnew, vself))):
        acc = dot_f32(rows_n[0:n_batch], wbuf[0, core, kv])
        for h in range(2):
            head = acc[:, h * HEAD_DIM:(h + 1) * HEAD_DIM]
            if kv == 0:
                head = rope_half(head, crow[0:n_batch, :], srow[0:n_batch, :])
            ktmp[pl.ds(h, n_batch, stride=2), :] = head
            head = head.astype(BF16).astype(F32)
            for s in range(2):
                own[pl.ds((s * 4 + h) * half, half), :] = head[s * half:(s + 1) * half]
        new.reshape(2 * n_batch, HEAD_DIM)[...] = ktmp[0:2 * n_batch, :].astype(BF16)
        news.append(pltpu.make_async_copy(new, outs[kv].at[pl.ds(0, n_batch), seq_len], new_sem.at[kv]))
        news[-1].start()

    fwds = []
    for kv in range(2):
        for slot in (1, 2):
            if n_rep > 1:
                wait_bytes(wbuf.at[slot, core, kv, pl.ds(0, d_model - slice_rows)], yrecv_sem.at[slot - 1, kv])
            fwds.append(remote(wbuf.at[slot, core, kv], wbuf.at[slot, core, kv], wfwd_sem.at[0, slot - 1, kv], wfwd_sem.at[1, slot - 1, kv], partner))
            fwds[-1].start()
    for kv in range(2):
        for slot in (1, 2):
            wait_bytes(wbuf.at[slot, 1 - core, kv], wfwd_sem.at[1, slot - 1, kv])

    @pl.loop(0, n_chunk)
    def _(ci):
        @pl.loop(0, 2)
        def _(kcore):
            for unit in range(2):
                make_kv(xown.at[pl.ds(firsts[unit] + ci * GROUP, GROUP)], unit, ci, me, firsts[unit] + ci * GROUP, slots[unit], kcore, kcore)

    gather_pass(1, qall)
    send_kv(LOTS[0])

    @pl.loop(0, n_chunk)
    def _(ci):
        for side in range(2):
            unit = 2 + side
            rows_ref = xrecv.at[side, pl.ds(ci * GROUP, GROUP)]
            b0 = firsts[unit] + ci * GROUP
            wait_bytes(rows_ref, xrecv_sem.at[side, ci])
            normalize(rows_ref)

            @pl.loop(0, 2)
            def _(kcore):
                make_kv(rows_ref, unit, ci, owners[unit], b0, slots[unit], kcore, kcore)

            make_kv(rows_ref, unit, ci, owners[unit], b0, 0, 1 - core, 2)
            make_kv(rows_ref, unit, ci, owners[unit], b0, 0, core, 3)

    gather_end(1, qall)
    n_q = 4 * half
    scale = HEAD_DIM ** -0.5
    lane = lax.broadcasted_iota(jnp.int32, (n_q, HEAD_DIM), 1)
    q_row = lax.broadcasted_iota(jnp.int32, (n_q, 1), 0)
    q_len = []
    for s in range(2):
        vec = jnp.zeros((n_q, 1), jnp.int32)
        for b in range(half):
            vec = jnp.where(lax.rem(q_row, half) == b, len_ref[s * half + b], vec)
        q_len.append(vec)

    def partial_att(unit, dst):
        s = unit % 2
        target = (aims[unit] * 2, aims[unit] * 2 + 1, partner, me)[dst]
        q32 = qall[target, s * n_q:(s + 1) * n_q, :]
        keys = stage.at[unit, dst, 0].reshape(2 * half * seq_loc, HEAD_DIM)[...]
        vals = stage.at[unit, dst, 1].reshape(2 * half * seq_loc, HEAD_DIM)[...]
        scores = lax.dot_general(q32, keys, (((1,), (1,)), ((), ())), preferred_element_type=F32) * scale
        scores = jnp.where(near[...] < q_len[s] - owners[unit] * seq_loc, scores, NEG_BIG)
        top = jnp.max(scores, axis=1, keepdims=True)
        prob = jnp.exp(scores - top)
        total = jnp.sum(prob, axis=1, keepdims=True)
        acc = dot_f32(prob.astype(BF16), vals)
        dest = prec.at[3, unit] if dst == 3 else psend.at[dst, unit]
        dest[0] = acc
        dest[1] = jnp.where(lane < HEAD_DIM // 2, top, total)
        if dst == 2:
            remote(psend.at[dst, unit], prec.at[2, unit], p_sem.at[0], p_sem.at[1], partner).start()
        elif dst < 2:
            remote(psend.at[dst, unit], prec.at[core, unit], p_sem.at[0], p_sem.at[1], target).start()

    for dst in range(4):
        for unit in range(4):
            partial_att(unit, dst)
        send_kv(LOTS[1])

    wait_bytes(prec.at[pl.ds(0, 3)], p_sem.at[1])
    for s in range(2):
        q32 = qall[me, s * n_q:(s + 1) * n_q, :].astype(F32)
        is_new = q_row < n_q // 2
        self_score = jnp.sum(q32 * kself[s * n_q:(s + 1) * n_q, :], axis=1, keepdims=True) * scale
        tops = [jnp.where(is_new, self_score, NEG_BIG)]
        sums = [jnp.where(is_new, 1.0, 0.0)]
        accs = [vself[s * n_q:(s + 1) * n_q, :]]
        for unit in (s, s + 2):
            for src in range(4):
                stat = prec[src, unit, 1]
                tops.append(stat[:, 0:1])
                sums.append(stat[:, HEAD_DIM // 2:HEAD_DIM // 2 + 1])
                accs.append(prec[src, unit, 0])
        top = functools.reduce(jnp.maximum, tops)
        facs = [jnp.exp(t - top) for t in tops]
        total = sum(f * l for f, l in zip(facs, sums))
        merged = sum(f * a for f, a in zip(facs, accs)) / total
        for r in range(2):
            for h in range(2):
                att[r * n_batch + s * half:r * n_batch + (s + 1) * half, h * HEAD_DIM:(h + 1) * HEAD_DIM] = \
                    merged[(r * 2 + h) * half:(r * 2 + h + 1) * half]

    def add_partials(step):
        sum_pair(1 + step, part.at[step], got.at[step])
        sum_chips(1 + step, part.at[step], got.at[step], pair.at[step], recv.at[step])
        send_kv(LOTS[2])
        mine = rows[:, col(me)].astype(F32)
        hid[step, me] = (mine + sum_end(1 + step, recv.at[step])).astype(BF16)
        gather(2 + step, hid.at[step])
        send_kv(LOTS[2])
        gather_pass(2 + step, hid.at[step])
        gather_end(2 + step, hid.at[step])

    later[1].wait()
    part[0] = dot_f32(att[...].astype(BF16), wo[...])
    add_partials(0)
    for j in range(n_dev):
        rows[:, j * width:(j + 1) * width] = hid[0, j]
    for cp in later[2:]:
        cp.wait()
    rows_n = rms_rows(rows[...].astype(F32), gain2_ref[...].astype(F32))
    gate = dot_f32(rows_n, wg[...])
    mid = (gate * (1.0 / (1.0 + jnp.exp(-gate))) * dot_f32(rows_n, wu[...])).astype(BF16)
    part[1] = dot_f32(mid, wd[...])
    add_partials(1)
    send_kv(len(waiting))
    for j in range(n_dev):
        dec_out[:, j * width:(j + 1) * width] = hid[1, j, 0:n_batch, :]
        last_out[:, j * width:(j + 1) * width] = hid[1, j, n_batch:2 * n_batch, :]

    for cp in wsends + fwds + xsends:
        cp.wait_send()
    if n_rep > 1:
        for slot in (1, 2):
            wait_bytes(wbuf.at[slot, 0, :, pl.ds(0, d_model - slice_rows)], ysend_sem)
    wait_bytes(psend, p_sem.at[0])
    for index, (got_ref, recv_ref) in enumerate(((lgot, lrecv), (got.at[0], recv.at[0]), (got.at[1], recv.at[1]))):
        wait_bytes(got_ref, sum_sem.at[index, 0])
        wait_bytes(recv_ref.at[pl.ds(0, n_chip - 1)], sum_sem.at[index, 2])
    for index, buf in enumerate((lcols, qall, hid.at[0], hid.at[1])):
        wait_bytes(buf.at[pl.ds(0, n_chip - 1)], all_sem.at[index, 0])
        wait_bytes(buf.at[pl.ds(0, n_chip)], all_sem.at[index, 2])
    quarter = n_batch // 4
    for kv in range(2):
        news[kv].wait()
        wait_bytes(outs[kv].at[pl.ds(0, quarter), pl.ds(0, seq_len)], kv_local_sem.at[kv])
        wait_bytes(outs[kv].at[pl.ds(0, 3 * quarter), pl.ds(0, seq_len)], kv_recv_sem.at[kv])
    wait_bytes(stage.at[:, pl.ds(0, 3)], kv_send_sem)


def rotary_tables(n_pos):
    inv_freq = np.float32(10000.0) ** (-2.0 * np.arange(HEAD_DIM // 2, dtype=np.float32) / HEAD_DIM).astype(np.float32)
    angles = np.arange(n_pos, dtype=np.float32)[:, None] * inv_freq.astype(np.float32)
    cos, sin = np.cos(angles), np.sin(angles)
    return (np.concatenate([cos, cos], axis=1).astype(np.float32), np.concatenate([-sin, sin], axis=1).astype(np.float32))


def solution(mesh):
    n_dev, n_rep = mesh.shape['model'], mesh.shape['replica']
    seq_spec = P('replica', 'model', None)
    col_spec = P(None, None, 'model')
    row_spec = P(None, 'model', None)
    gain_spec = P(None, None)
    tok_spec = P('replica', None)
    cache_spec = P(None, 'replica', None, 'model', None)
    in_specs = (seq_spec, P('replica'), tok_spec, gain_spec, col_spec, col_spec, col_spec, row_spec, gain_spec, col_spec, col_spec, row_spec)
    out_specs = (tok_spec, tok_spec, cache_spec, cache_spec)
    hbm = pl.BlockSpec(memory_space=pl.ANY)
    vmem = pl.BlockSpec(memory_space=pltpu.VMEM)
    smem = pl.BlockSpec(memory_space=pltpu.SMEM)
    dma = pltpu.SemaphoreType.DMA

    def per_device(prompt, lengths, new_tok, norm_attn, w_q, w_k, w_v, w_o, norm_mlp, w_gate, w_up, w_down):
        n_batch, seq_loc, d_model = prompt.shape
        kv_width = w_k.shape[2]
        heads = kv_width // HEAD_DIM
        seq_len = seq_loc * n_dev
        half = n_batch // 2
        n_chunk = half // GROUP
        width = d_model // n_dev
        wq, wk, wv, wo, wg, wu, wd = w_q[0], w_k[0], w_v[0], w_o[0], w_gate[0], w_up[0], w_down[0]
        cos_tab, sin_tab = (jnp.asarray(t) for t in rotary_tables(seq_len + 8))

        ff = wg.shape[1]
        n_q = 4 * half
        cache = jax.ShapeDtypeStruct((n_batch, seq_len + 1, heads, HEAD_DIM), BF16)
        scratch = lambda *shape, dtype=F32: pltpu.VMEM(shape, dtype)
        tail = jax.ShapeDtypeStruct((n_batch, d_model), BF16)
        n_chip = n_dev // 2
        key_cache, val_cache, dec, last = pl.pallas_call(
            functools.partial(layer_kernel, n_dev, n_rep),
            out_shape=(cache, cache, tail, tail),
            in_specs=[smem] + [hbm] * 8 + [vmem] * 5,
            out_specs=(hbm, hbm, vmem, vmem),
            scratch_shapes=[
                scratch(3, 2, 2, d_model, kv_width, dtype=BF16),
                scratch(d_model, kv_width, dtype=BF16),
                scratch(kv_width, d_model, dtype=BF16),
                scratch(d_model, ff, dtype=BF16), scratch(d_model, ff, dtype=BF16), scratch(ff, d_model, dtype=BF16),
                scratch(n_batch, seq_loc, d_model, dtype=BF16),
                scratch(2, half, seq_loc, d_model, dtype=BF16),
                scratch(4, 4, 2, half, seq_loc, heads, HEAD_DIM, dtype=BF16),
                scratch(2 * GROUP * seq_loc, HEAD_DIM),
                scratch(n_batch, d_model), scratch(n_chip, n_batch, width),
                scratch(n_chip, n_batch, width), scratch(n_chip, n_batch, width),
                scratch(n_dev, n_batch, width, dtype=BF16),
                scratch(2 * n_batch, HEAD_DIM), scratch(2 * n_batch, HEAD_DIM),
                scratch(2 * n_batch, d_model, dtype=BF16),
                scratch(2 * n_q, HEAD_DIM), scratch(n_dev, 2 * n_q, HEAD_DIM, dtype=BF16),
                scratch(n_batch, heads, HEAD_DIM, dtype=BF16), scratch(n_batch, heads, HEAD_DIM, dtype=BF16),
                scratch(2 * n_q, HEAD_DIM), scratch(2 * n_q, HEAD_DIM),
                scratch(n_q, 2 * half * seq_loc, dtype=jnp.int32),
                scratch(3, 4, 2, n_q, HEAD_DIM), scratch(4, 4, 2, n_q, HEAD_DIM),
                scratch(2 * n_batch, kv_width),
                scratch(2, 2 * n_batch, d_model), scratch(2, n_chip, 2 * n_batch, width),
                scratch(2, n_chip, 2 * n_batch, width), scratch(2, n_chip, 2 * n_batch, width),
                scratch(2, n_dev, 2 * n_batch, width, dtype=BF16),
                dma((2 * n_chunk,)), dma((7,)), dma((2, 2, 2)), dma((2, 2, 2)), dma((2, 2)), dma((2, 2, 2)), dma(()), dma((2, 2)),
                dma((2, n_chunk)), dma((2, n_chunk)),
                dma((2,)), dma(()), dma((2,)), dma((2,)), dma((2,)), dma((3, 4)), dma((4, 4)),
            ],
            compiler_params=pltpu.CompilerParams(collective_id=0, has_side_effects=True, vmem_limit_bytes=63 * 2 ** 20),
            name='layer',
        )(lengths, prompt, wk, wv, wq, wo, wg, wu, wd, new_tok, norm_attn, norm_mlp, cos_tab, sin_tab)
        return dec, last, key_cache[None], val_cache[None]

    return jax.shard_map(per_device, mesh=mesh, in_specs=in_specs, out_specs=out_specs, check_vma=False)
```

```python
import functools

import numpy as np

import jax
import jax.numpy as jnp
from jax import lax
from jax.experimental import pallas as pl
from jax.experimental.pallas import tpu as pltpu
from jax.sharding import PartitionSpec as P

HEAD_DIM = 128
NEG_BIG = -1e30
MESH = pl.DeviceIdType.MESH
GROUP = 2
VMEM_MIB = 49
LOTS = (9, 1, 2)
F32 = jnp.float32
BF16 = jnp.bfloat16


def dot_f32(lhs, rhs):
    return jnp.dot(lhs, rhs, preferred_element_type=F32)


def rms_rows(rows_f32, gain_f32):
    inv_rms = lax.rsqrt(jnp.mean(rows_f32 * rows_f32, axis=-1, keepdims=True) + 1e-5)
    return (rows_f32 * inv_rms * gain_f32).astype(BF16)


def rope_half(head_f32, cos_t, sin_t):
    return head_f32 * cos_t + pltpu.roll(head_f32, HEAD_DIM // 2, 1) * sin_t


def remote(src, dst, send_sem, recv_sem, dev):
    return pltpu.make_async_remote_copy(src_ref=src, dst_ref=dst, send_sem=send_sem, recv_sem=recv_sem,
                                        device_id={'model': dev}, device_id_type=MESH)


def wait_bytes(ref, sem):
    pltpu.make_async_copy(ref, ref, sem).wait()


def layer_kernel(n_dev, n_rep, len_ref, x_hbm, wk_hbm, wv_hbm, wq_hbm, wo_hbm, wg_hbm, wu_hbm, wd_hbm, tok_ref, gain_ref, gain2_ref, cos_ref, sin_ref,
                 kout, vout, dec_out, last_out,
                 wbuf, wq, wo, xown, xrecv, stage, ktmp, lfull, lgot, lpair, lrecv, lcols, crow, srow,
                 rows, qtmp, qall, knew, vnew, kself, vself, near, psend, prec, att, part, got, pair, recv, hid,
                 xcopy_sem, wcopy_sem, wrecv_sem, wsend_sem, wown_sem, wfwd_sem, ysend_sem, yrecv_sem, xrecv_sem, xsend_sem,
                 kv_recv_sem, kv_send_sem, p_sem, sum_sem, all_sem, mlp_sem):
    n_batch, seq_loc, d_model = xown.shape
    n_chip = n_dev // 2
    half = n_batch // 2
    n_chunk = half // GROUP
    m_rows = GROUP * seq_loc
    seq_len = seq_loc * n_dev
    width = d_model // n_dev
    me = lax.axis_index('model')
    rep = lax.axis_index('replica')
    chip, core = me // 2, lax.rem(me, 2)
    left, right = lax.rem(chip + n_chip - 1, n_chip), lax.rem(chip + 1, n_chip)
    partner = chip * 2 + 1 - core
    w_hbm = (wk_hbm, wv_hbm)
    outs = (kout, vout)
    owners = (me, me, left * 2 + core, right * 2 + core)
    firsts = (0, half, 0, half)
    aims = (left, right, right, left)
    slots = (1, 2, 2, 1)

    def col(j):
        return pl.ds(pl.multiple_of(j * width, width), width)

    wlocal = [pltpu.make_async_copy(w_hbm[kv], wbuf.at[0, core, kv], wcopy_sem.at[kv]) for kv in range(2)]
    for cp in wlocal:
        cp.start()

    def xcopy(ch):
        return pltpu.make_async_copy(x_hbm.at[pl.ds(ch * GROUP, GROUP)], xown.at[pl.ds(ch * GROUP, GROUP)], xcopy_sem.at[ch])

    for ch in range(2 * n_chunk):
        xcopy(ch).start()
    later = [pltpu.make_async_copy(src, dst, wcopy_sem.at[2 + i])
             for i, (src, dst) in enumerate(((wq_hbm, wq), (wo_hbm, wo)))]
    for cp in later:
        cp.start()

    barrier = pltpu.get_barrier_semaphore()
    for off in range(1, n_dev):
        pl.semaphore_signal(barrier, inc=1, device_id={'model': lax.rem(me + off, n_dev)}, device_id_type=MESH)

    @pl.loop(1, n_rep)
    def _(off):
        pl.semaphore_signal(barrier, inc=1, device_id={'replica': lax.rem(rep + off, n_rep)}, device_id_type=MESH)

    pl.semaphore_wait(barrier, n_dev + n_rep - 2)

    n_sub = 2
    slice_rows = d_model // n_rep
    sub_rows = slice_rows // n_sub

    def w_slice(h):
        return pl.ds(pl.multiple_of(rep * slice_rows + h * sub_rows, sub_rows), sub_rows)

    wsends = []
    for kv in range(2):
        for h in range(n_sub):
            for slot, aim in ((1, right), (2, left)):
                wsends.append(remote(w_hbm[kv].at[w_slice(h)], wbuf.at[slot, core, kv, w_slice(h)],
                                     wsend_sem.at[slot - 1, kv, h], wrecv_sem.at[slot - 1, kv, h], aim * 2 + core))
        wsends.append(remote(w_hbm[kv], wbuf.at[0, core, kv], wown_sem.at[0, kv], wown_sem.at[1, kv], partner))
    for cp in wsends:
        cp.start()

    def pass_on(kv, h):
        for slot in (1, 2):
            block = wbuf.at[slot, core, kv, w_slice(h)]
            wait_bytes(block, wrecv_sem.at[slot - 1, kv, h])

            @pl.loop(1, n_rep)
            def _(off):
                pltpu.make_async_remote_copy(src_ref=block, dst_ref=block, send_sem=ysend_sem, recv_sem=yrecv_sem.at[slot - 1, kv],
                                             device_id={'replica': lax.rem(rep + off, n_rep)}, device_id_type=MESH).start()

    xsends = []

    def send_rows(ci):
        for side, aim in ((0, right), (1, left)):
            xsends.append(remote(x_hbm.at[pl.ds(side * half + ci * GROUP, GROUP)], xrecv.at[side, pl.ds(ci * GROUP, GROUP)],
                                 xsend_sem.at[side, ci], xrecv_sem.at[side, ci], aim * 2 + core))
            xsends[-1].start()

    def other_chips():
        return [lax.rem(chip + off, n_chip) for off in range(1, n_chip)]

    def sum_pair(index, full, got_ref):
        for c in range(n_chip):
            remote(full.at[:, col(c * 2 + 1 - core)], got_ref.at[c], sum_sem.at[index, 0], sum_sem.at[index, 1], partner).start()

    def sum_chips(index, full, got_ref, pair_ref, recv_ref):
        wait_bytes(got_ref, sum_sem.at[index, 1])
        for c in range(n_chip):
            pair_ref[c] = full[:, col(c * 2 + core)] + got_ref[c]
        for c in other_chips():
            remote(pair_ref.at[c], recv_ref.at[chip], sum_sem.at[index, 2], sum_sem.at[index, 3], c * 2 + core).start()
        recv_ref[chip] = pair_ref[chip]

    def sum_end(index, recv_ref):
        wait_bytes(recv_ref.at[pl.ds(0, n_chip - 1)], sum_sem.at[index, 3])
        return jnp.sum(recv_ref[...], axis=0)

    def gather(index, buf):
        for c in other_chips():
            remote(buf.at[me], buf.at[me], all_sem.at[index, 0], all_sem.at[index, 1], c * 2 + core).start()
        remote(buf.at[me], buf.at[me], all_sem.at[index, 2], all_sem.at[index, 3], partner).start()

    def gather_pass(index, buf):
        wait_bytes(buf.at[pl.ds(0, n_chip - 1)], all_sem.at[index, 1])
        for c in other_chips():
            remote(buf.at[c * 2 + core], buf.at[c * 2 + core], all_sem.at[index, 2], all_sem.at[index, 3], partner).start()

    def gather_end(index, buf):
        wait_bytes(buf.at[pl.ds(0, n_chip)], all_sem.at[index, 3])

    gain = gain_ref[...].astype(F32)

    def normalize(ref):
        for g in range(GROUP):
            ref[g] = rms_rows(ref[g].astype(F32), gain)

    def make_kv(rows_ref, unit, ci, owner, b0, slot, kcore, dst):
        mat = rows_ref[...].reshape(m_rows, d_model)
        start = pl.multiple_of(owner * seq_loc, seq_loc)
        cos_t = jnp.concatenate([cos_ref[pl.ds(start, seq_loc), :]] * GROUP, axis=0)
        sin_t = jnp.concatenate([sin_ref[pl.ds(start, seq_loc), :]] * GROUP, axis=0)
        for kv in range(2):
            acc = dot_f32(mat, wbuf[slot, kcore, kv])
            for h in range(2):
                head = acc[:, h * HEAD_DIM:(h + 1) * HEAD_DIM]
                if kv == 0:
                    head = rope_half(head, cos_t, sin_t)
                ktmp[pl.ds(h, m_rows, stride=2), :] = head
            piece = stage.at[unit, dst, kv, pl.ds(ci * GROUP, GROUP)]
            made = ktmp[...].astype(BF16)
            piece.reshape(2 * m_rows, HEAD_DIM)[...] = made
            if slot == 0 and dst == 3:
                for g in range(GROUP):
                    outs[kv].at[b0 + g, pl.ds(start, seq_loc)].reshape(2 * seq_loc, HEAD_DIM)[...] = \
                        made[g * 2 * seq_loc:(g + 1) * 2 * seq_loc]
            elif slot == 0:
                remote(piece, outs[kv].at[pl.ds(b0, GROUP), pl.ds(start, seq_loc)], kv_send_sem, kv_recv_sem.at[kv], partner).start()

    waiting = [(units, ci, kcore, kv) for units in ((0, 1), (3, 2)) for ci in range(n_chunk) for kcore in range(2) for kv in range(2)]

    def send_kv(count):
        for _ in range(min(count, len(waiting))):
            units, ci, kcore, kv = waiting.pop(0)
            for unit in units:
                start = pl.multiple_of(owners[unit] * seq_loc, seq_loc)
                remote(stage.at[unit, kcore, kv, pl.ds(ci * GROUP, GROUP)],
                       outs[kv].at[pl.ds(firsts[unit] + ci * GROUP, GROUP), pl.ds(start, seq_loc)],
                       kv_send_sem, kv_recv_sem.at[kv], aims[unit] * 2 + kcore).start()

    for cp in wlocal:
        cp.wait()
    base = me * seq_loc

    @pl.loop(0, 2 * n_chunk)
    def _(ch):
        xcopy(ch).wait()
        own = xown.at[pl.ds(ch * GROUP, GROUP)]
        for g in range(GROUP):
            b = ch * GROUP + g
            hit = lax.broadcasted_iota(jnp.int32, (16, seq_loc), 1) == len_ref[b] - 1 - base
            row = dot_f32(jnp.where(hit, 1.0, 0.0).astype(BF16), xown[b])
            lfull[pl.ds(b, 1), :] = row[0:1]
        normalize(own)
        make_kv(own, ch // n_chunk, lax.rem(ch, n_chunk), me, ch * GROUP, 0, core, 3)

    pass_on(0, 0)
    sum_pair(0, lfull, lgot)
    for kv in range(2):
        wait_bytes(wbuf.at[0, 1 - core, kv], wown_sem.at[1, kv])

    @pl.loop(0, 2 * n_chunk)
    def _(ch):
        make_kv(xown.at[pl.ds(ch * GROUP, GROUP)], ch // n_chunk, lax.rem(ch, n_chunk), me, ch * GROUP, 0, 1 - core, 2)

        @pl.when(ch == n_chunk - 1)
        def _():
            pass_on(0, 1)
            sum_chips(0, lfull, lgot, lpair, lrecv)

    send_rows(0)
    pass_on(1, 0)

    far = 1 << 20
    r_idx = lax.broadcasted_iota(jnp.int32, near.shape, 0)
    c_idx = lax.broadcasted_iota(jnp.int32, near.shape, 1)
    match = (c_idx // (2 * seq_loc) == lax.rem(r_idx, half)) & (lax.rem(c_idx, 2) == lax.rem(r_idx // half, 2))
    near[...] = jnp.where(match, lax.rem(c_idx // 2, seq_loc), far)

    pass_on(1, 1)
    lcols[me] = sum_end(0, lrecv).astype(BF16)
    gather(0, lcols)
    send_rows(1)

    rows[0:n_batch, :] = tok_ref[...]
    for b in range(n_batch):
        for r in range(2):
            at = jnp.maximum(len_ref[b] - r, 0)
            crow[pl.ds(r * n_batch + b, 1), :] = cos_ref[pl.ds(at, 1), :]
            srow[pl.ds(r * n_batch + b, 1), :] = sin_ref[pl.ds(at, 1), :]
    later[0].wait()
    gather_pass(0, lcols)
    gather_end(0, lcols)
    for j in range(n_dev):
        rows[n_batch:2 * n_batch, j * width:(j + 1) * width] = lcols[j]
    rows_n = rms_rows(rows[...].astype(F32), gain)
    q_acc = dot_f32(rows_n, wq[...])
    for h in range(2):
        head = rope_half(q_acc[:, h * HEAD_DIM:(h + 1) * HEAD_DIM], crow[...], srow[...])
        for r in range(2):
            for s in range(2):
                qtmp[pl.ds(((s * 2 + r) * 2 + h) * half, half), :] = head[r * n_batch + s * half:r * n_batch + (s + 1) * half]
    qall[me] = qtmp[...].astype(BF16)
    gather(1, qall)
    for ci in range(2, n_chunk):
        send_rows(ci)
    kself[...] = jnp.zeros_like(kself)
    vself[...] = jnp.zeros_like(vself)
    for kv, (new, own) in enumerate(((knew, kself), (vnew, vself))):
        acc = dot_f32(rows_n[0:n_batch], wbuf[0, core, kv])
        for h in range(2):
            head = acc[:, h * HEAD_DIM:(h + 1) * HEAD_DIM]
            if kv == 0:
                head = rope_half(head, crow[0:n_batch, :], srow[0:n_batch, :])
            ktmp[pl.ds(h, n_batch, stride=2), :] = head
            head = head.astype(BF16).astype(F32)
            for s in range(2):
                own[pl.ds((s * 4 + h) * half, half), :] = head[s * half:(s + 1) * half]
        new.reshape(2 * n_batch, HEAD_DIM)[...] = ktmp[0:2 * n_batch, :].astype(BF16)
        for b in range(n_batch):
            outs[kv][b, seq_len] = new[b]

    fwds = []
    for kv in range(2):
        for slot in (1, 2):
            if n_rep > 1:
                wait_bytes(wbuf.at[slot, core, kv, pl.ds(0, d_model - slice_rows)], yrecv_sem.at[slot - 1, kv])
            fwds.append(remote(wbuf.at[slot, core, kv], wbuf.at[slot, core, kv], wfwd_sem.at[0, slot - 1, kv], wfwd_sem.at[1, slot - 1, kv], partner))
            fwds[-1].start()
    for kv in range(2):
        for slot in (1, 2):
            wait_bytes(wbuf.at[slot, 1 - core, kv], wfwd_sem.at[1, slot - 1, kv])

    @pl.loop(0, n_chunk)
    def _(ci):
        @pl.loop(0, 2)
        def _(kcore):
            for unit in range(2):
                make_kv(xown.at[pl.ds(firsts[unit] + ci * GROUP, GROUP)], unit, ci, me, firsts[unit] + ci * GROUP, slots[unit], kcore, kcore)

    gather_pass(1, qall)
    send_kv(LOTS[0])

    @pl.loop(0, n_chunk)
    def _(ci):
        for side in range(2):
            unit = 2 + side
            rows_ref = xrecv.at[side, pl.ds(ci * GROUP, GROUP)]
            b0 = firsts[unit] + ci * GROUP
            wait_bytes(rows_ref, xrecv_sem.at[side, ci])
            normalize(rows_ref)

            @pl.loop(0, 2)
            def _(kcore):
                make_kv(rows_ref, unit, ci, owners[unit], b0, slots[unit], kcore, kcore)

            make_kv(rows_ref, unit, ci, owners[unit], b0, 0, 1 - core, 2)
            make_kv(rows_ref, unit, ci, owners[unit], b0, 0, core, 3)

    for cp in wsends + fwds:
        cp.wait_send()
    if n_rep > 1:
        for slot in (1, 2):
            wait_bytes(wbuf.at[slot, 0, :, pl.ds(0, d_model - slice_rows)], ysend_sem)
    ff, block = wd_hbm.shape[0], wbuf.shape[4]
    places = [wbuf.at[i // 4, (i // 2) % 2, i % 2] for i in range(12)]
    gate_w, up_w = places[0:4], places[4:8]
    down_w = [places[8 + i // 2].at[pl.ds((i % 2) * ff, ff)] for i in range(8)]
    mlp_copies = []
    for i, (src, dsts) in enumerate(((wg_hbm, gate_w), (wu_hbm, up_w), (wd_hbm, down_w))):
        for j, dst in enumerate(dsts):
            mlp_copies.append(pltpu.make_async_copy(src.at[:, pl.ds(j * block, block)], dst, mlp_sem.at[i * 4 + j]))
            mlp_copies[-1].start()

    gather_end(1, qall)
    n_q = 4 * half
    scale = HEAD_DIM ** -0.5
    lane = lax.broadcasted_iota(jnp.int32, (n_q, HEAD_DIM), 1)
    q_row = lax.broadcasted_iota(jnp.int32, (n_q, 1), 0)
    q_len = []
    for s in range(2):
        vec = jnp.zeros((n_q, 1), jnp.int32)
        for b in range(half):
            vec = jnp.where(lax.rem(q_row, half) == b, len_ref[s * half + b], vec)
        q_len.append(vec)

    def partial_att(unit, dst):
        s = unit % 2
        target = (aims[unit] * 2, aims[unit] * 2 + 1, partner, me)[dst]
        q32 = qall[target, s * n_q:(s + 1) * n_q, :]
        keys = stage.at[unit, dst, 0].reshape(2 * half * seq_loc, HEAD_DIM)[...]
        vals = stage.at[unit, dst, 1].reshape(2 * half * seq_loc, HEAD_DIM)[...]
        scores = lax.dot_general(q32, keys, (((1,), (1,)), ((), ())), preferred_element_type=F32) * scale
        scores = jnp.where(near[...] < q_len[s] - owners[unit] * seq_loc, scores, NEG_BIG)
        top = jnp.max(scores, axis=1, keepdims=True)
        prob = jnp.exp(scores - top)
        total = jnp.sum(prob, axis=1, keepdims=True)
        acc = dot_f32(prob.astype(BF16), vals)
        dest = prec.at[3, unit] if dst == 3 else psend.at[dst, unit]
        dest[0] = acc
        dest[1] = jnp.where(lane < HEAD_DIM // 2, top, total)
        if dst == 2:
            remote(psend.at[dst, unit], prec.at[2, unit], p_sem.at[0], p_sem.at[1], partner).start()
        elif dst < 2:
            remote(psend.at[dst, unit], prec.at[core, unit], p_sem.at[0], p_sem.at[1], target).start()

    for dst in range(4):
        for unit in range(4):
            partial_att(unit, dst)
        send_kv(LOTS[1])

    wait_bytes(prec.at[pl.ds(0, 3)], p_sem.at[1])
    for s in range(2):
        q32 = qall[me, s * n_q:(s + 1) * n_q, :].astype(F32)
        is_new = q_row < n_q // 2
        self_score = jnp.sum(q32 * kself[s * n_q:(s + 1) * n_q, :], axis=1, keepdims=True) * scale
        tops = [jnp.where(is_new, self_score, NEG_BIG)]
        sums = [jnp.where(is_new, 1.0, 0.0)]
        accs = [vself[s * n_q:(s + 1) * n_q, :]]
        for unit in (s, s + 2):
            for src in range(4):
                stat = prec[src, unit, 1]
                tops.append(stat[:, 0:1])
                sums.append(stat[:, HEAD_DIM // 2:HEAD_DIM // 2 + 1])
                accs.append(prec[src, unit, 0])
        top = functools.reduce(jnp.maximum, tops)
        facs = [jnp.exp(t - top) for t in tops]
        total = sum(f * l for f, l in zip(facs, sums))
        merged = sum(f * a for f, a in zip(facs, accs)) / total
        for r in range(2):
            for h in range(2):
                att[r * n_batch + s * half:r * n_batch + (s + 1) * half, h * HEAD_DIM:(h + 1) * HEAD_DIM] = \
                    merged[(r * 2 + h) * half:(r * 2 + h + 1) * half]

    def add_partials(step):
        sum_pair(1 + step, part.at[step], got.at[step])
        sum_chips(1 + step, part.at[step], got.at[step], pair.at[step], recv.at[step])
        send_kv(LOTS[2])
        mine = rows[:, col(me)].astype(F32)
        hid[step, me] = (mine + sum_end(1 + step, recv.at[step])).astype(BF16)
        gather(2 + step, hid.at[step])
        send_kv(LOTS[2])
        gather_pass(2 + step, hid.at[step])
        gather_end(2 + step, hid.at[step])

    later[1].wait()
    part[0] = dot_f32(att[...].astype(BF16), wo[...])
    add_partials(0)
    for j in range(n_dev):
        rows[:, j * width:(j + 1) * width] = hid[0, j]
    for cp in mlp_copies:
        cp.wait()
    rows_n = rms_rows(rows[...].astype(F32), gain2_ref[...].astype(F32))
    mids = []
    for g_ref, u_ref in zip(gate_w, up_w):
        gate = dot_f32(rows_n, g_ref[...])
        mids.append((gate * (1.0 / (1.0 + jnp.exp(-gate))) * dot_f32(rows_n, u_ref[...])).astype(BF16))
    mid = jnp.concatenate(mids, axis=1)
    for j, d_ref in enumerate(down_w):
        part[1, :, j * block:(j + 1) * block] = dot_f32(mid, d_ref[...])
    add_partials(1)
    send_kv(len(waiting))
    for j in range(n_dev):
        dec_out[:, j * width:(j + 1) * width] = hid[1, j, 0:n_batch, :]
        last_out[:, j * width:(j + 1) * width] = hid[1, j, n_batch:2 * n_batch, :]

    for cp in xsends:
        cp.wait_send()
    wait_bytes(psend, p_sem.at[0])
    for index, (got_ref, recv_ref) in enumerate(((lgot, lrecv), (got.at[0], recv.at[0]), (got.at[1], recv.at[1]))):
        wait_bytes(got_ref, sum_sem.at[index, 0])
        wait_bytes(recv_ref.at[pl.ds(0, n_chip - 1)], sum_sem.at[index, 2])
    for index, buf in enumerate((lcols, qall, hid.at[0], hid.at[1])):
        wait_bytes(buf.at[pl.ds(0, n_chip - 1)], all_sem.at[index, 0])
        wait_bytes(buf.at[pl.ds(0, n_chip)], all_sem.at[index, 2])
    for kv in range(2):
        wait_bytes(outs[kv].at[pl.ds(0, 3 * n_batch // 4), pl.ds(0, seq_len)], kv_recv_sem.at[kv])
    wait_bytes(stage.at[:, pl.ds(0, 3)], kv_send_sem)


def deliver_kernel(k_in, v_in, d_in, l_in, k_out, v_out, d_out, l_out, sem):
    copies = [pltpu.make_async_copy(src, dst, sem.at[i])
              for i, (src, dst) in enumerate(((k_in, k_out), (v_in, v_out), (d_in, d_out), (l_in, l_out)))]
    for cp in copies:
        cp.start()
    for cp in copies:
        cp.wait()


def rotary_tables(n_pos):
    inv_freq = np.float32(10000.0) ** (-2.0 * np.arange(HEAD_DIM // 2, dtype=np.float32) / HEAD_DIM).astype(np.float32)
    angles = np.arange(n_pos, dtype=np.float32)[:, None] * inv_freq.astype(np.float32)
    cos, sin = np.cos(angles), np.sin(angles)
    return (np.concatenate([cos, cos], axis=1).astype(np.float32), np.concatenate([-sin, sin], axis=1).astype(np.float32))


def solution(mesh):
    n_dev, n_rep = mesh.shape['model'], mesh.shape['replica']
    seq_spec = P('replica', 'model', None)
    col_spec = P(None, None, 'model')
    row_spec = P(None, 'model', None)
    gain_spec = P(None, None)
    tok_spec = P('replica', None)
    cache_spec = P(None, 'replica', None, 'model', None)
    in_specs = (seq_spec, P('replica'), tok_spec, gain_spec, col_spec, col_spec, col_spec, row_spec, gain_spec, col_spec, col_spec, row_spec)
    out_specs = (tok_spec, tok_spec, cache_spec, cache_spec)
    hbm = pl.BlockSpec(memory_space=pl.ANY)
    vmem = pl.BlockSpec(memory_space=pltpu.VMEM)
    smem = pl.BlockSpec(memory_space=pltpu.SMEM)
    dma = pltpu.SemaphoreType.DMA

    def per_device(prompt, lengths, new_tok, norm_attn, w_q, w_k, w_v, w_o, norm_mlp, w_gate, w_up, w_down):
        n_batch, seq_loc, d_model = prompt.shape
        kv_width = w_k.shape[2]
        heads = kv_width // HEAD_DIM
        seq_len = seq_loc * n_dev
        half = n_batch // 2
        n_chunk = half // GROUP
        width = d_model // n_dev
        wq, wk, wv, wo, wg, wu, wd = w_q[0], w_k[0], w_v[0], w_o[0], w_gate[0], w_up[0], w_down[0]
        cos_tab, sin_tab = (jnp.asarray(t) for t in rotary_tables(seq_len + 8))

        ff = wg.shape[1]
        n_q = 4 * half
        cache = jax.ShapeDtypeStruct((n_batch, seq_len + 1, heads, HEAD_DIM), BF16)
        scratch = lambda *shape, dtype=F32: pltpu.VMEM(shape, dtype)
        held = pltpu.VMEM(cache.shape, BF16)
        tail = jax.ShapeDtypeStruct((n_batch, d_model), BF16)
        n_chip = n_dev // 2
        key_cache, val_cache, dec, last = pl.pallas_call(
            functools.partial(layer_kernel, n_dev, n_rep),
            out_shape=(held, held, pltpu.VMEM(tail.shape, BF16), pltpu.VMEM(tail.shape, BF16)),
            in_specs=[smem] + [hbm] * 8 + [vmem] * 5,
            out_specs=(vmem,) * 4,
            scratch_shapes=[
                scratch(3, 2, 2, d_model, kv_width, dtype=BF16),
                scratch(d_model, kv_width, dtype=BF16),
                scratch(kv_width, d_model, dtype=BF16),
                scratch(n_batch, seq_loc, d_model, dtype=BF16),
                scratch(2, half, seq_loc, d_model, dtype=BF16),
                scratch(4, 4, 2, half, seq_loc, heads, HEAD_DIM, dtype=BF16),
                scratch(2 * GROUP * seq_loc, HEAD_DIM),
                scratch(n_batch, d_model), scratch(n_chip, n_batch, width),
                scratch(n_chip, n_batch, width), scratch(n_chip, n_batch, width),
                scratch(n_dev, n_batch, width, dtype=BF16),
                scratch(2 * n_batch, HEAD_DIM), scratch(2 * n_batch, HEAD_DIM),
                scratch(2 * n_batch, d_model, dtype=BF16),
                scratch(2 * n_q, HEAD_DIM), scratch(n_dev, 2 * n_q, HEAD_DIM, dtype=BF16),
                scratch(n_batch, heads, HEAD_DIM, dtype=BF16), scratch(n_batch, heads, HEAD_DIM, dtype=BF16),
                scratch(2 * n_q, HEAD_DIM), scratch(2 * n_q, HEAD_DIM),
                scratch(n_q, 2 * half * seq_loc, dtype=jnp.int32),
                scratch(3, 4, 2, n_q, HEAD_DIM), scratch(4, 4, 2, n_q, HEAD_DIM),
                scratch(2 * n_batch, kv_width),
                scratch(2, 2 * n_batch, d_model), scratch(2, n_chip, 2 * n_batch, width),
                scratch(2, n_chip, 2 * n_batch, width), scratch(2, n_chip, 2 * n_batch, width),
                scratch(2, n_dev, 2 * n_batch, width, dtype=BF16),
                dma((2 * n_chunk,)), dma((4,)), dma((2, 2, 2)), dma((2, 2, 2)), dma((2, 2)), dma((2, 2, 2)), dma(()), dma((2, 2)),
                dma((2, n_chunk)), dma((2, n_chunk)),
                dma((2,)), dma(()), dma((2,)), dma((3, 4)), dma((4, 4)), dma((16,)),
            ],
            compiler_params=pltpu.CompilerParams(collective_id=0, has_side_effects=True, vmem_limit_bytes=VMEM_MIB * 2 ** 20),
            name='layer',
        )(*(pltpu.with_memory_space_constraint(a, pltpu.HBM) for a in
            (lengths, prompt, wk, wv, wq, wo, wg, wu, wd, new_tok, norm_attn, norm_mlp, cos_tab, sin_tab)))
        key_cache, val_cache, dec, last = pl.pallas_call(
            deliver_kernel, out_shape=(cache, cache, tail, tail), in_specs=[vmem] * 4, out_specs=(hbm,) * 4,
            scratch_shapes=[dma((4,))], name='deliver',
            compiler_params=pltpu.CompilerParams(vmem_limit_bytes=14 * 2 ** 20),
        )(key_cache, val_cache, dec, last)
        return dec, last, key_cache[None], val_cache[None]

    return jax.shard_map(per_device, mesh=mesh, in_specs=in_specs, out_specs=out_specs, check_vma=False)
```

```python
import functools

import numpy as np

import jax
import jax.numpy as jnp
from jax import lax
from jax.experimental import pallas as pl
from jax.experimental.pallas import tpu as pltpu
from jax.sharding import PartitionSpec as P

HEAD_DIM = 128
NEG_BIG = -1e30
MESH = pl.DeviceIdType.MESH
GROUP = 2
VMEM_MIB = 49
LOTS = (8, 1, 3, 2)
F32 = jnp.float32
BF16 = jnp.bfloat16


def dot_f32(lhs, rhs):
    return jnp.dot(lhs, rhs, preferred_element_type=F32)


def rms_rows(rows_f32, gain_f32):
    inv_rms = lax.rsqrt(jnp.mean(rows_f32 * rows_f32, axis=-1, keepdims=True) + 1e-5)
    return (rows_f32 * inv_rms * gain_f32).astype(BF16)


def rope_half(head_f32, cos_t, sin_t):
    return head_f32 * cos_t + pltpu.roll(head_f32, HEAD_DIM // 2, 1) * sin_t


def remote(src, dst, send_sem, recv_sem, dev):
    return pltpu.make_async_remote_copy(src_ref=src, dst_ref=dst, send_sem=send_sem, recv_sem=recv_sem,
                                        device_id={'model': dev}, device_id_type=MESH)


def wait_bytes(ref, sem):
    pltpu.make_async_copy(ref, ref, sem).wait()


def layer_kernel(n_dev, n_rep, len_ref, x_hbm, wk_hbm, wv_hbm, wq_hbm, wo_hbm, wg_hbm, wu_hbm, wd_hbm, tok_hbm, gain_hbm, gain2_hbm, cos_hbm, sin_hbm,
                 kout, vout, dec_out, last_out,
                 wbuf, wq, wo, xown, xrecv, stage, ktmp, lfull, lgot, lpair, lrecv, lcols, crow, srow,
                 rows, qtmp, qall, knew, vnew, kself, vself, near, psend, prec, att, part, got, pair, far_got, comb, recv, hid, tok_ref, gain_ref, gain2_ref, cos_ref, sin_ref,
                 xcopy_sem, wcopy_sem, wrecv_sem, wsend_sem, wown_sem, wfwd_sem, ysend_sem, yrecv_sem, xrecv_sem, xsend_sem,
                 kv_recv_sem, kv_send_sem, p_sem, sum_sem, all_sem, mlp_sem, small_sem):
    n_batch, seq_loc, d_model = xown.shape
    n_chip = n_dev // 2
    half = n_batch // 2
    n_chunk = half // GROUP
    m_rows = GROUP * seq_loc
    seq_len = seq_loc * n_dev
    width = d_model // n_dev
    me = lax.axis_index('model')
    rep = lax.axis_index('replica')
    chip, core = me // 2, lax.rem(me, 2)
    left, right = lax.rem(chip + n_chip - 1, n_chip), lax.rem(chip + 1, n_chip)
    partner = chip * 2 + 1 - core
    w_hbm = (wk_hbm, wv_hbm)
    outs = (kout, vout)
    owners = (me, me, left * 2 + core, right * 2 + core)
    firsts = (0, half, 0, half)
    aims = (left, right, right, left)
    slots = (1, 2, 2, 1)

    def col(j):
        return pl.ds(pl.multiple_of(j * width, width), width)

    barrier = pltpu.get_barrier_semaphore()
    for off in range(1, n_dev):
        pl.semaphore_signal(barrier, inc=1, device_id={'model': lax.rem(me + off, n_dev)}, device_id_type=MESH)

    @pl.loop(1, n_rep)
    def _(off):
        pl.semaphore_signal(barrier, inc=1, device_id={'replica': lax.rem(rep + off, n_rep)}, device_id_type=MESH)

    small = [pltpu.make_async_copy(src, dst, small_sem.at[i])
             for i, (src, dst) in enumerate(((tok_hbm, tok_ref), (gain_hbm, gain_ref), (gain2_hbm, gain2_ref), (cos_hbm, cos_ref), (sin_hbm, sin_ref)))]
    for cp in small:
        cp.start()
    wlocal = [pltpu.make_async_copy(w_hbm[kv], wbuf.at[0, core, kv], wcopy_sem.at[kv]) for kv in range(2)]
    for cp in wlocal:
        cp.start()

    def xcopy(ch):
        return pltpu.make_async_copy(x_hbm.at[pl.ds(ch * GROUP, GROUP)], xown.at[pl.ds(ch * GROUP, GROUP)], xcopy_sem.at[ch])

    for ch in range(2 * n_chunk):
        xcopy(ch).start()
    later = [pltpu.make_async_copy(src, dst, wcopy_sem.at[2 + i])
             for i, (src, dst) in enumerate(((wq_hbm, wq), (wo_hbm, wo)))]
    for cp in later:
        cp.start()

    pl.semaphore_wait(barrier, n_dev + n_rep - 2)

    n_sub = 2
    slice_rows = d_model // n_rep
    sub_rows = slice_rows // n_sub

    def w_slice(h):
        return pl.ds(pl.multiple_of(rep * slice_rows + h * sub_rows, sub_rows), sub_rows)

    wsends = []
    for kv in range(2):
        for h in range(n_sub):
            for slot, aim in ((1, right), (2, left)):
                wsends.append(remote(w_hbm[kv].at[w_slice(h)], wbuf.at[slot, core, kv, w_slice(h)],
                                     wsend_sem.at[slot - 1, kv, h], wrecv_sem.at[slot - 1, kv, h], aim * 2 + core))
        wsends.append(remote(w_hbm[kv], wbuf.at[0, core, kv], wown_sem.at[0, kv], wown_sem.at[1, kv], partner))
    for cp in wsends:
        cp.start()

    def pass_on(kv, h):
        for slot in (1, 2):
            block = wbuf.at[slot, core, kv, w_slice(h)]
            wait_bytes(block, wrecv_sem.at[slot - 1, kv, h])

            @pl.loop(1, n_rep)
            def _(off):
                pltpu.make_async_remote_copy(src_ref=block, dst_ref=block, send_sem=ysend_sem, recv_sem=yrecv_sem.at[slot - 1, kv],
                                             device_id={'replica': lax.rem(rep + off, n_rep)}, device_id_type=MESH).start()

    xsends = []

    def send_rows(ci):
        for side, aim in ((0, right), (1, left)):
            xsends.append(remote(x_hbm.at[pl.ds(side * half + ci * GROUP, GROUP)], xrecv.at[side, pl.ds(ci * GROUP, GROUP)],
                                 xsend_sem.at[side, ci], xrecv_sem.at[side, ci], aim * 2 + core))
            xsends[-1].start()

    opposite = lax.rem(chip + 2, n_chip)
    lane_half = (pl.ds(0, width // 2), pl.ds(width // 2, width // 2))

    def sum_pair(index, full, got_ref):
        for c in range(n_chip):
            remote(full.at[:, col(c * 2 + 1 - core)], got_ref.at[c], sum_sem.at[index, 0], sum_sem.at[index, 1], partner).start()

    def other_chips():
        return [lax.rem(chip + off, n_chip) for off in range(1, n_chip)]

    def sum_direct(full, got_ref, pair_ref, recv_ref):
        wait_bytes(got_ref, sum_sem.at[0, 1])
        for c in range(n_chip):
            pair_ref[c] = full[:, col(c * 2 + core)] + got_ref[c]
        for c in other_chips():
            remote(pair_ref.at[c], recv_ref.at[chip], sum_sem.at[0, 2], sum_sem.at[0, 3], c * 2 + core).start()
        recv_ref[chip] = pair_ref[chip]

    def gather_direct(buf):
        for c in other_chips():
            remote(buf.at[me], buf.at[me], all_sem.at[0, 0], all_sem.at[0, 1], c * 2 + core).start()
        remote(buf.at[me], buf.at[me], all_sem.at[0, 2], all_sem.at[0, 3], partner).start()

    def gather_direct_end(buf):
        wait_bytes(buf.at[pl.ds(0, n_chip - 1)], all_sem.at[0, 1])
        for c in other_chips():
            remote(buf.at[c * 2 + core], buf.at[c * 2 + core], all_sem.at[0, 2], all_sem.at[0, 3], partner).start()
        wait_bytes(buf.at[pl.ds(0, n_chip)], all_sem.at[0, 3])

    def sum_far(index, full, got_ref, pair_ref, far_ref):
        wait_bytes(got_ref, sum_sem.at[index, 1])
        for c in range(n_chip):
            pair_ref[c] = full[:, col(c * 2 + core)] + got_ref[c]
        for side, aim in ((0, right), (1, left)):
            remote(pair_ref.at[opposite, :, lane_half[side]], far_ref.at[side], sum_sem.at[index, 2], sum_sem.at[index, 3], aim * 2 + core).start()

    def sum_near(index, pair_ref, far_ref, comb_ref, recv_ref):
        wait_bytes(far_ref, sum_sem.at[index, 3])
        for side, aim in ((0, right), (1, left)):
            comb_ref[side] = pair_ref[aim]
            comb_ref[side, :, lane_half[side]] = pair_ref[aim, :, lane_half[side]] + far_ref[side]
            remote(comb_ref.at[side], recv_ref.at[side], sum_sem.at[index, 4], sum_sem.at[index, 5], aim * 2 + core).start()

    def sum_end(index, pair_ref, recv_ref):
        wait_bytes(recv_ref, sum_sem.at[index, 5])
        return pair_ref[chip] + recv_ref[0] + recv_ref[1]

    def half_of(ref, side):
        if ref.shape[1] == width:
            return ref.at[:, lane_half[side]]
        return ref.at[pl.ds(side * (ref.shape[0] // 2), ref.shape[0] // 2)]

    def gather(index, buf):
        for aim in (right, left):
            remote(buf.at[me], buf.at[me], all_sem.at[index, 0], all_sem.at[index, 1], aim * 2 + core).start()
        remote(buf.at[me], buf.at[me], all_sem.at[index, 2], all_sem.at[index, 3], partner).start()

    def gather_pass(index, buf):
        wait_bytes(buf.at[pl.ds(0, 2)], all_sem.at[index, 1])
        for side, (source, aim) in enumerate(((left, right), (right, left))):
            slot = buf.at[source * 2 + core]
            remote(half_of(slot, side), half_of(slot, side), all_sem.at[index, 4], all_sem.at[index, 5], aim * 2 + core).start()
            remote(slot, slot, all_sem.at[index, 2], all_sem.at[index, 3], partner).start()

    def gather_end(index, buf):
        wait_bytes(buf.at[0], all_sem.at[index, 5])
        slot = buf.at[opposite * 2 + core]
        remote(slot, slot, all_sem.at[index, 2], all_sem.at[index, 3], partner).start()
        wait_bytes(buf.at[pl.ds(0, n_chip)], all_sem.at[index, 3])

    for cp in small:
        cp.wait()
    gain = gain_ref[...].astype(F32)

    def normalize(ref):
        for g in range(GROUP):
            ref[g] = rms_rows(ref[g].astype(F32), gain)

    def make_kv(rows_ref, unit, ci, owner, b0, slot, kcore, dst):
        mat = rows_ref[...].reshape(m_rows, d_model)
        start = pl.multiple_of(owner * seq_loc, seq_loc)
        cos_t = jnp.concatenate([cos_ref[pl.ds(start, seq_loc), :]] * GROUP, axis=0)
        sin_t = jnp.concatenate([sin_ref[pl.ds(start, seq_loc), :]] * GROUP, axis=0)
        for kv in range(2):
            acc = dot_f32(mat, wbuf[slot, kcore, kv])
            for h in range(2):
                head = acc[:, h * HEAD_DIM:(h + 1) * HEAD_DIM]
                if kv == 0:
                    head = rope_half(head, cos_t, sin_t)
                ktmp[pl.ds(h, m_rows, stride=2), :] = head
            piece = stage.at[unit, dst, kv, pl.ds(ci * GROUP, GROUP)]
            made = ktmp[...].astype(BF16)
            piece.reshape(2 * m_rows, HEAD_DIM)[...] = made
            if slot == 0 and dst == 3:
                for g in range(GROUP):
                    outs[kv].at[b0 + g, pl.ds(start, seq_loc)].reshape(2 * seq_loc, HEAD_DIM)[...] = \
                        made[g * 2 * seq_loc:(g + 1) * 2 * seq_loc]
            elif slot == 0:
                remote(piece, outs[kv].at[pl.ds(b0, GROUP), pl.ds(start, seq_loc)], kv_send_sem, kv_recv_sem.at[kv], partner).start()

    waiting = [(units, ci, kcore, kv) for units in ((0, 1), (3, 2)) for ci in range(n_chunk) for kcore in range(2) for kv in range(2)]

    def send_kv(count):
        for _ in range(min(count, len(waiting))):
            units, ci, kcore, kv = waiting.pop(0)
            for unit in units:
                start = pl.multiple_of(owners[unit] * seq_loc, seq_loc)
                remote(stage.at[unit, kcore, kv, pl.ds(ci * GROUP, GROUP)],
                       outs[kv].at[pl.ds(firsts[unit] + ci * GROUP, GROUP), pl.ds(start, seq_loc)],
                       kv_send_sem, kv_recv_sem.at[kv], aims[unit] * 2 + kcore).start()

    for cp in wlocal:
        cp.wait()
    base = me * seq_loc

    @pl.loop(0, 2 * n_chunk)
    def _(ch):
        xcopy(ch).wait()
        own = xown.at[pl.ds(ch * GROUP, GROUP)]
        for g in range(GROUP):
            b = ch * GROUP + g
            hit = lax.broadcasted_iota(jnp.int32, (16, seq_loc), 1) == len_ref[b] - 1 - base
            row = dot_f32(jnp.where(hit, 1.0, 0.0).astype(BF16), xown[b])
            lfull[pl.ds(b, 1), :] = row[0:1]
        normalize(own)
        make_kv(own, ch // n_chunk, lax.rem(ch, n_chunk), me, ch * GROUP, 0, core, 3)

    pass_on(0, 0)
    sum_pair(0, lfull, lgot)
    for kv in range(2):
        wait_bytes(wbuf.at[0, 1 - core, kv], wown_sem.at[1, kv])

    @pl.loop(0, 2 * n_chunk)
    def _(ch):
        make_kv(xown.at[pl.ds(ch * GROUP, GROUP)], ch // n_chunk, lax.rem(ch, n_chunk), me, ch * GROUP, 0, 1 - core, 2)

        @pl.when(ch == n_chunk - 1)
        def _():
            pass_on(0, 1)
            sum_direct(lfull, lgot, lpair, lrecv)

    send_rows(0)
    pass_on(1, 0)

    far = 1 << 20
    r_idx = lax.broadcasted_iota(jnp.int32, near.shape, 0)
    c_idx = lax.broadcasted_iota(jnp.int32, near.shape, 1)
    match = (c_idx // (2 * seq_loc) == lax.rem(r_idx, half)) & (lax.rem(c_idx, 2) == lax.rem(r_idx // half, 2))
    near[...] = jnp.where(match, lax.rem(c_idx // 2, seq_loc), far)

    pass_on(1, 1)
    wait_bytes(lrecv.at[pl.ds(0, n_chip - 1)], sum_sem.at[0, 3])
    lcols[me] = jnp.sum(lrecv[...], axis=0).astype(BF16)
    gather_direct(lcols)
    send_rows(1)

    def received_own(ci):
        for side in range(2):
            unit = 2 + side
            rows_ref = xrecv.at[side, pl.ds(ci * GROUP, GROUP)]
            wait_bytes(rows_ref, xrecv_sem.at[side, ci])
            normalize(rows_ref)
            make_kv(rows_ref, unit, ci, owners[unit], firsts[unit] + ci * GROUP, 0, 1 - core, 2)
            make_kv(rows_ref, unit, ci, owners[unit], firsts[unit] + ci * GROUP, 0, core, 3)

    def received_far(ci):
        for side in range(2):
            unit = 2 + side

            @pl.loop(0, 2)
            def _(kcore):
                make_kv(xrecv.at[side, pl.ds(ci * GROUP, GROUP)], unit, ci, owners[unit], firsts[unit] + ci * GROUP, slots[unit], kcore, kcore)

    n_q = 4 * half
    scale = HEAD_DIM ** -0.5
    lane = lax.broadcasted_iota(jnp.int32, (n_q, HEAD_DIM), 1)
    q_row = lax.broadcasted_iota(jnp.int32, (n_q, 1), 0)
    q_len = []
    for s in range(2):
        vec = jnp.zeros((n_q, 1), jnp.int32)
        for b in range(half):
            vec = jnp.where(lax.rem(q_row, half) == b, len_ref[s * half + b], vec)
        q_len.append(vec)

    def partial_att(unit, dst):
        s = unit % 2
        target = (aims[unit] * 2, aims[unit] * 2 + 1, partner, me)[dst]
        q32 = qall[target, s * n_q:(s + 1) * n_q, :]
        keys = stage.at[unit, dst, 0].reshape(2 * half * seq_loc, HEAD_DIM)[...]
        vals = stage.at[unit, dst, 1].reshape(2 * half * seq_loc, HEAD_DIM)[...]
        scores = lax.dot_general(q32, keys, (((1,), (1,)), ((), ())), preferred_element_type=F32) * scale
        scores = jnp.where(near[...] < q_len[s] - owners[unit] * seq_loc, scores, NEG_BIG)
        top = jnp.max(scores, axis=1, keepdims=True)
        prob = jnp.exp(scores - top)
        total = jnp.sum(prob, axis=1, keepdims=True)
        acc = dot_f32((prob / total).astype(BF16), vals)
        dest = prec.at[3, unit] if dst == 3 else psend.at[dst, unit]
        dest[0] = acc
        dest[1] = jnp.where(lane < HEAD_DIM // 2, top, total)
        if dst == 2:
            remote(psend.at[dst, unit], prec.at[2, unit], p_sem.at[0], p_sem.at[1], partner).start()
        elif dst < 2:
            remote(psend.at[dst, unit], prec.at[core, unit], p_sem.at[0], p_sem.at[1], target).start()

    rows[0:n_batch, :] = tok_ref[...]
    for b in range(n_batch):
        for r in range(2):
            at = jnp.maximum(len_ref[b] - r, 0)
            crow[pl.ds(r * n_batch + b, 1), :] = cos_ref[pl.ds(at, 1), :]
            srow[pl.ds(r * n_batch + b, 1), :] = sin_ref[pl.ds(at, 1), :]
    later[0].wait()
    received_own(0)
    gather_direct_end(lcols)
    for j in range(n_dev):
        rows[n_batch:2 * n_batch, j * width:(j + 1) * width] = lcols[j]
    rows_n = rms_rows(rows[...].astype(F32), gain)
    q_acc = dot_f32(rows_n, wq[...])
    for h in range(2):
        head = rope_half(q_acc[:, h * HEAD_DIM:(h + 1) * HEAD_DIM], crow[...], srow[...])
        for r in range(2):
            for s in range(2):
                qtmp[pl.ds(((s * 2 + r) * 2 + h) * half, half), :] = head[r * n_batch + s * half:r * n_batch + (s + 1) * half]
    qall[me] = qtmp[...].astype(BF16)
    gather(1, qall)
    for ci in range(2, n_chunk - 1):
        send_rows(ci)
    kself[...] = jnp.zeros_like(kself)
    vself[...] = jnp.zeros_like(vself)
    for kv, (new, own) in enumerate(((knew, kself), (vnew, vself))):
        acc = dot_f32(rows_n[0:n_batch], wbuf[0, core, kv])
        for h in range(2):
            head = acc[:, h * HEAD_DIM:(h + 1) * HEAD_DIM]
            if kv == 0:
                head = rope_half(head, crow[0:n_batch, :], srow[0:n_batch, :])
            ktmp[pl.ds(h, n_batch, stride=2), :] = head
            head = head.astype(BF16).astype(F32)
            for s in range(2):
                own[pl.ds((s * 4 + h) * half, half), :] = head[s * half:(s + 1) * half]
        new.reshape(2 * n_batch, HEAD_DIM)[...] = ktmp[0:2 * n_batch, :].astype(BF16)
        for b in range(n_batch):
            outs[kv][b, seq_len] = new[b]

    fwds = []
    for kv in range(2):
        for slot in (1, 2):
            if n_rep > 1:
                wait_bytes(wbuf.at[slot, core, kv, pl.ds(0, d_model - slice_rows)], yrecv_sem.at[slot - 1, kv])
            fwds.append(remote(wbuf.at[slot, core, kv], wbuf.at[slot, core, kv], wfwd_sem.at[0, slot - 1, kv], wfwd_sem.at[1, slot - 1, kv], partner))
            fwds[-1].start()
    for kv in range(2):
        for slot in (1, 2):
            wait_bytes(wbuf.at[slot, 1 - core, kv], wfwd_sem.at[1, slot - 1, kv])

    @pl.loop(0, n_chunk)
    def _(ci):
        @pl.loop(0, 2)
        def _(kcore):
            for unit in range(2):
                make_kv(xown.at[pl.ds(firsts[unit] + ci * GROUP, GROUP)], unit, ci, me, firsts[unit] + ci * GROUP, slots[unit], kcore, kcore)

    gather_pass(1, qall)
    send_rows(n_chunk - 1)
    send_kv(LOTS[0])

    received_far(0)

    @pl.loop(1, n_chunk)
    def _(ci):
        @pl.when(ci == n_chunk - 1)
        def _():
            gather_end(1, qall)
            for dst in range(4):
                for unit in range(2):
                    partial_att(unit, dst)

        received_own(ci)
        received_far(ci)

    for cp in wsends + fwds:
        cp.wait_send()
    if n_rep > 1:
        for slot in (1, 2):
            wait_bytes(wbuf.at[slot, 0, :, pl.ds(0, d_model - slice_rows)], ysend_sem)
    ff, block = wd_hbm.shape[0], wbuf.shape[4]
    places = [wbuf.at[i // 4, (i // 2) % 2, i % 2] for i in range(12)]
    gate_w, up_w = places[0:4], places[4:8]
    down_w = [places[8 + i // 2].at[pl.ds((i % 2) * ff, ff)] for i in range(8)]
    mlp_copies = []
    for i, (src, dsts) in enumerate(((wg_hbm, gate_w), (wu_hbm, up_w), (wd_hbm, down_w))):
        for j, dst in enumerate(dsts):
            mlp_copies.append(pltpu.make_async_copy(src.at[:, pl.ds(j * block, block)], dst, mlp_sem.at[i * 4 + j]))
            mlp_copies[-1].start()

    for dst in range(4):
        for unit in range(2, 4):
            partial_att(unit, dst)
        send_kv(LOTS[1])

    wait_bytes(prec.at[pl.ds(0, 3)], p_sem.at[1])
    for s in range(2):
        q32 = qall[me, s * n_q:(s + 1) * n_q, :].astype(F32)
        is_new = q_row < n_q // 2
        self_score = jnp.sum(q32 * kself[s * n_q:(s + 1) * n_q, :], axis=1, keepdims=True) * scale
        tops = [jnp.where(is_new, self_score, NEG_BIG)]
        sums = [jnp.where(is_new, 1.0, 0.0)]
        accs = [vself[s * n_q:(s + 1) * n_q, :]]
        for unit in (s, s + 2):
            for src in range(4):
                stat = prec[src, unit, 1]
                tops.append(stat[:, 0:1])
                sums.append(stat[:, HEAD_DIM // 2:HEAD_DIM // 2 + 1])
                accs.append(prec[src, unit, 0])
        top = functools.reduce(jnp.maximum, tops)
        facs = [jnp.exp(t - top) for t in tops]
        facs = [f * l for f, l in zip(facs, sums)]
        total = sum(facs)
        merged = sum((f / total) * a for f, a in zip(facs, accs))
        for r in range(2):
            for h in range(2):
                att[r * n_batch + s * half:r * n_batch + (s + 1) * half, h * HEAD_DIM:(h + 1) * HEAD_DIM] = \
                    merged[(r * 2 + h) * half:(r * 2 + h + 1) * half]

    def add_partials(step):
        sum_pair(1 + step, part.at[step], got.at[step])
        sum_far(1 + step, part.at[step], got.at[step], pair.at[step], far_got.at[step])
        send_kv(LOTS[2 + step])
        sum_near(1 + step, pair.at[step], far_got.at[step], comb.at[step], recv.at[step])
        send_kv(LOTS[2 + step])
        mine = rows[:, col(me)].astype(F32)
        hid[step, me] = (mine + sum_end(1 + step, pair.at[step], recv.at[step])).astype(BF16)
        gather(2 + step, hid.at[step])
        send_kv(LOTS[2 + step])
        gather_pass(2 + step, hid.at[step])
        send_kv(LOTS[2 + step])
        gather_end(2 + step, hid.at[step])

    later[1].wait()
    part[0] = dot_f32(att[...].astype(BF16), wo[...])
    add_partials(0)
    for j in range(n_dev):
        rows[:, j * width:(j + 1) * width] = hid[0, j]
    for cp in mlp_copies:
        cp.wait()
    rows_n = rms_rows(rows[...].astype(F32), gain2_ref[...].astype(F32))
    mids = []
    for g_ref, u_ref in zip(gate_w, up_w):
        gate = dot_f32(rows_n, g_ref[...])
        mids.append((gate * (1.0 / (1.0 + jnp.exp(-gate))) * dot_f32(rows_n, u_ref[...])).astype(BF16))
    mid = jnp.concatenate(mids, axis=1)
    for j, d_ref in enumerate(down_w):
        part[1, :, j * block:(j + 1) * block] = dot_f32(mid, d_ref[...])
    add_partials(1)
    send_kv(len(waiting))
    for j in range(n_dev):
        dec_out[:, j * width:(j + 1) * width] = hid[1, j, 0:n_batch, :]
        last_out[:, j * width:(j + 1) * width] = hid[1, j, n_batch:2 * n_batch, :]

    for cp in xsends:
        cp.wait_send()
    wait_bytes(psend, p_sem.at[0])
    for index, refs in enumerate(((lgot, lrecv.at[pl.ds(0, n_chip - 1)]), (got.at[0], far_got.at[0], comb.at[0]), (got.at[1], far_got.at[1], comb.at[1]))):
        for i, ref in enumerate(refs):
            wait_bytes(ref, sum_sem.at[index, 2 * i])
    for index, buf in enumerate((lcols, qall, hid.at[0], hid.at[1])):
        wait_bytes(buf.at[pl.ds(0, 2 if index else n_chip - 1)], all_sem.at[index, 0])
        wait_bytes(buf.at[pl.ds(0, n_chip)], all_sem.at[index, 2])
        if index:
            wait_bytes(buf.at[0], all_sem.at[index, 4])
    for kv in range(2):
        wait_bytes(outs[kv].at[pl.ds(0, 3 * n_batch // 4), pl.ds(0, seq_len)], kv_recv_sem.at[kv])
    wait_bytes(stage.at[:, pl.ds(0, 3)], kv_send_sem)


def deliver_kernel(k_in, v_in, d_in, l_in, k_out, v_out, d_out, l_out, sem):
    copies = [pltpu.make_async_copy(src, dst, sem.at[i])
              for i, (src, dst) in enumerate(((k_in, k_out), (v_in, v_out), (d_in, d_out), (l_in, l_out)))]
    for cp in copies:
        cp.start()
    for cp in copies:
        cp.wait()


def rotary_tables(n_pos):
    inv_freq = np.float32(10000.0) ** (-2.0 * np.arange(HEAD_DIM // 2, dtype=np.float32) / HEAD_DIM).astype(np.float32)
    angles = np.arange(n_pos, dtype=np.float32)[:, None] * inv_freq.astype(np.float32)
    cos, sin = np.cos(angles), np.sin(angles)
    return (np.concatenate([cos, cos], axis=1).astype(np.float32), np.concatenate([-sin, sin], axis=1).astype(np.float32))


def solution(mesh):
    n_dev, n_rep = mesh.shape['model'], mesh.shape['replica']
    seq_spec = P('replica', 'model', None)
    col_spec = P(None, None, 'model')
    row_spec = P(None, 'model', None)
    gain_spec = P(None, None)
    tok_spec = P('replica', None)
    cache_spec = P(None, 'replica', None, 'model', None)
    in_specs = (seq_spec, P('replica'), tok_spec, gain_spec, col_spec, col_spec, col_spec, row_spec, gain_spec, col_spec, col_spec, row_spec)
    out_specs = (tok_spec, tok_spec, cache_spec, cache_spec)
    hbm = pl.BlockSpec(memory_space=pl.ANY)
    vmem = pl.BlockSpec(memory_space=pltpu.VMEM)
    smem = pl.BlockSpec(memory_space=pltpu.SMEM)
    dma = pltpu.SemaphoreType.DMA

    def per_device(prompt, lengths, new_tok, norm_attn, w_q, w_k, w_v, w_o, norm_mlp, w_gate, w_up, w_down):
        n_batch, seq_loc, d_model = prompt.shape
        kv_width = w_k.shape[2]
        heads = kv_width // HEAD_DIM
        seq_len = seq_loc * n_dev
        half = n_batch // 2
        n_chunk = half // GROUP
        width = d_model // n_dev
        wq, wk, wv, wo, wg, wu, wd = w_q[0], w_k[0], w_v[0], w_o[0], w_gate[0], w_up[0], w_down[0]
        cos_tab, sin_tab = (jnp.asarray(t) for t in rotary_tables(seq_len + 8))

        ff = wg.shape[1]
        n_q = 4 * half
        cache = jax.ShapeDtypeStruct((n_batch, seq_len + 1, heads, HEAD_DIM), BF16)
        scratch = lambda *shape, dtype=F32: pltpu.VMEM(shape, dtype)
        held = pltpu.VMEM(cache.shape, BF16)
        tail = jax.ShapeDtypeStruct((n_batch, d_model), BF16)
        n_chip = n_dev // 2
        key_cache, val_cache, dec, last = pl.pallas_call(
            functools.partial(layer_kernel, n_dev, n_rep),
            out_shape=(held, held, pltpu.VMEM(tail.shape, BF16), pltpu.VMEM(tail.shape, BF16)),
            in_specs=[smem] + [hbm] * 13,
            out_specs=(vmem,) * 4,
            scratch_shapes=[
                scratch(3, 2, 2, d_model, kv_width, dtype=BF16),
                scratch(d_model, kv_width, dtype=BF16),
                scratch(kv_width, d_model, dtype=BF16),
                scratch(n_batch, seq_loc, d_model, dtype=BF16),
                scratch(2, half, seq_loc, d_model, dtype=BF16),
                scratch(4, 4, 2, half, seq_loc, heads, HEAD_DIM, dtype=BF16),
                scratch(2 * GROUP * seq_loc, HEAD_DIM),
                scratch(n_batch, d_model), scratch(n_chip, n_batch, width),
                scratch(n_chip, n_batch, width), scratch(n_chip, n_batch, width),
                scratch(n_dev, n_batch, width, dtype=BF16),
                scratch(2 * n_batch, HEAD_DIM), scratch(2 * n_batch, HEAD_DIM),
                scratch(2 * n_batch, d_model, dtype=BF16),
                scratch(2 * n_q, HEAD_DIM), scratch(n_dev, 2 * n_q, HEAD_DIM, dtype=BF16),
                scratch(n_batch, heads, HEAD_DIM, dtype=BF16), scratch(n_batch, heads, HEAD_DIM, dtype=BF16),
                scratch(2 * n_q, HEAD_DIM), scratch(2 * n_q, HEAD_DIM),
                scratch(n_q, 2 * half * seq_loc, dtype=jnp.int32),
                scratch(3, 4, 2, n_q, HEAD_DIM), scratch(4, 4, 2, n_q, HEAD_DIM),
                scratch(2 * n_batch, kv_width),
                scratch(2, 2 * n_batch, d_model), scratch(2, n_chip, 2 * n_batch, width),
                scratch(2, n_chip, 2 * n_batch, width), scratch(2, 2, 2 * n_batch, width // 2),
                scratch(2, 2, 2 * n_batch, width), scratch(2, 2, 2 * n_batch, width),
                scratch(2, n_dev, 2 * n_batch, width, dtype=BF16),
                scratch(n_batch, d_model, dtype=BF16), scratch(1, d_model, dtype=BF16), scratch(1, d_model, dtype=BF16),
                scratch(seq_len + 8, HEAD_DIM), scratch(seq_len + 8, HEAD_DIM),
                dma((2 * n_chunk,)), dma((4,)), dma((2, 2, 2)), dma((2, 2, 2)), dma((2, 2)), dma((2, 2, 2)), dma(()), dma((2, 2)),
                dma((2, n_chunk)), dma((2, n_chunk)),
                dma((2,)), dma(()), dma((2,)), dma((3, 6)), dma((4, 6)), dma((16,)), dma((5,)),
            ],
            compiler_params=pltpu.CompilerParams(collective_id=0, has_side_effects=True, vmem_limit_bytes=VMEM_MIB * 2 ** 20),
            name='layer',
        )(*(pltpu.with_memory_space_constraint(a, pltpu.HBM) for a in
            (lengths, prompt, wk, wv, wq, wo, wg, wu, wd, new_tok, norm_attn, norm_mlp, cos_tab, sin_tab)))
        key_cache, val_cache, dec, last = pl.pallas_call(
            deliver_kernel, out_shape=(cache, cache, tail, tail), in_specs=[vmem] * 4, out_specs=(hbm,) * 4,
            scratch_shapes=[dma((4,))], name='deliver',
            compiler_params=pltpu.CompilerParams(vmem_limit_bytes=14 * 2 ** 20),
        )(key_cache, val_cache, dec, last)
        return dec, last, key_cache[None], val_cache[None]

    return jax.shard_map(per_device, mesh=mesh, in_specs=in_specs, out_specs=out_specs, check_vma=False)
```

```python
import functools

import numpy as np

import jax
import jax.numpy as jnp
from jax import lax
from jax.experimental import pallas as pl
from jax.experimental.pallas import tpu as pltpu
from jax.sharding import PartitionSpec as P

HEAD_DIM = 128
NEG_BIG = -1e30
MESH = pl.DeviceIdType.MESH
GROUP = 2
PARTS = 4
VMEM_MIB = 49
LOTS = (8, 1, 3, 2)
BOTH = (0, 1)
F32 = jnp.float32
BF16 = jnp.bfloat16


def dot_f32(lhs, rhs):
    return jnp.dot(lhs, rhs, preferred_element_type=F32)


def rms_rows(rows_f32, gain_f32):
    inv_rms = lax.rsqrt(jnp.mean(rows_f32 * rows_f32, axis=-1, keepdims=True) + 1e-5)
    return (rows_f32 * inv_rms * gain_f32).astype(BF16)


def rope_half(head_f32, cos_t, sin_t):
    return head_f32 * cos_t + pltpu.roll(head_f32, HEAD_DIM // 2, 1) * sin_t


def remote(src, dst, send_sem, recv_sem, dev):
    return pltpu.make_async_remote_copy(src_ref=src, dst_ref=dst, send_sem=send_sem, recv_sem=recv_sem,
                                        device_id={'model': dev}, device_id_type=MESH)


def wait_bytes(ref, sem):
    pltpu.make_async_copy(ref, ref, sem).wait()


def layer_kernel(n_dev, n_rep, len_ref, x_hbm, wk_hbm, wv_hbm, wq_hbm, wo_hbm, wg_hbm, wu_hbm, wd_hbm, tok_hbm, gain_hbm, gain2_hbm, cos_hbm, sin_hbm,
                 kout, vout, dec_out, last_out,
                 wbuf, wq, wo, xown, xrecv, stage, ktmp, lfull, lgot, lpair, lrecv, lcols, crow, srow,
                 rows, qtmp, qall, knew, vnew, kself, vself, near, psend, prec, att, part, got, pair, far_got, comb, recv, hid, tok_ref, gain_ref, gain2_ref, cos_ref, sin_ref,
                 xcopy_sem, wcopy_sem, wrecv_sem, wsend_sem, wown_sem, wfwd_sem, ysend_sem, yrecv_sem, xrecv_sem, xsend_sem,
                 kv_recv_sem, kv_send_sem, p_sem, sum_sem, all_sem, mlp_sem, small_sem):
    n_batch, seq_loc, d_model = xown.shape
    n_chip = n_dev // 2
    half = n_batch // 2
    n_chunk = half // GROUP
    n_all = xcopy_sem.shape[0]
    m_rows = GROUP * seq_loc
    n_row, n_units = rows.shape[0], stage.shape[0]
    seq_len = seq_loc * n_dev
    width = d_model // n_dev
    me = lax.axis_index('model')
    rep = lax.axis_index('replica')
    chip, core = me // 2, lax.rem(me, 2)
    left, right = lax.rem(chip + n_chip - 1, n_chip), lax.rem(chip + 1, n_chip)
    other = 1 - core
    partner = chip * 2 + other

    def same(c):
        return c * 2 + core

    w_hbm = (wk_hbm, wv_hbm)
    outs = (kout, vout)
    owners = (me, me, same(left), same(right))
    firsts = (0, half, 0, half)
    aims = (left, right, right, left)
    slots = (1, 2, 2, 1)
    hops = ((1, right), (2, left))
    sides = ((0, right), (1, left))

    def col(j):
        return pl.ds(pl.multiple_of(j * width, width), width)

    barrier = pltpu.get_barrier_semaphore()
    for off in range(1, n_dev):
        pl.semaphore_signal(barrier, inc=1, device_id={'model': lax.rem(me + off, n_dev)}, device_id_type=MESH)

    @pl.loop(1, n_rep)
    def _(off):
        pl.semaphore_signal(barrier, inc=1, device_id={'replica': lax.rem(rep + off, n_rep)}, device_id_type=MESH)

    small = [pltpu.make_async_copy(src, dst, small_sem.at[i])
             for i, (src, dst) in enumerate(((tok_hbm, tok_ref), (gain_hbm, gain_ref), (gain2_hbm, gain2_ref), (cos_hbm, cos_ref), (sin_hbm, sin_ref)))]
    for cp in small:
        cp.start()
    wlocal = [pltpu.make_async_copy(w_hbm[kv], wbuf.at[0, core, kv], wcopy_sem.at[kv]) for kv in BOTH]
    for cp in wlocal:
        cp.start()

    def xcopy(ch):
        return pltpu.make_async_copy(x_hbm.at[pl.ds(ch * GROUP, GROUP)], xown.at[pl.ds(ch * GROUP, GROUP)], xcopy_sem.at[ch])

    for ch in range(n_all):
        xcopy(ch).start()
    later = [pltpu.make_async_copy(src, dst, wcopy_sem.at[2 + i])
             for i, (src, dst) in enumerate(((wq_hbm, wq), (wo_hbm, wo)))]
    for cp in later:
        cp.start()

    pl.semaphore_wait(barrier, n_dev + n_rep - 2)

    n_sub = 2
    slice_rows = d_model // n_rep
    sub_rows = slice_rows // n_sub

    def w_slice(h):
        return pl.ds(pl.multiple_of(rep * slice_rows + h * sub_rows, sub_rows), sub_rows)

    wsends = []
    for kv in BOTH:
        for h in range(n_sub):
            for slot, aim in hops:
                wsends.append(remote(w_hbm[kv].at[w_slice(h)], wbuf.at[slot, core, kv, w_slice(h)],
                                     wsend_sem.at[slot - 1, kv, h], wrecv_sem.at[slot - 1, kv, h], same(aim)))
        wsends.append(remote(w_hbm[kv], wbuf.at[0, core, kv], wown_sem.at[0, kv], wown_sem.at[1, kv], partner))
    for cp in wsends:
        cp.start()

    def pass_on(kv, h):
        for slot, _ in hops:
            block = wbuf.at[slot, core, kv, w_slice(h)]
            wait_bytes(block, wrecv_sem.at[slot - 1, kv, h])

            @pl.loop(1, n_rep)
            def _(off):
                pltpu.make_async_remote_copy(src_ref=block, dst_ref=block, send_sem=ysend_sem, recv_sem=yrecv_sem.at[slot - 1, kv],
                                             device_id={'replica': lax.rem(rep + off, n_rep)}, device_id_type=MESH).start()

    xsends = []

    def send_rows(ci):
        for side, aim in sides:
            xsends.append(remote(x_hbm.at[pl.ds(side * half + ci * GROUP, GROUP)], xrecv.at[side, pl.ds(ci * GROUP, GROUP)],
                                 xsend_sem.at[side, ci], xrecv_sem.at[side, ci], same(aim)))
            xsends[-1].start()

    opposite = lax.rem(chip + 2, n_chip)
    lane_half = (pl.ds(0, width // 2), pl.ds(width // 2, width // 2))

    def sum_pair(index, full, got_ref):
        for c in range(n_chip):
            remote(full.at[:, col(c * 2 + other)], got_ref.at[c], sum_sem.at[index, 0], sum_sem.at[index, 1], partner).start()

    def other_chips():
        return [lax.rem(chip + off, n_chip) for off in range(1, n_chip)]

    def sum_direct(full, got_ref, pair_ref, recv_ref):
        wait_bytes(got_ref, sum_sem.at[0, 1])
        for c in range(n_chip):
            pair_ref[c] = full[:, col(same(c))] + got_ref[c]
        for c in other_chips():
            remote(pair_ref.at[c], recv_ref.at[chip], sum_sem.at[0, 2], sum_sem.at[0, 3], same(c)).start()
        recv_ref[chip] = pair_ref[chip]

    def gather_direct(buf):
        for c in other_chips():
            remote(buf.at[me], buf.at[me], all_sem.at[0, 0], all_sem.at[0, 1], same(c)).start()
        remote(buf.at[me], buf.at[me], all_sem.at[0, 2], all_sem.at[0, 3], partner).start()

    def gather_direct_end(buf):
        wait_bytes(buf.at[pl.ds(0, n_chip - 1)], all_sem.at[0, 1])
        for c in other_chips():
            remote(buf.at[same(c)], buf.at[same(c)], all_sem.at[0, 2], all_sem.at[0, 3], partner).start()
        wait_bytes(buf.at[pl.ds(0, n_chip)], all_sem.at[0, 3])

    def sum_far(index, full, got_ref, pair_ref, far_ref):
        wait_bytes(got_ref, sum_sem.at[index, 1])
        for c in range(n_chip):
            pair_ref[c] = full[:, col(same(c))] + got_ref[c]
        for side, aim in sides:
            remote(pair_ref.at[opposite, :, lane_half[side]], far_ref.at[side], sum_sem.at[index, 2], sum_sem.at[index, 3], same(aim)).start()

    def sum_near(index, pair_ref, far_ref, comb_ref, recv_ref):
        wait_bytes(far_ref, sum_sem.at[index, 3])
        for side, aim in sides:
            comb_ref[side] = pair_ref[aim]
            comb_ref[side, :, lane_half[side]] = pair_ref[aim, :, lane_half[side]] + far_ref[side]
            remote(comb_ref.at[side], recv_ref.at[side], sum_sem.at[index, 4], sum_sem.at[index, 5], same(aim)).start()

    def sum_end(index, pair_ref, recv_ref):
        wait_bytes(recv_ref, sum_sem.at[index, 5])
        return pair_ref[chip] + recv_ref[0] + recv_ref[1]

    def half_of(ref, side):
        if ref.shape[1] == width:
            return ref.at[:, lane_half[side]]
        return ref.at[pl.ds(side * (ref.shape[0] // 2), ref.shape[0] // 2)]

    def gather(index, buf):
        for aim in (right, left):
            remote(buf.at[me], buf.at[me], all_sem.at[index, 0], all_sem.at[index, 1], same(aim)).start()
        remote(buf.at[me], buf.at[me], all_sem.at[index, 2], all_sem.at[index, 3], partner).start()

    def gather_pass(index, buf):
        wait_bytes(buf.at[pl.ds(0, 2)], all_sem.at[index, 1])
        for side, (source, aim) in enumerate(((left, right), (right, left))):
            slot = buf.at[same(source)]
            remote(half_of(slot, side), half_of(slot, side), all_sem.at[index, 4], all_sem.at[index, 5], same(aim)).start()
            remote(slot, slot, all_sem.at[index, 2], all_sem.at[index, 3], partner).start()

    def gather_end(index, buf):
        wait_bytes(buf.at[0], all_sem.at[index, 5])
        slot = buf.at[same(opposite)]
        remote(slot, slot, all_sem.at[index, 2], all_sem.at[index, 3], partner).start()
        wait_bytes(buf.at[pl.ds(0, n_chip)], all_sem.at[index, 3])

    for cp in small:
        cp.wait()
    gain = gain_ref[...].astype(F32)

    def normalize(ref):
        for g in range(GROUP):
            ref[g] = rms_rows(ref[g].astype(F32), gain)

    def make_kv(rows_ref, unit, ci, owner, b0, slot, kcore, dst):
        mat = rows_ref[...].reshape(m_rows, d_model)
        start = pl.multiple_of(owner * seq_loc, seq_loc)
        cos_t = jnp.concatenate([cos_ref[pl.ds(start, seq_loc), :]] * GROUP, axis=0)
        sin_t = jnp.concatenate([sin_ref[pl.ds(start, seq_loc), :]] * GROUP, axis=0)
        for kv in BOTH:
            acc = dot_f32(mat, wbuf[slot, kcore, kv])
            for h in BOTH:
                head = acc[:, h * HEAD_DIM:(h + 1) * HEAD_DIM]
                if kv == 0:
                    head = rope_half(head, cos_t, sin_t)
                ktmp[pl.ds(h, m_rows, stride=2), :] = head
            piece = stage.at[unit, dst, kv, pl.ds(ci * GROUP, GROUP)]
            made = ktmp[...].astype(BF16)
            piece.reshape(ktmp.shape[0], HEAD_DIM)[...] = made
            if slot == 0 and dst == 3:
                for g in range(GROUP):
                    outs[kv].at[b0 + g, pl.ds(start, seq_loc)].reshape(2 * seq_loc, HEAD_DIM)[...] = \
                        made[g * 2 * seq_loc:(g + 1) * 2 * seq_loc]
            elif slot == 0:
                remote(piece, outs[kv].at[pl.ds(b0, GROUP), pl.ds(start, seq_loc)], kv_send_sem, kv_recv_sem.at[kv], partner).start()

    waiting = [(units, ci, kcore, kv) for units in ((0, 1), (3, 2)) for ci in range(n_chunk) for kcore in BOTH for kv in BOTH]

    def send_kv(count):
        for _ in range(min(count, len(waiting))):
            units, ci, kcore, kv = waiting.pop(0)
            for unit in units:
                start = pl.multiple_of(owners[unit] * seq_loc, seq_loc)
                remote(stage.at[unit, kcore, kv, pl.ds(ci * GROUP, GROUP)],
                       outs[kv].at[pl.ds(firsts[unit] + ci * GROUP, GROUP), pl.ds(start, seq_loc)],
                       kv_send_sem, kv_recv_sem.at[kv], aims[unit] * 2 + kcore).start()

    for cp in wlocal:
        cp.wait()
    base = me * seq_loc

    @pl.loop(0, n_all)
    def _(ch):
        xcopy(ch).wait()
        own = xown.at[pl.ds(ch * GROUP, GROUP)]
        for g in range(GROUP):
            b = ch * GROUP + g
            hit = lax.broadcasted_iota(jnp.int32, (16, seq_loc), 1) == len_ref[b] - 1 - base
            row = dot_f32(jnp.where(hit, 1.0, 0.0).astype(BF16), xown[b])
            lfull[pl.ds(b, 1), :] = row[0:1]
        normalize(own)
        make_kv(own, ch // n_chunk, lax.rem(ch, n_chunk), me, ch * GROUP, 0, core, 3)

    pass_on(0, 0)
    sum_pair(0, lfull, lgot)
    for kv in BOTH:
        wait_bytes(wbuf.at[0, other, kv], wown_sem.at[1, kv])

    @pl.loop(0, n_all)
    def _(ch):
        make_kv(xown.at[pl.ds(ch * GROUP, GROUP)], ch // n_chunk, lax.rem(ch, n_chunk), me, ch * GROUP, 0, other, 2)

        @pl.when(ch == n_chunk - 1)
        def _():
            pass_on(0, 1)
            sum_direct(lfull, lgot, lpair, lrecv)

    send_rows(0)
    pass_on(1, 0)

    far = 1 << 20
    r_idx = lax.broadcasted_iota(jnp.int32, near.shape, 0)
    c_idx = lax.broadcasted_iota(jnp.int32, near.shape, 1)
    match = (c_idx // (2 * seq_loc) == lax.rem(r_idx, half)) & (lax.rem(c_idx, 2) == lax.rem(r_idx // half, 2))
    near[...] = jnp.where(match, lax.rem(c_idx // 2, seq_loc), far)

    pass_on(1, 1)
    wait_bytes(lrecv.at[pl.ds(0, n_chip - 1)], sum_sem.at[0, 3])
    lcols[me] = jnp.sum(lrecv[...], axis=0).astype(BF16)
    gather_direct(lcols)
    send_rows(1)

    def received_own(ci):
        for side in BOTH:
            unit = 2 + side
            rows_ref = xrecv.at[side, pl.ds(ci * GROUP, GROUP)]
            wait_bytes(rows_ref, xrecv_sem.at[side, ci])
            normalize(rows_ref)
            make_kv(rows_ref, unit, ci, owners[unit], firsts[unit] + ci * GROUP, 0, other, 2)
            make_kv(rows_ref, unit, ci, owners[unit], firsts[unit] + ci * GROUP, 0, core, 3)

    def received_far(ci):
        for side in BOTH:
            unit = 2 + side

            @pl.loop(0, 2)
            def _(kcore):
                make_kv(xrecv.at[side, pl.ds(ci * GROUP, GROUP)], unit, ci, owners[unit], firsts[unit] + ci * GROUP, slots[unit], kcore, kcore)

    n_q = 4 * half
    scale = HEAD_DIM ** -0.5
    lane = lax.broadcasted_iota(jnp.int32, (n_q, HEAD_DIM), 1)
    q_row = lax.broadcasted_iota(jnp.int32, (n_q, 1), 0)
    q_len = []
    for s in BOTH:
        vec = jnp.zeros((n_q, 1), jnp.int32)
        for b in range(half):
            vec = jnp.where(lax.rem(q_row, half) == b, len_ref[s * half + b], vec)
        q_len.append(vec)

    def partial_att(unit, dst):
        s = unit % 2
        target = (aims[unit] * 2, aims[unit] * 2 + 1, partner, me)[dst]
        q32 = qall[target, s * n_q:(s + 1) * n_q, :]
        keys = stage.at[unit, dst, 0].reshape(2 * half * seq_loc, HEAD_DIM)[...]
        vals = stage.at[unit, dst, 1].reshape(2 * half * seq_loc, HEAD_DIM)[...]
        scores = lax.dot_general(q32, keys, (((1,), (1,)), ((), ())), preferred_element_type=F32) * scale
        scores = jnp.where(near[...] < q_len[s] - owners[unit] * seq_loc, scores, NEG_BIG)
        top = jnp.max(scores, axis=1, keepdims=True)
        prob = jnp.exp(scores - top)
        total = jnp.sum(prob, axis=1, keepdims=True)
        acc = dot_f32((prob / total).astype(BF16), vals)
        dest = prec.at[3, unit] if dst == 3 else psend.at[dst, unit]
        dest[0] = acc
        dest[1] = jnp.where(lane < HEAD_DIM // 2, top, total)
        if dst == 2:
            remote(psend.at[dst, unit], prec.at[2, unit], p_sem.at[0], p_sem.at[1], partner).start()
        elif dst < 2:
            remote(psend.at[dst, unit], prec.at[core, unit], p_sem.at[0], p_sem.at[1], target).start()

    rows[0:n_batch, :] = tok_ref[...]
    for b in range(n_batch):
        for r in BOTH:
            at = jnp.maximum(len_ref[b] - r, 0)
            crow[pl.ds(r * n_batch + b, 1), :] = cos_ref[pl.ds(at, 1), :]
            srow[pl.ds(r * n_batch + b, 1), :] = sin_ref[pl.ds(at, 1), :]
    later[0].wait()
    received_own(0)
    gather_direct_end(lcols)
    for j in range(n_dev):
        rows[n_batch:n_row, j * width:(j + 1) * width] = lcols[j]
    rows_n = rms_rows(rows[...].astype(F32), gain)
    q_acc = dot_f32(rows_n, wq[...])
    for h in BOTH:
        head = rope_half(q_acc[:, h * HEAD_DIM:(h + 1) * HEAD_DIM], crow[...], srow[...])
        for r in BOTH:
            for s in BOTH:
                qtmp[pl.ds(((s * 2 + r) * 2 + h) * half, half), :] = head[r * n_batch + s * half:r * n_batch + (s + 1) * half]
    qall[me] = qtmp[...].astype(BF16)
    gather(1, qall)
    for ci in range(2, n_chunk - 1):
        send_rows(ci)
    kself[...] = jnp.zeros_like(kself)
    vself[...] = jnp.zeros_like(vself)
    for kv, (new, own) in enumerate(((knew, kself), (vnew, vself))):
        acc = dot_f32(rows_n[0:n_batch], wbuf[0, core, kv])
        for h in BOTH:
            head = acc[:, h * HEAD_DIM:(h + 1) * HEAD_DIM]
            if kv == 0:
                head = rope_half(head, crow[0:n_batch, :], srow[0:n_batch, :])
            ktmp[pl.ds(h, n_batch, stride=2), :] = head
            head = head.astype(BF16).astype(F32)
            for s in BOTH:
                own[pl.ds((s * 4 + h) * half, half), :] = head[s * half:(s + 1) * half]
        new.reshape(n_row, HEAD_DIM)[...] = ktmp[0:n_row, :].astype(BF16)
        for b in range(n_batch):
            outs[kv][b, seq_len] = new[b]

    fwds = []
    for kv in BOTH:
        for slot, _ in hops:
            if n_rep > 1:
                wait_bytes(wbuf.at[slot, core, kv, pl.ds(0, d_model - slice_rows)], yrecv_sem.at[slot - 1, kv])
            fwds.append(remote(wbuf.at[slot, core, kv], wbuf.at[slot, core, kv], wfwd_sem.at[0, slot - 1, kv], wfwd_sem.at[1, slot - 1, kv], partner))
            fwds[-1].start()
    for kv in BOTH:
        for slot, _ in hops:
            wait_bytes(wbuf.at[slot, other, kv], wfwd_sem.at[1, slot - 1, kv])

    @pl.loop(0, n_chunk)
    def _(ci):
        @pl.loop(0, 2)
        def _(kcore):
            for unit in BOTH:
                make_kv(xown.at[pl.ds(firsts[unit] + ci * GROUP, GROUP)], unit, ci, me, firsts[unit] + ci * GROUP, slots[unit], kcore, kcore)

    gather_pass(1, qall)
    send_rows(n_chunk - 1)
    send_kv(LOTS[0])

    received_far(0)

    @pl.loop(1, n_chunk)
    def _(ci):
        @pl.when(ci == n_chunk - 1)
        def _():
            gather_end(1, qall)
            for dst in range(n_units):
                for unit in BOTH:
                    partial_att(unit, dst)

        received_own(ci)
        received_far(ci)

    for cp in wsends + fwds:
        cp.wait_send()
    if n_rep > 1:
        for slot, _ in hops:
            wait_bytes(wbuf.at[slot, 0, :, pl.ds(0, d_model - slice_rows)], ysend_sem)
    ff, block = wd_hbm.shape[0], wbuf.shape[4]
    places = [wbuf.at[i // 4, (i // 2) % 2, i % 2] for i in range(12)]
    gate_w, up_w = places[0:4], places[4:8]
    down_w = [places[8 + i // 2].at[pl.ds((i % 2) * ff, ff)] for i in range(8)]
    mlp_copies = []
    for i, (src, dsts) in enumerate(((wg_hbm, gate_w), (wu_hbm, up_w), (wd_hbm, down_w))):
        for j, dst in enumerate(dsts):
            mlp_copies.append(pltpu.make_async_copy(src.at[:, pl.ds(j * block, block)], dst, mlp_sem.at[i * 4 + j]))
            mlp_copies[-1].start()

    for dst in range(n_units):
        for unit in range(2, 4):
            partial_att(unit, dst)
        send_kv(LOTS[1])

    wait_bytes(prec.at[pl.ds(0, 3)], p_sem.at[1])
    for s in BOTH:
        q32 = qall[me, s * n_q:(s + 1) * n_q, :].astype(F32)
        is_new = q_row < n_q // 2
        self_score = jnp.sum(q32 * kself[s * n_q:(s + 1) * n_q, :], axis=1, keepdims=True) * scale
        tops = [jnp.where(is_new, self_score, NEG_BIG)]
        sums = [jnp.where(is_new, 1.0, 0.0)]
        accs = [vself[s * n_q:(s + 1) * n_q, :]]
        for unit in (s, s + 2):
            for src in range(n_units):
                stat = prec[src, unit, 1]
                tops.append(stat[:, 0:1])
                sums.append(stat[:, HEAD_DIM // 2:HEAD_DIM // 2 + 1])
                accs.append(prec[src, unit, 0])
        top = functools.reduce(jnp.maximum, tops)
        facs = [jnp.exp(t - top) for t in tops]
        facs = [f * l for f, l in zip(facs, sums)]
        total = sum(facs)
        merged = sum((f / total) * a for f, a in zip(facs, accs))
        for r in BOTH:
            for h in BOTH:
                att[r * n_batch + s * half:r * n_batch + (s + 1) * half, h * HEAD_DIM:(h + 1) * HEAD_DIM] = \
                    merged[(r * 2 + h) * half:(r * 2 + h + 1) * half]

    def add_partials(step):
        sum_pair(1 + step, part.at[step], got.at[step])
        sum_far(1 + step, part.at[step], got.at[step], pair.at[step], far_got.at[step])
        send_kv(LOTS[2 + step])
        sum_near(1 + step, pair.at[step], far_got.at[step], comb.at[step], recv.at[step])
        send_kv(LOTS[2 + step])
        mine = rows[:, col(me)].astype(F32)
        hid[step, me] = (mine + sum_end(1 + step, pair.at[step], recv.at[step])).astype(BF16)
        gather(2 + step, hid.at[step])
        send_kv(LOTS[2 + step])
        gather_pass(2 + step, hid.at[step])
        send_kv(LOTS[2 + step])
        gather_end(2 + step, hid.at[step])

    later[1].wait()
    part[0] = dot_f32(att[...].astype(BF16), wo[...])
    add_partials(0)
    for j in range(n_dev):
        rows[:, j * width:(j + 1) * width] = hid[0, j]
    for cp in mlp_copies:
        cp.wait()
    rows_n = rms_rows(rows[...].astype(F32), gain2_ref[...].astype(F32))
    mids = []
    for g_ref, u_ref in zip(gate_w, up_w):
        gate = dot_f32(rows_n, g_ref[...])
        mids.append((gate * (1.0 / (1.0 + jnp.exp(-gate))) * dot_f32(rows_n, u_ref[...])).astype(BF16))
    mid = jnp.concatenate(mids, axis=1)
    for j, d_ref in enumerate(down_w):
        part[1, :, j * block:(j + 1) * block] = dot_f32(mid, d_ref[...])
    add_partials(1)
    send_kv(len(waiting))
    for j in range(n_dev):
        dec_out[:, j * width:(j + 1) * width] = hid[1, j, 0:n_batch, :]
        last_out[:, j * width:(j + 1) * width] = hid[1, j, n_batch:n_row, :]

    for cp in xsends:
        cp.wait_send()
    wait_bytes(psend, p_sem.at[0])
    for index, refs in enumerate(((lgot, lrecv.at[pl.ds(0, n_chip - 1)]), (got.at[0], far_got.at[0], comb.at[0]), (got.at[1], far_got.at[1], comb.at[1]))):
        for i, ref in enumerate(refs):
            wait_bytes(ref, sum_sem.at[index, 2 * i])
    for index, buf in enumerate((lcols, qall, hid.at[0], hid.at[1])):
        wait_bytes(buf.at[pl.ds(0, 2 if index else n_chip - 1)], all_sem.at[index, 0])
        wait_bytes(buf.at[pl.ds(0, n_chip)], all_sem.at[index, 2])
        if index:
            wait_bytes(buf.at[0], all_sem.at[index, 4])
    for kv in BOTH:
        wait_bytes(outs[kv].at[pl.ds(0, 3 * n_batch // 4), pl.ds(0, seq_len)], kv_recv_sem.at[kv])
    wait_bytes(stage.at[:, pl.ds(0, 3)], kv_send_sem)


def deliver_kernel(k_in, v_in, d_in, l_in, k_out, v_out, d_out, l_out, sem):
    part = k_in.shape[0] // PARTS
    pairs = [(src.at[pl.ds(i * part, part)], dst.at[pl.ds(i * part, part)]) for i in range(PARTS) for src, dst in ((k_in, k_out), (v_in, v_out))]
    copies = [pltpu.make_async_copy(src, dst, sem.at[i]) for i, (src, dst) in enumerate(pairs + [(d_in, d_out), (l_in, l_out)])]
    for cp in copies:
        cp.start()
    for cp in copies:
        cp.wait()


def rotary_tables(n_pos):
    inv_freq = np.float32(10000.0) ** (-2.0 * np.arange(HEAD_DIM // 2, dtype=np.float32) / HEAD_DIM).astype(np.float32)
    angles = np.arange(n_pos, dtype=np.float32)[:, None] * inv_freq.astype(np.float32)
    cos, sin = np.cos(angles), np.sin(angles)
    return (np.concatenate([cos, cos], axis=1).astype(np.float32), np.concatenate([-sin, sin], axis=1).astype(np.float32))


def solution(mesh):
    n_dev, n_rep = mesh.shape['model'], mesh.shape['replica']
    seq_spec = P('replica', 'model', None)
    col_spec = P(None, None, 'model')
    row_spec = P(None, 'model', None)
    gain_spec = P(None, None)
    tok_spec = P('replica', None)
    cache_spec = P(None, 'replica', None, 'model', None)
    in_specs = (seq_spec, P('replica'), tok_spec, gain_spec, col_spec, col_spec, col_spec, row_spec, gain_spec, col_spec, col_spec, row_spec)
    out_specs = (tok_spec, tok_spec, cache_spec, cache_spec)
    hbm = pl.BlockSpec(memory_space=pl.ANY)
    vmem = pl.BlockSpec(memory_space=pltpu.VMEM)
    smem = pl.BlockSpec(memory_space=pltpu.SMEM)
    dma = pltpu.SemaphoreType.DMA

    def per_device(prompt, lengths, new_tok, norm_attn, w_q, w_k, w_v, w_o, norm_mlp, w_gate, w_up, w_down):
        n_batch, seq_loc, d_model = prompt.shape
        kv_width = w_k.shape[2]
        heads = kv_width // HEAD_DIM
        seq_len = seq_loc * n_dev
        half = n_batch // 2
        n_chunk = half // GROUP
        width = d_model // n_dev
        wq, wk, wv, wo, wg, wu, wd = w_q[0], w_k[0], w_v[0], w_o[0], w_gate[0], w_up[0], w_down[0]
        cos_tab, sin_tab = (jnp.asarray(t) for t in rotary_tables(seq_len + 8))

        ff = wg.shape[1]
        n_q, n_row, two = 4 * half, 2 * n_batch, dma((2,))
        cache = jax.ShapeDtypeStruct((n_batch, seq_len + 1, heads, HEAD_DIM), BF16)
        cube, square, chunked = dma((2, 2, 2)), dma((2, 2)), dma((2, n_chunk))
        scratch = lambda *shape, dtype=F32: pltpu.VMEM(shape, dtype)
        held = pltpu.VMEM(cache.shape, BF16)
        tail = jax.ShapeDtypeStruct((n_batch, d_model), BF16)
        n_chip = n_dev // 2
        key_cache, val_cache, dec, last = pl.pallas_call(
            functools.partial(layer_kernel, n_dev, n_rep),
            out_shape=(held, held, pltpu.VMEM(tail.shape, BF16), pltpu.VMEM(tail.shape, BF16)),
            in_specs=[smem] + [hbm] * 13,
            out_specs=(vmem,) * 4,
            scratch_shapes=[
                scratch(3, 2, 2, d_model, kv_width, dtype=BF16),
                scratch(d_model, kv_width, dtype=BF16),
                scratch(kv_width, d_model, dtype=BF16),
                scratch(n_batch, seq_loc, d_model, dtype=BF16),
                scratch(2, half, seq_loc, d_model, dtype=BF16),
                scratch(4, 4, 2, half, seq_loc, heads, HEAD_DIM, dtype=BF16),
                scratch(2 * GROUP * seq_loc, HEAD_DIM),
                scratch(n_batch, d_model), scratch(n_chip, n_batch, width),
                scratch(n_chip, n_batch, width), scratch(n_chip, n_batch, width),
                scratch(n_dev, n_batch, width, dtype=BF16),
                scratch(n_row, HEAD_DIM), scratch(n_row, HEAD_DIM),
                scratch(n_row, d_model, dtype=BF16),
                scratch(2 * n_q, HEAD_DIM), scratch(n_dev, 2 * n_q, HEAD_DIM, dtype=BF16),
                scratch(n_batch, heads, HEAD_DIM, dtype=BF16), scratch(n_batch, heads, HEAD_DIM, dtype=BF16),
                scratch(2 * n_q, HEAD_DIM), scratch(2 * n_q, HEAD_DIM),
                scratch(n_q, 2 * half * seq_loc, dtype=jnp.int32),
                scratch(3, 4, 2, n_q, HEAD_DIM), scratch(4, 4, 2, n_q, HEAD_DIM),
                scratch(n_row, kv_width),
                scratch(2, n_row, d_model), scratch(2, n_chip, n_row, width),
                scratch(2, n_chip, n_row, width), scratch(2, 2, n_row, width // 2),
                scratch(2, 2, n_row, width), scratch(2, 2, n_row, width),
                scratch(2, n_dev, n_row, width, dtype=BF16),
                scratch(n_batch, d_model, dtype=BF16), scratch(1, d_model, dtype=BF16), scratch(1, d_model, dtype=BF16),
                scratch(seq_len + 8, HEAD_DIM), scratch(seq_len + 8, HEAD_DIM),
                dma((2 * n_chunk,)), dma((4,)), cube, cube, square, cube, dma(()), square,
                chunked, chunked,
                two, dma(()), two, dma((3, 6)), dma((4, 6)), dma((16,)), dma((5,)),
            ],
            compiler_params=pltpu.CompilerParams(collective_id=0, has_side_effects=True, vmem_limit_bytes=VMEM_MIB * 2 ** 20),
            name='layer',
        )(*(pltpu.with_memory_space_constraint(a, pltpu.HBM) for a in
            (lengths, prompt, wk, wv, wq, wo, wg, wu, wd, new_tok, norm_attn, norm_mlp, cos_tab, sin_tab)))
        key_cache, val_cache, dec, last = pl.pallas_call(
            deliver_kernel, out_shape=(cache, cache, tail, tail), in_specs=[vmem] * 4, out_specs=(hbm,) * 4,
            scratch_shapes=[dma((2 * PARTS + 2,))], name='deliver',
            compiler_params=pltpu.CompilerParams(vmem_limit_bytes=14 * 2 ** 20),
        )(key_cache, val_cache, dec, last)
        return dec, last, key_cache[None], val_cache[None]

    return jax.shard_map(per_device, mesh=mesh, in_specs=in_specs, out_specs=out_specs, check_vma=False)
```

```python
import functools

import numpy as np

import jax
import jax.numpy as jnp
from jax import lax
from jax.experimental import pallas as pl
from jax.experimental.pallas import tpu as pltpu
from jax.sharding import PartitionSpec as P

HEAD_DIM = 128
NEG_BIG = -1e30
MESH = pl.DeviceIdType.MESH
GROUP = 2
PARTS = 4
VMEM_MIB = 49
LOTS = (8, 1, 3, 2)
BOTH = (0, 1)
F32 = jnp.float32
BF16 = jnp.bfloat16


def dot_f32(lhs, rhs):
    return jnp.dot(lhs, rhs, preferred_element_type=F32)


def rms_rows(rows_f32, gain_f32):
    inv_rms = lax.rsqrt(jnp.mean(rows_f32 * rows_f32, axis=-1, keepdims=True) + 1e-5)
    return (rows_f32 * inv_rms * gain_f32).astype(BF16)


def rope_half(head_f32, cos_t, sin_t):
    return head_f32 * cos_t + pltpu.roll(head_f32, HEAD_DIM // 2, 1) * sin_t


def remote(src, dst, send_sem, recv_sem, dev):
    return pltpu.make_async_remote_copy(src_ref=src, dst_ref=dst, send_sem=send_sem, recv_sem=recv_sem,
                                        device_id={'model': dev}, device_id_type=MESH)


def wait_bytes(ref, sem):
    pltpu.make_async_copy(ref, ref, sem).wait()


def layer_kernel(n_dev, n_pair, len_ref, x_hbm, wk_hbm, wv_hbm, wq_hbm, wo_hbm, wg_hbm, wu_hbm, wd_hbm, tok_hbm, gain_hbm, gain2_hbm, cos_hbm, sin_hbm,
                 kout, vout, dec_out, last_out,
                 wbuf, wq, wo, xown, xrecv, stage, ktmp, lfull, lgot, lpair, lrecv, lcols, crow, srow,
                 rows, qtmp, qall, knew, vnew, kself, vself, near, psend, prec, att, part, got, pair, far_got, comb, recv, hid, tok_ref, gain_ref, gain2_ref, cos_ref, sin_ref,
                 xcopy_sem, wcopy_sem, wrecv_sem, wsend_sem, wown_sem, wfwd_sem, ysend_sem, yrecv_sem, xrecv_sem, xsend_sem,
                 kv_recv_sem, kv_send_sem, p_sem, sum_sem, all_sem, mlp_sem, small_sem):
    n_batch, seq_loc, d_model = xown.shape
    n_chip = n_dev // 2
    half = n_batch // 2
    n_chunk = half // GROUP
    n_all = xcopy_sem.shape[0]
    m_rows = GROUP * seq_loc
    n_row, n_units = rows.shape[0], stage.shape[0]
    seq_len = seq_loc * n_dev
    width = d_model // n_dev
    me = lax.axis_index('model')
    rep = lax.axis_index('replica')
    turn = lax.rem(rep, n_pair)
    twin = rep + 1 - 2 * turn
    chip, core = me // 2, lax.rem(me, 2)
    left, right = lax.rem(chip + n_chip - 1, n_chip), lax.rem(chip + 1, n_chip)
    other = 1 - core
    partner = chip * 2 + other

    def same(c):
        return c * 2 + core

    w_hbm = (wk_hbm, wv_hbm)
    outs = (kout, vout)
    owners = (me, me, same(left), same(right))
    firsts = (0, half, 0, half)
    aims = (left, right, right, left)
    slots = (1, 2, 2, 1)
    hops = ((1, right), (2, left))
    sides = ((0, right), (1, left))

    def col(j):
        return pl.ds(pl.multiple_of(j * width, width), width)

    barrier = pltpu.get_barrier_semaphore()
    for off in range(1, n_dev):
        pl.semaphore_signal(barrier, inc=1, device_id={'model': lax.rem(me + off, n_dev)}, device_id_type=MESH)

    if n_pair > 1:
        pl.semaphore_signal(barrier, inc=1, device_id={'replica': twin}, device_id_type=MESH)

    small = [pltpu.make_async_copy(src, dst, small_sem.at[i])
             for i, (src, dst) in enumerate(((tok_hbm, tok_ref), (gain_hbm, gain_ref), (gain2_hbm, gain2_ref), (cos_hbm, cos_ref), (sin_hbm, sin_ref)))]
    for cp in small:
        cp.start()
    wlocal = [pltpu.make_async_copy(w_hbm[kv], wbuf.at[0, core, kv], wcopy_sem.at[kv]) for kv in BOTH]
    for cp in wlocal:
        cp.start()

    def xcopy(ch):
        return pltpu.make_async_copy(x_hbm.at[pl.ds(ch * GROUP, GROUP)], xown.at[pl.ds(ch * GROUP, GROUP)], xcopy_sem.at[ch])

    for ch in range(n_all):
        xcopy(ch).start()
    later = [pltpu.make_async_copy(src, dst, wcopy_sem.at[2 + i])
             for i, (src, dst) in enumerate(((wq_hbm, wq), (wo_hbm, wo)))]
    for cp in later:
        cp.start()

    pl.semaphore_wait(barrier, n_dev + n_pair - 2)

    n_sub = 2
    slice_rows = d_model // n_pair
    sub_rows = slice_rows // n_sub

    def w_slice(h):
        return pl.ds(pl.multiple_of(turn * slice_rows + h * sub_rows, sub_rows), sub_rows)

    wsends = []
    for kv in BOTH:
        for h in range(n_sub):
            for slot, aim in hops:
                wsends.append(remote(w_hbm[kv].at[w_slice(h)], wbuf.at[slot, core, kv, w_slice(h)],
                                     wsend_sem.at[slot - 1, kv, h], wrecv_sem.at[slot - 1, kv, h], same(aim)))
        wsends.append(remote(w_hbm[kv], wbuf.at[0, core, kv], wown_sem.at[0, kv], wown_sem.at[1, kv], partner))
    for cp in wsends:
        cp.start()

    def pass_on(kv, h):
        for slot, _ in hops:
            block = wbuf.at[slot, core, kv, w_slice(h)]
            wait_bytes(block, wrecv_sem.at[slot - 1, kv, h])

            if n_pair > 1:
                pltpu.make_async_remote_copy(src_ref=block, dst_ref=block, send_sem=ysend_sem, recv_sem=yrecv_sem.at[slot - 1, kv],
                                             device_id={'replica': twin}, device_id_type=MESH).start()

    xsends = []

    def send_rows(ci):
        for side, aim in sides:
            xsends.append(remote(x_hbm.at[pl.ds(side * half + ci * GROUP, GROUP)], xrecv.at[side, pl.ds(ci * GROUP, GROUP)],
                                 xsend_sem.at[side, ci], xrecv_sem.at[side, ci], same(aim)))
            xsends[-1].start()

    opposite = lax.rem(chip + 2, n_chip)
    lane_half = (pl.ds(0, width // 2), pl.ds(width // 2, width // 2))

    def sum_pair(index, full, got_ref):
        for c in range(n_chip):
            remote(full.at[:, col(c * 2 + other)], got_ref.at[c], sum_sem.at[index, 0], sum_sem.at[index, 1], partner).start()

    def other_chips():
        return [lax.rem(chip + off, n_chip) for off in range(1, n_chip)]

    def sum_direct(full, got_ref, pair_ref, recv_ref):
        wait_bytes(got_ref, sum_sem.at[0, 1])
        for c in range(n_chip):
            pair_ref[c] = full[:, col(same(c))] + got_ref[c]
        for c in other_chips():
            remote(pair_ref.at[c], recv_ref.at[chip], sum_sem.at[0, 2], sum_sem.at[0, 3], same(c)).start()
        recv_ref[chip] = pair_ref[chip]

    def gather_direct(buf):
        for c in other_chips():
            remote(buf.at[me], buf.at[me], all_sem.at[0, 0], all_sem.at[0, 1], same(c)).start()
        remote(buf.at[me], buf.at[me], all_sem.at[0, 2], all_sem.at[0, 3], partner).start()

    def gather_direct_end(buf):
        wait_bytes(buf.at[pl.ds(0, n_chip - 1)], all_sem.at[0, 1])
        for c in other_chips():
            remote(buf.at[same(c)], buf.at[same(c)], all_sem.at[0, 2], all_sem.at[0, 3], partner).start()
        wait_bytes(buf.at[pl.ds(0, n_chip)], all_sem.at[0, 3])

    def sum_far(index, full, got_ref, pair_ref, far_ref):
        wait_bytes(got_ref, sum_sem.at[index, 1])
        for c in range(n_chip):
            pair_ref[c] = full[:, col(same(c))] + got_ref[c]
        for side, aim in sides:
            remote(pair_ref.at[opposite, :, lane_half[side]], far_ref.at[side], sum_sem.at[index, 2], sum_sem.at[index, 3], same(aim)).start()

    def sum_near(index, pair_ref, far_ref, comb_ref, recv_ref):
        wait_bytes(far_ref, sum_sem.at[index, 3])
        for side, aim in sides:
            comb_ref[side] = pair_ref[aim]
            comb_ref[side, :, lane_half[side]] = pair_ref[aim, :, lane_half[side]] + far_ref[side]
            remote(comb_ref.at[side], recv_ref.at[side], sum_sem.at[index, 4], sum_sem.at[index, 5], same(aim)).start()

    def sum_end(index, pair_ref, recv_ref):
        wait_bytes(recv_ref, sum_sem.at[index, 5])
        return pair_ref[chip] + recv_ref[0] + recv_ref[1]

    def half_of(ref, side):
        if ref.shape[1] == width:
            return ref.at[:, lane_half[side]]
        return ref.at[pl.ds(side * (ref.shape[0] // 2), ref.shape[0] // 2)]

    def gather(index, buf):
        for aim in (right, left):
            remote(buf.at[me], buf.at[me], all_sem.at[index, 0], all_sem.at[index, 1], same(aim)).start()
        remote(buf.at[me], buf.at[me], all_sem.at[index, 2], all_sem.at[index, 3], partner).start()

    def gather_pass(index, buf):
        wait_bytes(buf.at[pl.ds(0, 2)], all_sem.at[index, 1])
        for side, (source, aim) in enumerate(((left, right), (right, left))):
            slot = buf.at[same(source)]
            remote(half_of(slot, side), half_of(slot, side), all_sem.at[index, 4], all_sem.at[index, 5], same(aim)).start()
            remote(slot, slot, all_sem.at[index, 2], all_sem.at[index, 3], partner).start()

    def gather_end(index, buf):
        wait_bytes(buf.at[0], all_sem.at[index, 5])
        slot = buf.at[same(opposite)]
        remote(slot, slot, all_sem.at[index, 2], all_sem.at[index, 3], partner).start()
        wait_bytes(buf.at[pl.ds(0, n_chip)], all_sem.at[index, 3])

    for cp in small:
        cp.wait()
    gain = gain_ref[...].astype(F32)

    def normalize(ref):
        for g in range(GROUP):
            ref[g] = rms_rows(ref[g].astype(F32), gain)

    def make_kv(rows_ref, unit, ci, owner, b0, slot, kcore, dst):
        mat = rows_ref[...].reshape(m_rows, d_model)
        start = pl.multiple_of(owner * seq_loc, seq_loc)
        cos_t = jnp.concatenate([cos_ref[pl.ds(start, seq_loc), :]] * GROUP, axis=0)
        sin_t = jnp.concatenate([sin_ref[pl.ds(start, seq_loc), :]] * GROUP, axis=0)
        for kv in BOTH:
            acc = dot_f32(mat, wbuf[slot, kcore, kv])
            for h in BOTH:
                head = acc[:, h * HEAD_DIM:(h + 1) * HEAD_DIM]
                if kv == 0:
                    head = rope_half(head, cos_t, sin_t)
                ktmp[pl.ds(h, m_rows, stride=2), :] = head
            piece = stage.at[unit, dst, kv, pl.ds(ci * GROUP, GROUP)]
            made = ktmp[...].astype(BF16)
            piece.reshape(ktmp.shape[0], HEAD_DIM)[...] = made
            if slot == 0 and dst == 3:
                for g in range(GROUP):
                    outs[kv].at[b0 + g, pl.ds(start, seq_loc)].reshape(2 * seq_loc, HEAD_DIM)[...] = \
                        made[g * 2 * seq_loc:(g + 1) * 2 * seq_loc]
            elif slot == 0:
                remote(piece, outs[kv].at[pl.ds(b0, GROUP), pl.ds(start, seq_loc)], kv_send_sem, kv_recv_sem.at[kv], partner).start()

    waiting = [(units, ci, kcore, kv) for units in ((0, 1), (3, 2)) for ci in range(n_chunk) for kcore in BOTH for kv in BOTH]

    def send_kv(count):
        for _ in range(min(count, len(waiting))):
            units, ci, kcore, kv = waiting.pop(0)
            for unit in units:
                start = pl.multiple_of(owners[unit] * seq_loc, seq_loc)
                remote(stage.at[unit, kcore, kv, pl.ds(ci * GROUP, GROUP)],
                       outs[kv].at[pl.ds(firsts[unit] + ci * GROUP, GROUP), pl.ds(start, seq_loc)],
                       kv_send_sem, kv_recv_sem.at[kv], aims[unit] * 2 + kcore).start()

    for cp in wlocal:
        cp.wait()
    base = me * seq_loc

    @pl.loop(0, n_all)
    def _(ch):
        xcopy(ch).wait()
        own = xown.at[pl.ds(ch * GROUP, GROUP)]
        for g in range(GROUP):
            b = ch * GROUP + g
            hit = lax.broadcasted_iota(jnp.int32, (16, seq_loc), 1) == len_ref[b] - 1 - base
            row = dot_f32(jnp.where(hit, 1.0, 0.0).astype(BF16), xown[b])
            lfull[pl.ds(b, 1), :] = row[0:1]
        normalize(own)
        make_kv(own, ch // n_chunk, lax.rem(ch, n_chunk), me, ch * GROUP, 0, core, 3)

    pass_on(0, 0)
    sum_pair(0, lfull, lgot)
    for kv in BOTH:
        wait_bytes(wbuf.at[0, other, kv], wown_sem.at[1, kv])

    @pl.loop(0, n_all)
    def _(ch):
        make_kv(xown.at[pl.ds(ch * GROUP, GROUP)], ch // n_chunk, lax.rem(ch, n_chunk), me, ch * GROUP, 0, other, 2)

        @pl.when(ch == n_chunk - 1)
        def _():
            pass_on(0, 1)
            sum_direct(lfull, lgot, lpair, lrecv)

    send_rows(0)
    pass_on(1, 0)

    far = 1 << 20
    r_idx = lax.broadcasted_iota(jnp.int32, near.shape, 0)
    c_idx = lax.broadcasted_iota(jnp.int32, near.shape, 1)
    match = (c_idx // (2 * seq_loc) == lax.rem(r_idx, half)) & (lax.rem(c_idx, 2) == lax.rem(r_idx // half, 2))
    near[...] = jnp.where(match, lax.rem(c_idx // 2, seq_loc), far)

    pass_on(1, 1)
    wait_bytes(lrecv.at[pl.ds(0, n_chip - 1)], sum_sem.at[0, 3])
    lcols[me] = jnp.sum(lrecv[...], axis=0).astype(BF16)
    gather_direct(lcols)
    send_rows(1)

    def received_own(ci):
        for side in BOTH:
            unit = 2 + side
            rows_ref = xrecv.at[side, pl.ds(ci * GROUP, GROUP)]
            wait_bytes(rows_ref, xrecv_sem.at[side, ci])
            normalize(rows_ref)
            make_kv(rows_ref, unit, ci, owners[unit], firsts[unit] + ci * GROUP, 0, other, 2)
            make_kv(rows_ref, unit, ci, owners[unit], firsts[unit] + ci * GROUP, 0, core, 3)

    def received_far(ci):
        for side in BOTH:
            unit = 2 + side

            @pl.loop(0, 2)
            def _(kcore):
                make_kv(xrecv.at[side, pl.ds(ci * GROUP, GROUP)], unit, ci, owners[unit], firsts[unit] + ci * GROUP, slots[unit], kcore, kcore)

    n_q = 4 * half
    scale = HEAD_DIM ** -0.5
    lane = lax.broadcasted_iota(jnp.int32, (n_q, HEAD_DIM), 1)
    q_row = lax.broadcasted_iota(jnp.int32, (n_q, 1), 0)
    q_len = []
    for s in BOTH:
        vec = jnp.zeros((n_q, 1), jnp.int32)
        for b in range(half):
            vec = jnp.where(lax.rem(q_row, half) == b, len_ref[s * half + b], vec)
        q_len.append(vec)

    def partial_att(unit, dst):
        s = unit % 2
        target = (aims[unit] * 2, aims[unit] * 2 + 1, partner, me)[dst]
        q32 = qall[target, s * n_q:(s + 1) * n_q, :]
        keys = stage.at[unit, dst, 0].reshape(2 * half * seq_loc, HEAD_DIM)[...]
        vals = stage.at[unit, dst, 1].reshape(2 * half * seq_loc, HEAD_DIM)[...]
        scores = lax.dot_general(q32, keys, (((1,), (1,)), ((), ())), preferred_element_type=F32) * scale
        scores = jnp.where(near[...] < q_len[s] - owners[unit] * seq_loc, scores, NEG_BIG)
        top = jnp.max(scores, axis=1, keepdims=True)
        prob = jnp.exp(scores - top)
        total = jnp.sum(prob, axis=1, keepdims=True)
        acc = dot_f32((prob / total).astype(BF16), vals)
        dest = prec.at[3, unit] if dst == 3 else psend.at[dst, unit]
        dest[0] = acc
        dest[1] = jnp.where(lane < HEAD_DIM // 2, top, total)
        if dst == 2:
            remote(psend.at[dst, unit], prec.at[2, unit], p_sem.at[0], p_sem.at[1], partner).start()
        elif dst < 2:
            remote(psend.at[dst, unit], prec.at[core, unit], p_sem.at[0], p_sem.at[1], target).start()

    rows[0:n_batch, :] = tok_ref[...]
    for b in range(n_batch):
        for r in BOTH:
            at = jnp.maximum(len_ref[b] - r, 0)
            crow[pl.ds(r * n_batch + b, 1), :] = cos_ref[pl.ds(at, 1), :]
            srow[pl.ds(r * n_batch + b, 1), :] = sin_ref[pl.ds(at, 1), :]
    later[0].wait()
    received_own(0)
    gather_direct_end(lcols)
    for j in range(n_dev):
        rows[n_batch:n_row, j * width:(j + 1) * width] = lcols[j]
    rows_n = rms_rows(rows[...].astype(F32), gain)
    q_acc = dot_f32(rows_n, wq[...])
    for h in BOTH:
        head = rope_half(q_acc[:, h * HEAD_DIM:(h + 1) * HEAD_DIM], crow[...], srow[...])
        for r in BOTH:
            for s in BOTH:
                qtmp[pl.ds(((s * 2 + r) * 2 + h) * half, half), :] = head[r * n_batch + s * half:r * n_batch + (s + 1) * half]
    qall[me] = qtmp[...].astype(BF16)
    gather(1, qall)
    for ci in range(2, n_chunk - 1):
        send_rows(ci)
    kself[...] = jnp.zeros_like(kself)
    vself[...] = jnp.zeros_like(vself)
    for kv, (new, own) in enumerate(((knew, kself), (vnew, vself))):
        acc = dot_f32(rows_n[0:n_batch], wbuf[0, core, kv])
        for h in BOTH:
            head = acc[:, h * HEAD_DIM:(h + 1) * HEAD_DIM]
            if kv == 0:
                head = rope_half(head, crow[0:n_batch, :], srow[0:n_batch, :])
            ktmp[pl.ds(h, n_batch, stride=2), :] = head
            head = head.astype(BF16).astype(F32)
            for s in BOTH:
                own[pl.ds((s * 4 + h) * half, half), :] = head[s * half:(s + 1) * half]
        new.reshape(n_row, HEAD_DIM)[...] = ktmp[0:n_row, :].astype(BF16)
        for b in range(n_batch):
            outs[kv][b, seq_len] = new[b]

    fwds = []
    for kv in BOTH:
        for slot, _ in hops:
            if n_pair > 1:
                wait_bytes(wbuf.at[slot, core, kv, pl.ds(0, d_model - slice_rows)], yrecv_sem.at[slot - 1, kv])
            fwds.append(remote(wbuf.at[slot, core, kv], wbuf.at[slot, core, kv], wfwd_sem.at[0, slot - 1, kv], wfwd_sem.at[1, slot - 1, kv], partner))
            fwds[-1].start()
    for kv in BOTH:
        for slot, _ in hops:
            wait_bytes(wbuf.at[slot, other, kv], wfwd_sem.at[1, slot - 1, kv])

    @pl.loop(0, n_chunk)
    def _(ci):
        @pl.loop(0, 2)
        def _(kcore):
            for unit in BOTH:
                make_kv(xown.at[pl.ds(firsts[unit] + ci * GROUP, GROUP)], unit, ci, me, firsts[unit] + ci * GROUP, slots[unit], kcore, kcore)

    gather_pass(1, qall)
    send_rows(n_chunk - 1)
    send_kv(LOTS[0])

    received_far(0)

    @pl.loop(1, n_chunk)
    def _(ci):
        @pl.when(ci == n_chunk - 1)
        def _():
            gather_end(1, qall)
            for dst in range(n_units):
                for unit in BOTH:
                    partial_att(unit, dst)

        received_own(ci)
        received_far(ci)

    for cp in wsends + fwds:
        cp.wait_send()
    if n_pair > 1:
        for slot, _ in hops:
            wait_bytes(wbuf.at[slot, 0, :, pl.ds(0, d_model - slice_rows)], ysend_sem)
    ff, block = wd_hbm.shape[0], wbuf.shape[4]
    places = [wbuf.at[i // 4, (i // 2) % 2, i % 2] for i in range(12)]
    gate_w, up_w = places[0:4], places[4:8]
    down_w = [places[8 + i // 2].at[pl.ds((i % 2) * ff, ff)] for i in range(8)]
    mlp_copies = []
    for i, (src, dsts) in enumerate(((wg_hbm, gate_w), (wu_hbm, up_w), (wd_hbm, down_w))):
        for j, dst in enumerate(dsts):
            mlp_copies.append(pltpu.make_async_copy(src.at[:, pl.ds(j * block, block)], dst, mlp_sem.at[i * 4 + j]))
            mlp_copies[-1].start()

    for dst in range(n_units):
        for unit in range(2, 4):
            partial_att(unit, dst)
        send_kv(LOTS[1])

    wait_bytes(prec.at[pl.ds(0, 3)], p_sem.at[1])
    for s in BOTH:
        q32 = qall[me, s * n_q:(s + 1) * n_q, :].astype(F32)
        is_new = q_row < n_q // 2
        self_score = jnp.sum(q32 * kself[s * n_q:(s + 1) * n_q, :], axis=1, keepdims=True) * scale
        tops = [jnp.where(is_new, self_score, NEG_BIG)]
        sums = [jnp.where(is_new, 1.0, 0.0)]
        accs = [vself[s * n_q:(s + 1) * n_q, :]]
        for unit in (s, s + 2):
            for src in range(n_units):
                stat = prec[src, unit, 1]
                tops.append(stat[:, 0:1])
                sums.append(stat[:, HEAD_DIM // 2:HEAD_DIM // 2 + 1])
                accs.append(prec[src, unit, 0])
        top = functools.reduce(jnp.maximum, tops)
        facs = [jnp.exp(t - top) for t in tops]
        facs = [f * l for f, l in zip(facs, sums)]
        total = sum(facs)
        merged = sum((f / total) * a for f, a in zip(facs, accs))
        for r in BOTH:
            for h in BOTH:
                att[r * n_batch + s * half:r * n_batch + (s + 1) * half, h * HEAD_DIM:(h + 1) * HEAD_DIM] = \
                    merged[(r * 2 + h) * half:(r * 2 + h + 1) * half]

    def add_partials(step):
        sum_pair(1 + step, part.at[step], got.at[step])
        sum_far(1 + step, part.at[step], got.at[step], pair.at[step], far_got.at[step])
        send_kv(LOTS[2 + step])
        sum_near(1 + step, pair.at[step], far_got.at[step], comb.at[step], recv.at[step])
        send_kv(LOTS[2 + step])
        mine = rows[:, col(me)].astype(F32)
        hid[step, me] = (mine + sum_end(1 + step, pair.at[step], recv.at[step])).astype(BF16)
        gather(2 + step, hid.at[step])
        send_kv(LOTS[2 + step])
        gather_pass(2 + step, hid.at[step])
        send_kv(LOTS[2 + step])
        gather_end(2 + step, hid.at[step])

    later[1].wait()
    part[0] = dot_f32(att[...].astype(BF16), wo[...])
    add_partials(0)
    for j in range(n_dev):
        rows[:, j * width:(j + 1) * width] = hid[0, j]
    for cp in mlp_copies:
        cp.wait()
    rows_n = rms_rows(rows[...].astype(F32), gain2_ref[...].astype(F32))
    mids = []
    for g_ref, u_ref in zip(gate_w, up_w):
        gate = dot_f32(rows_n, g_ref[...])
        mids.append((gate * (1.0 / (1.0 + jnp.exp(-gate))) * dot_f32(rows_n, u_ref[...])).astype(BF16))
    mid = jnp.concatenate(mids, axis=1)
    for j, d_ref in enumerate(down_w):
        part[1, :, j * block:(j + 1) * block] = dot_f32(mid, d_ref[...])
    add_partials(1)
    send_kv(len(waiting))
    for j in range(n_dev):
        dec_out[:, j * width:(j + 1) * width] = hid[1, j, 0:n_batch, :]
        last_out[:, j * width:(j + 1) * width] = hid[1, j, n_batch:n_row, :]

    for cp in xsends:
        cp.wait_send()
    wait_bytes(psend, p_sem.at[0])
    for index, refs in enumerate(((lgot, lrecv.at[pl.ds(0, n_chip - 1)]), (got.at[0], far_got.at[0], comb.at[0]), (got.at[1], far_got.at[1], comb.at[1]))):
        for i, ref in enumerate(refs):
            wait_bytes(ref, sum_sem.at[index, 2 * i])
    for index, buf in enumerate((lcols, qall, hid.at[0], hid.at[1])):
        wait_bytes(buf.at[pl.ds(0, 2 if index else n_chip - 1)], all_sem.at[index, 0])
        wait_bytes(buf.at[pl.ds(0, n_chip)], all_sem.at[index, 2])
        if index:
            wait_bytes(buf.at[0], all_sem.at[index, 4])
    for kv in BOTH:
        wait_bytes(outs[kv].at[pl.ds(0, 3 * n_batch // 4), pl.ds(0, seq_len)], kv_recv_sem.at[kv])
    wait_bytes(stage.at[:, pl.ds(0, 3)], kv_send_sem)


def deliver_kernel(k_in, v_in, d_in, l_in, k_out, v_out, d_out, l_out, sem):
    part = k_in.shape[0] // PARTS
    pairs = [(src.at[pl.ds(i * part, part)], dst.at[pl.ds(i * part, part)]) for i in range(PARTS) for src, dst in ((k_in, k_out), (v_in, v_out))]
    copies = [pltpu.make_async_copy(src, dst, sem.at[i]) for i, (src, dst) in enumerate(pairs + [(d_in, d_out), (l_in, l_out)])]
    for cp in copies:
        cp.start()
    for cp in copies:
        cp.wait()


def rotary_tables(n_pos):
    inv_freq = np.float32(10000.0) ** (-2.0 * np.arange(HEAD_DIM // 2, dtype=np.float32) / HEAD_DIM).astype(np.float32)
    angles = np.arange(n_pos, dtype=np.float32)[:, None] * inv_freq.astype(np.float32)
    cos, sin = np.cos(angles), np.sin(angles)
    return (np.concatenate([cos, cos], axis=1).astype(np.float32), np.concatenate([-sin, sin], axis=1).astype(np.float32))


def solution(mesh):
    n_dev = mesh.shape['model']
    n_pair = 1 + (mesh.shape['replica'] + 1) % 2
    seq_spec = P('replica', 'model', None)
    col_spec = P(None, None, 'model')
    row_spec = P(None, 'model', None)
    gain_spec = P(None, None)
    tok_spec = P('replica', None)
    cache_spec = P(None, 'replica', None, 'model', None)
    in_specs = (seq_spec, P('replica'), tok_spec, gain_spec, col_spec, col_spec, col_spec, row_spec, gain_spec, col_spec, col_spec, row_spec)
    out_specs = (tok_spec, tok_spec, cache_spec, cache_spec)
    hbm = pl.BlockSpec(memory_space=pl.ANY)
    vmem = pl.BlockSpec(memory_space=pltpu.VMEM)
    smem = pl.BlockSpec(memory_space=pltpu.SMEM)
    dma = pltpu.SemaphoreType.DMA

    def per_device(prompt, lengths, new_tok, norm_attn, w_q, w_k, w_v, w_o, norm_mlp, w_gate, w_up, w_down):
        n_batch, seq_loc, d_model = prompt.shape
        kv_width = w_k.shape[2]
        heads = kv_width // HEAD_DIM
        seq_len = seq_loc * n_dev
        half = n_batch // 2
        n_chunk = half // GROUP
        width = d_model // n_dev
        wq, wk, wv, wo, wg, wu, wd = w_q[0], w_k[0], w_v[0], w_o[0], w_gate[0], w_up[0], w_down[0]
        cos_tab, sin_tab = (jnp.asarray(t) for t in rotary_tables(seq_len + 8))

        ff = wg.shape[1]
        n_q, n_row, two = 4 * half, 2 * n_batch, dma((2,))
        cache = jax.ShapeDtypeStruct((n_batch, seq_len + 1, heads, HEAD_DIM), BF16)
        cube, square, chunked = dma((2, 2, 2)), dma((2, 2)), dma((2, n_chunk))
        scratch = lambda *shape, dtype=F32: pltpu.VMEM(shape, dtype)
        held = pltpu.VMEM(cache.shape, BF16)
        tail = jax.ShapeDtypeStruct((n_batch, d_model), BF16)
        n_chip = n_dev // 2
        key_cache, val_cache, dec, last = pl.pallas_call(
            functools.partial(layer_kernel, n_dev, n_pair),
            out_shape=(held, held, pltpu.VMEM(tail.shape, BF16), pltpu.VMEM(tail.shape, BF16)),
            in_specs=[smem] + [hbm] * 13,
            out_specs=(vmem,) * 4,
            scratch_shapes=[
                scratch(3, 2, 2, d_model, kv_width, dtype=BF16),
                scratch(d_model, kv_width, dtype=BF16),
                scratch(kv_width, d_model, dtype=BF16),
                scratch(n_batch, seq_loc, d_model, dtype=BF16),
                scratch(2, half, seq_loc, d_model, dtype=BF16),
                scratch(4, 4, 2, half, seq_loc, heads, HEAD_DIM, dtype=BF16),
                scratch(2 * GROUP * seq_loc, HEAD_DIM),
                scratch(n_batch, d_model), scratch(n_chip, n_batch, width),
                scratch(n_chip, n_batch, width), scratch(n_chip, n_batch, width),
                scratch(n_dev, n_batch, width, dtype=BF16),
                scratch(n_row, HEAD_DIM), scratch(n_row, HEAD_DIM),
                scratch(n_row, d_model, dtype=BF16),
                scratch(2 * n_q, HEAD_DIM), scratch(n_dev, 2 * n_q, HEAD_DIM, dtype=BF16),
                scratch(n_batch, heads, HEAD_DIM, dtype=BF16), scratch(n_batch, heads, HEAD_DIM, dtype=BF16),
                scratch(2 * n_q, HEAD_DIM), scratch(2 * n_q, HEAD_DIM),
                scratch(n_q, 2 * half * seq_loc, dtype=jnp.int32),
                scratch(3, 4, 2, n_q, HEAD_DIM), scratch(4, 4, 2, n_q, HEAD_DIM),
                scratch(n_row, kv_width),
                scratch(2, n_row, d_model), scratch(2, n_chip, n_row, width),
                scratch(2, n_chip, n_row, width), scratch(2, 2, n_row, width // 2),
                scratch(2, 2, n_row, width), scratch(2, 2, n_row, width),
                scratch(2, n_dev, n_row, width, dtype=BF16),
                scratch(n_batch, d_model, dtype=BF16), scratch(1, d_model, dtype=BF16), scratch(1, d_model, dtype=BF16),
                scratch(seq_len + 8, HEAD_DIM), scratch(seq_len + 8, HEAD_DIM),
                dma((2 * n_chunk,)), dma((4,)), cube, cube, square, cube, dma(()), square,
                chunked, chunked,
                two, dma(()), two, dma((3, 6)), dma((4, 6)), dma((16,)), dma((5,)),
            ],
            compiler_params=pltpu.CompilerParams(collective_id=0, has_side_effects=True, vmem_limit_bytes=VMEM_MIB * 2 ** 20),
            name='layer',
        )(*(pltpu.with_memory_space_constraint(a, pltpu.HBM) for a in
            (lengths, prompt, wk, wv, wq, wo, wg, wu, wd, new_tok, norm_attn, norm_mlp, cos_tab, sin_tab)))
        key_cache, val_cache, dec, last = pl.pallas_call(
            deliver_kernel, out_shape=(cache, cache, tail, tail), in_specs=[vmem] * 4, out_specs=(hbm,) * 4,
            scratch_shapes=[dma((2 * PARTS + 2,))], name='deliver',
            compiler_params=pltpu.CompilerParams(vmem_limit_bytes=14 * 2 ** 20),
        )(key_cache, val_cache, dec, last)
        return dec, last, key_cache[None], val_cache[None]

    return jax.shard_map(per_device, mesh=mesh, in_specs=in_specs, out_specs=out_specs, check_vma=False)
```
